16 devices in a mesh: nodes: 16 (over z, y, x, core).
Axes of the slice: x: 2, y: 2, z: 2, core: 2. Of those that a mesh axis runs over, the one named last changes fastest.
Arguments:
- adjacency: bfloat16 [16384, 16384], P('nodes')
- features: bfloat16 [16384, 602], P('nodes')
- w_one: float32 [602, 128], replicated
- w_two: float32 [128, 41], replicated
- labels: int32 [16384], P('nodes')
- label_mask: int32 [16384], P('nodes')
Outputs:
- output 1: float32 [1], replicated
- output 2: float32 [602, 128], replicated
- output 3: float32 [128, 41], replicated
All inputs are finite; a program needn't handle non-finite values.
Results may differ from the reference program's by a relative error of at most 0.001.
Values are sent between devices in bfloat16 or wider.
A program may use at most 1 GiB of HBM per device.

```python
import math
import jax
import jax.numpy as jnp
from jax import lax

NODES = 16384
BLOCK_ROWS = 1024
F_IN = 602
HIDDEN = 128
CLASSES = 41

ROW_CONTRACT = (((0,), (0,)), ((), ()))
COL_CONTRACT = (((1,), (1,)), ((), ()))


def setup_inputs(seed: int = 0) -> dict:
    key_list = jax.random.split(jax.random.key(seed), 8)
    num_comms = NODES // BLOCK_ROWS
    shifts = jax.random.randint(key_list[0], (2,), 1, num_comms)
    col_ids = jnp.arange(NODES)
    col_comm = col_ids // BLOCK_ROWS
    row_ids = jnp.arange(BLOCK_ROWS)

    def draw_rows(block_idx):
        hot_cols = (col_comm == (block_idx + shifts[0]) % num_comms) | (col_comm == (block_idx + shifts[1]) % num_comms)
        edge_prob = jnp.where(hot_cols, 0.5, 0.01)
        coin_flip = jax.random.uniform(jax.random.fold_in(key_list[1], block_idx), (BLOCK_ROWS, NODES))
        self_loop = col_ids[None, :] == block_idx * BLOCK_ROWS + row_ids[:, None]
        raw_edges = jnp.where((coin_flip < edge_prob[None, :]) | self_loop, 1.0, 0.0)
        return (raw_edges / jnp.sum(raw_edges, axis=1, keepdims=True)).astype(jnp.bfloat16)

    adjacency = lax.map(draw_rows, jnp.arange(num_comms)).reshape(NODES, NODES)
    centers = jax.random.normal(key_list[2], (num_comms, F_IN))
    feat_noise = jax.random.normal(key_list[3], (NODES, F_IN))
    features = (jnp.repeat(centers, BLOCK_ROWS, axis=0) + feat_noise).astype(jnp.bfloat16)
    w_one = jax.random.normal(key_list[4], (F_IN, HIDDEN)) * math.sqrt(2.0 / F_IN)
    w_two = jax.random.normal(key_list[5], (HIDDEN, CLASSES)) * (2.0 / math.sqrt(HIDDEN))
    labels = jax.random.randint(key_list[6], (NODES,), 0, CLASSES, dtype=jnp.int32)
    drawn_mask = jax.random.randint(key_list[7], (NODES,), 0, 10, dtype=jnp.int32) < 3
    label_mask = jnp.where((jnp.arange(NODES) % 10 == 0) | drawn_mask, 1, 0).astype(jnp.int32)
    return {'adjacency': adjacency, 'features': features, 'w_one': w_one.astype(jnp.float32), 'w_two': w_two.astype(jnp.float32), 'labels': labels, 'label_mask': label_mask}


def reference(adjacency, features, w_one, w_two, labels, label_mask):
    weight_one = w_one.astype(jnp.bfloat16)
    weight_two = w_two.astype(jnp.bfloat16)
    agg_one = jnp.dot(adjacency, features, preferred_element_type=jnp.float32).astype(jnp.bfloat16)
    pre_one = jnp.dot(agg_one, weight_one, preferred_element_type=jnp.float32)
    hidden = jnp.maximum(pre_one, 0.0).astype(jnp.bfloat16)
    agg_two = jnp.dot(adjacency, hidden, preferred_element_type=jnp.float32).astype(jnp.bfloat16)
    logits = jnp.dot(agg_two, weight_two, preferred_element_type=jnp.float32)
    weight = label_mask.astype(jnp.float32)
    label_count = jnp.sum(weight)
    onehot = (labels[:, None] == jnp.arange(CLASSES)[None, :]).astype(jnp.float32)
    log_prob = jax.nn.log_softmax(logits, axis=-1)
    loss_value = -jnp.sum(weight * jnp.sum(onehot * log_prob, axis=-1)) / label_count
    grad_two = (weight[:, None] * (jnp.exp(log_prob) - onehot) / label_count).astype(jnp.bfloat16)
    dw_two = lax.dot_general(agg_two, grad_two, ROW_CONTRACT, preferred_element_type=jnp.float32)
    back_two = lax.dot_general(grad_two, weight_two, COL_CONTRACT, preferred_element_type=jnp.float32).astype(jnp.bfloat16)
    d_hidden = lax.dot_general(adjacency, back_two, ROW_CONTRACT, preferred_element_type=jnp.float32)
    grad_one = jnp.where(pre_one > 0.0, d_hidden, 0.0).astype(jnp.bfloat16)
    dw_one = lax.dot_general(agg_one, grad_one, ROW_CONTRACT, preferred_element_type=jnp.float32)
    return (loss_value.reshape(1), dw_one, dw_two)
```

```python
import functools

import jax
import jax.numpy as jnp
from jax import lax
from jax.experimental import pallas as pl
from jax.experimental.pallas import tpu as pltpu
from jax.sharding import PartitionSpec as P

MESH = pl.DeviceIdType.MESH
AXIS = 'nodes'
TREES = 4
STEPS = 8
ROW_CONTRACT = (((0,), (0,)), ((), ()))
COL_CONTRACT = (((1,), (1,)), ((), ()))


def tree_axis(tree, k, core, chip):
    if tree < 3:
        weight = 2 ** ((tree + k) % 3)
        return weight, lax.rem(chip // weight, 2)
    weight = (1 - core) * 2 ** k + core * 2 ** (2 - k)
    low, high = lax.rem(chip // 2 ** k, 2), lax.rem(chip // 2 ** (2 - k), 2)
    return weight, (1 - core) * low + core * high


def chip_at(tree, offset, core, chip):
    out = chip
    for k in range(3):
        weight, bit = tree_axis(tree, k, core, chip)
        out = out + lax.rem(offset // 2 ** k, 2) * weight * (1 - 2 * bit)
    return out


def unit_at(tree, offset, core, chip):
    return (chip_at(tree, offset, core, chip) * 2 + core) * TREES + tree


def neighbour(tree, k, core, chip):
    weight, bit = tree_axis(tree, k, core, chip)
    return (chip + weight * (1 - 2 * bit)) * 2 + core


def remote(src, dst, send_sem, recv_sem, device):
    return pltpu.make_async_remote_copy(src_ref=src, dst_ref=dst, send_sem=send_sem, recv_sem=recv_sem, device_id=(device,), device_id_type=MESH)


def place():
    me = lax.axis_index(AXIS)
    core, chip = lax.rem(me, 2), me // 2
    return me, core, chip, chip * 2 + 1 - core


def gather_start(own, buf, sems):
    send, recv, dsend, drecv = sems
    me, core, chip, partner = place()
    for k in range(3):
        for t in range(TREES):
            u = me * TREES + t
            remote(own.at[t], buf.at[u], send.at[0, t, k], recv.at[2 ** k, t], neighbour(t, k, core, chip)).start()
    for t in range(TREES):
        u = me * TREES + t
        remote(own.at[t], buf.at[u], dsend.at[0, t], drecv.at[0, t], partner).start()


def gather_loop(own, buf, sems, consume):
    send, recv, dsend, drecv = sems
    me, core, chip, partner = place()

    def step(s, carry):
        for t in range(TREES):
            u = unit_at(t, s, core, chip)

            @pl.when(s > 0)
            def _():
                remote(own.at[t], buf.at[u], send.at[0, t, 0], recv.at[s, t], partner).wait_recv()
                for k in range(1, 3):
                    @pl.when(s < 2 ** k)
                    def _():
                        remote(buf.at[u], buf.at[u], send.at[s, t, k], recv.at[s + 2 ** k, t], neighbour(t, k, core, chip)).start()
                remote(buf.at[u], buf.at[u], dsend.at[s, t], drecv.at[s, t], partner).start()
        for t in range(TREES):
            other = unit_at(t, s, 1 - core, chip)
            remote(own.at[t], buf.at[other], dsend.at[0, t], drecv.at[s, t], partner).wait_recv()
            consume(unit_at(t, s, core, chip), other)
        return carry

    lax.fori_loop(0, STEPS, step, 0)


def gather_drain(own, buf, sems):
    send, recv, dsend, drecv = sems
    me, core, chip, partner = place()

    def step(s, carry):
        for t in range(TREES):
            for k in range(3):
                @pl.when(s < 2 ** k)
                def _():
                    remote(own.at[t], buf.at[0], send.at[s, t, k], recv.at[0, t], partner).wait_send()
            remote(own.at[t], buf.at[0], dsend.at[s, t], drecv.at[0, t], partner).wait_send()
        return carry

    lax.fori_loop(0, STEPS, step, 0)


def gather_sems():
    dma = pltpu.SemaphoreType.DMA
    return [dma((4, TREES, 3)), dma((STEPS, TREES)), dma((STEPS, TREES)), dma((STEPS, TREES))]


def barrier_near():
    me, core, chip, partner = place()
    sem = pltpu.get_barrier_semaphore()
    pl.semaphore_signal(sem, inc=1, device_id=(partner,), device_id_type=MESH)
    for k in range(3):
        pl.semaphore_signal(sem, inc=1, device_id=(neighbour(0, k, core, chip),), device_id_type=MESH)
    pl.semaphore_wait(sem, 4)


def load_adj(adj, adj_v, sems):
    blocks = sems.shape[0]
    width = adj.shape[1] // blocks
    return [pltpu.make_async_copy(adj.at[:, pl.ds(b * width, width)], adj_v.at[:, pl.ds(b * width, width)], sems.at[b]) for b in range(blocks)]


def layer_one_kernel(x_ref, w_ref, adj, s_ref, z_ref, h_ref, adj_v, buf, acc, adj_sem, *sems):
    me, core, chip, partner = place()
    loads = load_adj(adj, adj_v, adj_sem)
    for copy in loads:
        copy.start()
    barrier_near()
    gather_start(x_ref, buf, sems)
    width = x_ref.shape[2]
    for t in range(TREES):
        buf[me * TREES + t] = x_ref[t]
    acc[...] = jnp.zeros_like(acc)
    for copy in loads:
        copy.wait()

    def term(u):
        cols = pl.ds(pl.multiple_of(u * width, width), width)
        return lax.dot_general(buf[u], adj_v[:, cols], COL_CONTRACT, preferred_element_type=jnp.float32)

    def consume(mine, other):
        acc[...] += term(mine) + term(other)

    gather_loop(x_ref, buf, sems, consume)
    s_ref[...] = acc[...].astype(jnp.bfloat16)
    z = jnp.dot(w_ref[...], s_ref[...], preferred_element_type=jnp.float32)
    z_ref[...] = z
    h_ref[...] = jnp.maximum(z, 0.0).astype(jnp.bfloat16)
    gather_drain(x_ref, buf, sems)


def layer_one(x_units, w_rows, adj):
    rows, nodes = adj.shape
    units, feats, width = nodes // x_units.shape[2], x_units.shape[1], x_units.shape[2]
    hidden = w_rows.shape[0]
    vmem = pl.BlockSpec(memory_space=pltpu.VMEM)
    return pl.pallas_call(
        layer_one_kernel,
        name='layer_one',
        out_shape=(jax.ShapeDtypeStruct((feats, rows), jnp.bfloat16), jax.ShapeDtypeStruct((hidden, rows), jnp.float32), jax.ShapeDtypeStruct((hidden, rows), jnp.bfloat16)),
        in_specs=[vmem, vmem, pl.BlockSpec(memory_space=pl.ANY)],
        out_specs=(vmem, vmem, vmem),
        scratch_shapes=[pltpu.VMEM((rows, nodes), jnp.bfloat16), pltpu.VMEM((units, feats, width), jnp.bfloat16), pltpu.VMEM((feats, rows), jnp.float32), pltpu.SemaphoreType.DMA((16,)), *gather_sems()],
        compiler_params=pltpu.CompilerParams(collective_id=0, has_side_effects=True, vmem_limit_bytes=67043328),
        cost_estimate=pl.CostEstimate(flops=2 * rows * nodes * feats, bytes_accessed=2 * rows * nodes, transcendentals=0),
    )(x_units, w_rows, adj)


def solution(mesh):
    axis_name = AXIS

    def local_step(adj_rows, feat_rows, w_one, w_two, label_rows, mask_rows):
        rows, feats = feat_rows.shape
        padded = -(-feats // 16) * 16
        width = rows // TREES
        x_units = jnp.pad(feat_rows.reshape(TREES, width, feats).transpose(0, 2, 1), ((0, 0), (0, padded - feats), (0, 0)))
        w_rows = jnp.pad(w_one.T, ((0, 0), (0, padded - feats))).astype(jnp.bfloat16)
        agg_one, pre_one, hidden = layer_one(x_units, w_rows, adj_rows)
        weight_two = w_two.astype(jnp.bfloat16)
        num_classes = w_two.shape[1]
        hidden_all = lax.all_gather(hidden, axis_name, tiled=True, axis=1)
        agg_two = lax.dot_general(adj_rows, hidden_all, COL_CONTRACT, preferred_element_type=jnp.float32).astype(jnp.bfloat16)
        logits = jnp.dot(agg_two, weight_two, preferred_element_type=jnp.float32)
        weight = mask_rows.astype(jnp.float32)
        label_count = lax.psum(jnp.sum(weight), axis_name)
        onehot = (label_rows[:, None] == jnp.arange(num_classes)[None, :]).astype(jnp.float32)
        log_prob = jax.nn.log_softmax(logits, axis=-1)
        loss_sum = lax.psum(-jnp.sum(weight * jnp.sum(onehot * log_prob, axis=-1)), axis_name)
        grad_two = (weight[:, None] * (jnp.exp(log_prob) - onehot) / label_count).astype(jnp.bfloat16)
        dw_two = lax.psum(lax.dot_general(agg_two, grad_two, ROW_CONTRACT, preferred_element_type=jnp.float32), axis_name)
        back_two = lax.dot_general(grad_two, weight_two, COL_CONTRACT, preferred_element_type=jnp.float32).astype(jnp.bfloat16)
        part_sums = lax.dot_general(adj_rows, back_two, ROW_CONTRACT, preferred_element_type=jnp.float32)
        d_hidden = lax.psum_scatter(part_sums, axis_name, scatter_dimension=0, tiled=True)
        grad_one = jnp.where(pre_one.T > 0.0, d_hidden, 0.0).astype(jnp.bfloat16)
        dw_one = lax.psum(lax.dot_general(agg_one, grad_one, (((1,), (0,)), ((), ())), preferred_element_type=jnp.float32), axis_name)[:feats]
        return ((loss_sum / label_count).reshape(1), dw_one, dw_two)

    return jax.shard_map(local_step, mesh=mesh, in_specs=(P(axis_name, None), P(axis_name, None), P(None, None), P(None, None), P(axis_name), P(axis_name)), out_specs=(P(None), P(None, None), P(None, None)), check_vma=False)
```

```python
import functools

import jax
import jax.numpy as jnp
from jax import lax
from jax.experimental import pallas as pl
from jax.experimental.pallas import tpu as pltpu
from jax.sharding import PartitionSpec as P

MESH = pl.DeviceIdType.MESH
AXIS = 'nodes'
TREES = 4
STEPS = 8
COL_CONTRACT = (((1,), (1,)), ((), ()))
ROW_CONTRACT = (((0,), (0,)), ((), ()))


def tree_axis(tree, k, core, chip):
    if tree < 3:
        weight = 2 ** ((tree + k) % 3)
        return weight, lax.rem(chip // weight, 2)
    weight = (1 - core) * 2 ** k + core * 2 ** (2 - k)
    low, high = lax.rem(chip // 2 ** k, 2), lax.rem(chip // 2 ** (2 - k), 2)
    return weight, (1 - core) * low + core * high


def chip_at(tree, offset, core, chip):
    out = chip
    for k in range(3):
        weight, bit = tree_axis(tree, k, core, chip)
        out = out + lax.rem(offset // 2 ** k, 2) * weight * (1 - 2 * bit)
    return out


def unit_at(tree, offset, core, chip):
    return (chip_at(tree, offset, core, chip) * 2 + core) * TREES + tree


def neighbour(tree, k, core, chip):
    weight, bit = tree_axis(tree, k, core, chip)
    return (chip + weight * (1 - 2 * bit)) * 2 + core


def remote(src, dst, send_sem, recv_sem, device):
    return pltpu.make_async_remote_copy(src_ref=src, dst_ref=dst, send_sem=send_sem, recv_sem=recv_sem, device_id=(device,), device_id_type=MESH)


def place():
    me = lax.axis_index(AXIS)
    core, chip = lax.rem(me, 2), me // 2
    return me, core, chip, chip * 2 + 1 - core


def gather_start(buf, sems):
    send, recv, dsend, drecv = sems
    me, core, chip, partner = place()
    for k in range(3):
        for t in range(TREES):
            u = me * TREES + t
            remote(buf.at[u], buf.at[u], send.at[0, t, k], recv.at[2 ** k, t], neighbour(t, k, core, chip)).start()
    for t in range(TREES):
        u = me * TREES + t
        remote(buf.at[u], buf.at[u], dsend.at[0, t], drecv.at[0, t], partner).start()


def gather_loop(buf, sems, consume):
    send, recv, dsend, drecv = sems
    me, core, chip, partner = place()

    def step(s, carry):
        for t in range(TREES):
            u = unit_at(t, s, core, chip)

            @pl.when(s > 0)
            def _():
                remote(buf.at[u], buf.at[u], send.at[0, t, 0], recv.at[s, t], partner).wait_recv()
                for k in range(1, 3):
                    @pl.when(s < 2 ** k)
                    def _():
                        remote(buf.at[u], buf.at[u], send.at[s, t, k], recv.at[s + 2 ** k, t], neighbour(t, k, core, chip)).start()
                remote(buf.at[u], buf.at[u], dsend.at[s, t], drecv.at[s, t], partner).start()
        for t in range(TREES):
            other = unit_at(t, s, 1 - core, chip)
            remote(buf.at[other], buf.at[other], dsend.at[0, t], drecv.at[s, t], partner).wait_recv()
            consume(unit_at(t, s, core, chip), other)
        return carry

    lax.fori_loop(0, STEPS, step, 0)


def gather_drain(buf, sems):
    send, recv, dsend, drecv = sems
    me, core, chip, partner = place()

    def step(s, carry):
        for t in range(TREES):
            for k in range(3):
                @pl.when(s < 2 ** k)
                def _():
                    remote(buf.at[0], buf.at[0], send.at[s, t, k], recv.at[0, t], partner).wait_send()
            remote(buf.at[0], buf.at[0], dsend.at[s, t], drecv.at[0, t], partner).wait_send()
        return carry

    lax.fori_loop(0, STEPS, step, 0)


def gather_sems():
    dma = pltpu.SemaphoreType.DMA
    return [dma((4, TREES, 3)), dma((STEPS, TREES)), dma((STEPS, TREES)), dma((STEPS, TREES))]


def barrier_all(n):
    me = lax.axis_index(AXIS)
    sem = pltpu.get_barrier_semaphore()
    for i in range(1, n):
        pl.semaphore_signal(sem, inc=1, device_id=(lax.rem(me + i, n),), device_id_type=MESH)
    pl.semaphore_wait(sem, n - 1)


def send_all(n, src, dst, send_sem, recv_sem):
    me = lax.axis_index(AXIS)
    for i in range(1, n):
        to = lax.rem(me + i, n)
        remote(src(to), dst, send_sem.at[i], recv_sem.at[i], to).start()


def wait_all(n, src, dst, send_sem, recv_sem):
    me = lax.axis_index(AXIS)
    for i in range(1, n):
        to = lax.rem(me + i, n)
        copy = remote(src(to), dst, send_sem.at[i], recv_sem.at[i], to)
        copy.wait_send()
        copy.wait_recv()


def forward_kernel(n, x_ref, w_ref, w2t_ref, y_ref, m_ref, adj, s_ref, z_ref, u_ref, small_ref,
                   adj_v, buf, acc, h_buf, count, adj_sem, x_sem, count_send, count_recv, *sems):
    me, core, chip, partner = place()
    sems_x, sems_h = sems[:4], sems[4:]
    width = buf.shape[2]
    hidden = h_buf.shape[1]
    fetch = [pltpu.make_async_copy(x_ref.at[:, pl.ds(t * width, width)], buf.at[me * TREES + t], x_sem.at[t]) for t in range(TREES)]
    for copy in fetch:
        copy.start()
    blocks = adj_sem.shape[0]
    block = adj.shape[1] // blocks
    loads = [pltpu.make_async_copy(adj.at[:, pl.ds(b * block, block)], adj_v.at[:, pl.ds(b * block, block)], adj_sem.at[b]) for b in range(blocks)]
    for copy in loads:
        copy.start()
    weight = m_ref[...].astype(jnp.float32)
    count[me] = jnp.broadcast_to(jnp.sum(weight, axis=1, keepdims=True), count.shape[1:])
    barrier_all(n)
    for copy in fetch:
        copy.wait()
    gather_start(buf, sems_x)
    send_all(n, lambda to: count.at[me], count.at[me], count_send, count_recv)
    acc[...] = jnp.zeros_like(acc)
    for copy in loads:
        copy.wait()

    def term(units, u):
        cols = pl.ds(pl.multiple_of(u * width, width), width)
        return lax.dot_general(units[u], adj_v[:, cols], COL_CONTRACT, preferred_element_type=jnp.float32)

    def consume_one(mine, other):
        acc[...] += term(buf, mine) + term(buf, other)

    def consume_two(mine, other):
        acc[0:hidden] += term(h_buf, mine) + term(h_buf, other)

    gather_loop(buf, sems_x, consume_one)
    s_ref[...] = acc[...].astype(jnp.bfloat16)
    w_rows = w_ref[...].astype(jnp.bfloat16)
    for t in range(TREES):
        cols = slice(t * width, (t + 1) * width)
        z = lax.dot_general(w_rows, s_ref[:, cols], ROW_CONTRACT, preferred_element_type=jnp.float32)
        z_ref[:, cols] = z
        h_buf[me * TREES + t] = jnp.maximum(z, 0.0).astype(jnp.bfloat16)
    gather_start(h_buf, sems_h)
    acc[0:hidden] = jnp.zeros_like(acc[0:hidden])
    gather_drain(buf, sems_x)
    wait_all(n, lambda to: count.at[me], count.at[me], count_send, count_recv)
    total = jnp.sum(count[...], axis=0)[0:1, 0:1]
    gather_loop(h_buf, sems_h, consume_two)

    s_two = acc[0:hidden].astype(jnp.bfloat16)
    w_two = w2t_ref[...].astype(jnp.bfloat16)
    logits = jnp.dot(w_two, s_two, preferred_element_type=jnp.float32)
    shifted = logits - jnp.max(logits, axis=0, keepdims=True)
    log_prob = shifted - jnp.log(jnp.sum(jnp.exp(shifted), axis=0, keepdims=True))
    hot = lax.broadcasted_iota(jnp.int32, logits.shape, 0) == y_ref[...]
    loss = -jnp.sum(weight * jnp.sum(jnp.where(hot, log_prob, 0.0), axis=0, keepdims=True), axis=1, keepdims=True)
    grad = (weight * (jnp.exp(log_prob) - hot.astype(jnp.float32)) / total).astype(jnp.bfloat16)
    u_ref[...] = lax.dot_general(w_two, grad, ROW_CONTRACT, preferred_element_type=jnp.float32).astype(jnp.bfloat16)
    classes = logits.shape[0]
    edge = small_ref.shape[0] - 8
    small_ref[0:classes] = lax.dot_general(grad, s_two, COL_CONTRACT, preferred_element_type=jnp.float32)
    small_ref[classes:edge] = jnp.zeros((edge - classes, hidden), jnp.float32)
    small_ref[edge:] = jnp.broadcast_to(loss / total, (8, hidden))
    gather_drain(h_buf, sems_h)


def forward(x_rows, w_one, w2t, labels, mask, adj):
    rows, nodes = adj.shape
    n = nodes // rows
    feats, width = x_rows.shape[0], rows // TREES
    classes, hidden = w2t.shape
    units = n * TREES
    edge = -(-classes // 8) * 8 + 8
    vmem, hbm = pl.BlockSpec(memory_space=pltpu.VMEM), pl.BlockSpec(memory_space=pl.ANY)
    dma = pltpu.SemaphoreType.DMA
    return pl.pallas_call(
        functools.partial(forward_kernel, n),
        name='forward',
        out_shape=(jax.ShapeDtypeStruct((feats, rows), jnp.bfloat16), jax.ShapeDtypeStruct((hidden, rows), jnp.float32),
                   jax.ShapeDtypeStruct((hidden, rows), jnp.bfloat16), jax.ShapeDtypeStruct((edge, hidden), jnp.float32)),
        in_specs=[hbm] + [vmem] * 4 + [hbm],
        out_specs=(vmem,) * 4,
        scratch_shapes=[
            pltpu.VMEM((rows, nodes), jnp.bfloat16), pltpu.VMEM((units, feats, width), jnp.bfloat16), pltpu.VMEM((feats, rows), jnp.float32),
            pltpu.VMEM((units, hidden, width), jnp.bfloat16), pltpu.VMEM((n, 8, 128), jnp.float32),
            dma((16,)), dma((TREES,)), dma((n,)), dma((n,)), *gather_sems(), *gather_sems()],
        compiler_params=pltpu.CompilerParams(collective_id=0, has_side_effects=True, vmem_limit_bytes=67043328),
        cost_estimate=pl.CostEstimate(flops=2 * rows * nodes * (feats + hidden), bytes_accessed=2 * rows * nodes, transcendentals=0),
    )(x_rows, w_one, w2t, labels, mask, adj)


def backward_kernel(n, u_ref, s_ref, z_ref, small_ref, adj, loss_ref, dw_ref, dw2_ref,
                    adj_v, stage, total, child, part, parts, whole, adj_sem, dsend, drecv, csend, crecv, fsend, frecv, gsend, grecv):
    me, core, chip, partner = place()
    width = adj_v.shape[2]

    def load(s, t, side):
        which = core + side - 2 * core * side
        u = unit_at(t, s, which, chip)
        cols = pl.ds(pl.multiple_of(u * width, width), width)
        return pltpu.make_async_copy(adj.at[:, cols], adj_v.at[(s * TREES + t) * 2 + side], adj_sem.at[s, t, side])

    def load_step(i, carry):
        s = STEPS - 1 - i
        for side in (1, 0):
            for t in range(TREES):
                load(s, t, side).start()
        return carry

    lax.fori_loop(0, STEPS, load_step, 0)
    barrier_all(n)

    def to_partner(s, t):
        return remote(stage.at[s, t], total.at[s, t], dsend.at[s, t], drecv.at[s, t], partner)

    def to_parent(s, t, k):
        return remote(total.at[s, t], child.at[s - 1, t], csend.at[s, t], crecv.at[s, t], neighbour(t, k, core, chip))

    def give(s):
        for t in range(TREES):
            load(s, t, 1).wait()
            stage[s, t] = jnp.dot(u_ref[...], adj_v[(s * TREES + t) * 2 + 1], preferred_element_type=jnp.float32)
            to_partner(s, t).start()

    def take(s):
        for t in range(TREES):
            load(s, t, 0).wait()
            mine = jnp.dot(u_ref[...], adj_v[(s * TREES + t) * 2], preferred_element_type=jnp.float32)
            to_partner(s, t).wait_recv()
            total[s, t] = total[s, t] + mine
            for k in range(3):
                @pl.when(s < 2 ** k)
                def _():
                    to_parent(s + 2 ** k, t, k).wait_recv()
                    total[s, t] = total[s, t] + child[s + 2 ** k - 1, t]
            for k in range(3):
                @pl.when((s >= 2 ** k) & (s < 2 ** (k + 1)))
                def _():
                    to_parent(s, t, k).start()

    def step(i, carry):
        @pl.when(i < STEPS)
        def _():
            give(STEPS - 1 - i)

        @pl.when(i > 0)
        def _():
            take(STEPS - i)
        return carry

    lax.fori_loop(0, STEPS + 1, step, 0)
    feats = s_ref.shape[0]
    start = -(-feats // 8) * 8
    grad = []
    for t in range(TREES):
        cols = slice(t * width, (t + 1) * width)
        grad.append(jnp.where(z_ref[:, cols] > 0.0, total[0, t], 0.0).astype(jnp.bfloat16))
    part[0:feats] = lax.dot_general(s_ref[...], jnp.concatenate(grad, axis=1), COL_CONTRACT, preferred_element_type=jnp.float32)
    extra = small_ref.shape[0]
    part[feats:start] = jnp.zeros((start - feats, part.shape[1]), jnp.float32)
    part[start:start + extra] = small_ref[...]
    part[start + extra:] = jnp.zeros_like(part[start + extra:])
    share = part.shape[0] // n

    def rows_of(to):
        return part.at[pl.ds(pl.multiple_of(to * share, 8), share)]

    send_all(n, rows_of, parts.at[me], fsend, frecv)
    parts[me] = part[pl.ds(pl.multiple_of(me * share, 8), share)]

    def drain(s, carry):
        for t in range(TREES):
            to_partner(s, t).wait_send()

            @pl.when(s > 0)
            def _():
                to_parent(s, t, 0).wait_send()
        return carry

    lax.fori_loop(0, STEPS, drain, 0)
    wait_all(n, rows_of, parts.at[me], fsend, frecv)
    mine = whole.at[pl.ds(pl.multiple_of(me * share, 8), share)]
    mine[...] = jnp.sum(parts[...], axis=0)
    send_all(n, lambda to: mine, mine, gsend, grecv)
    wait_all(n, lambda to: mine, mine, gsend, grecv)
    dw_ref[...] = whole[0:feats]
    dw2_ref[...] = whole[start:start + dw2_ref.shape[0]]
    loss_ref[...] = whole[start + extra - 8:start + extra]


def backward(classes, u, s, z, small, adj):
    rows, nodes = adj.shape
    n = nodes // rows
    hidden, feats = u.shape[0], s.shape[0]
    width = rows // TREES
    share = -(-(-(-feats // 8) * 8 + small.shape[0]) // (8 * n)) * 8
    vmem = pl.BlockSpec(memory_space=pltpu.VMEM)
    dma = pltpu.SemaphoreType.DMA
    block = (TREES, hidden, width)
    return pl.pallas_call(
        functools.partial(backward_kernel, n),
        name='backward',
        out_shape=(jax.ShapeDtypeStruct((8, hidden), jnp.float32), jax.ShapeDtypeStruct((feats, hidden), jnp.float32), jax.ShapeDtypeStruct((classes, hidden), jnp.float32)),
        in_specs=[vmem] * 4 + [pl.BlockSpec(memory_space=pl.ANY)],
        out_specs=(vmem,) * 3,
        scratch_shapes=[
            pltpu.VMEM((2 * n // 2 * TREES, rows, width), jnp.bfloat16), pltpu.VMEM((STEPS, *block), jnp.float32), pltpu.VMEM((STEPS, *block), jnp.float32),
            pltpu.VMEM((STEPS - 1, *block), jnp.float32), pltpu.VMEM((n * share, hidden), jnp.float32), pltpu.VMEM((n, share, hidden), jnp.float32),
            pltpu.VMEM((n * share, hidden), jnp.float32), dma((STEPS, TREES, 2)), dma((STEPS, TREES)), dma((STEPS, TREES)), dma((STEPS, TREES)), dma((STEPS, TREES)),
            dma((n,)), dma((n,)), dma((n,)), dma((n,))],
        compiler_params=pltpu.CompilerParams(collective_id=1, has_side_effects=True, vmem_limit_bytes=67043328),
        cost_estimate=pl.CostEstimate(flops=2 * rows * nodes * hidden, bytes_accessed=2 * rows * nodes, transcendentals=0),
    )(u, s, z, small, adj)


def solution(mesh):
    axis_name = AXIS

    def local_step(adj_rows, feat_rows, w_one, w_two, label_rows, mask_rows):
        rows = adj_rows.shape[0]
        s, z, u, small = forward(feat_rows.T, w_one, w_two.T, label_rows.reshape(1, rows), mask_rows.reshape(1, rows), adj_rows)
        loss, dw_one, dw_two = backward(w_two.shape[1], u, s, z, small, adj_rows)
        return loss[0, 0:1], dw_one, dw_two.T

    return jax.shard_map(local_step, mesh=mesh, in_specs=(P(axis_name, None), P(axis_name, None), P(None, None), P(None, None), P(axis_name), P(axis_name)), out_specs=(P(None), P(None, None), P(None, None)), check_vma=False)
```

```python
import functools

import jax
import jax.numpy as jnp
from jax import lax
from jax.experimental import pallas as pl
from jax.experimental.pallas import tpu as pltpu
from jax.sharding import PartitionSpec as P

MESH = pl.DeviceIdType.MESH
AXIS = 'nodes'
TREES = 4
RING = 4
STEPS = 8
COL_CONTRACT = (((1,), (1,)), ((), ()))
ROW_CONTRACT = (((0,), (0,)), ((), ()))


def tree_axis(tree, k, core, chip):
    if tree < 3:
        weight = 2 ** ((tree + k) % 3)
        return weight, lax.rem(chip // weight, 2)
    weight = (1 - core) * 2 ** k + core * 2 ** (2 - k)
    low, high = lax.rem(chip // 2 ** k, 2), lax.rem(chip // 2 ** (2 - k), 2)
    return weight, (1 - core) * low + core * high


def chip_at(tree, offset, core, chip):
    out = chip
    for k in range(3):
        weight, bit = tree_axis(tree, k, core, chip)
        out = out + lax.rem(offset // 2 ** k, 2) * weight * (1 - 2 * bit)
    return out


def unit_at(tree, offset, core, chip):
    return (chip_at(tree, offset, core, chip) * 2 + core) * TREES + tree


def neighbour(tree, k, core, chip):
    weight, bit = tree_axis(tree, k, core, chip)
    return (chip + weight * (1 - 2 * bit)) * 2 + core


def remote(src, dst, send_sem, recv_sem, device):
    return pltpu.make_async_remote_copy(src_ref=src, dst_ref=dst, send_sem=send_sem, recv_sem=recv_sem, device_id=(device,), device_id_type=MESH)


def place():
    me = lax.axis_index(AXIS)
    core, chip = lax.rem(me, 2), me // 2
    return me, core, chip, chip * 2 + 1 - core


def gather_send(buf, sems, tree, offset, k, unit):
    send, recv, dsend, drecv = sems
    me, core, chip, partner = place()
    remote(buf.at[unit], buf.at[unit], send.at[offset, tree, k], recv.at[offset + 2 ** k, tree], neighbour(tree, k, core, chip)).start()


def gather_hand(buf, sems, tree, offset, unit):
    send, recv, dsend, drecv = sems
    me, core, chip, partner = place()
    remote(buf.at[unit], buf.at[unit], dsend.at[offset, tree], drecv.at[offset, tree], partner).start()


def gather_start(buf, sems):
    me = lax.axis_index(AXIS)
    for k in range(2):
        for t in range(TREES):
            gather_send(buf, sems, t, 0, k, me * TREES + t)
    for t in range(TREES):
        gather_hand(buf, sems, t, 0, me * TREES + t)


def gather_arrive(buf, sems, s):
    send, recv, dsend, drecv = sems
    me, core, chip, partner = place()
    units = [unit_at(t, s, core, chip) for t in range(TREES)]
    for t, u in enumerate(units):
        remote(buf.at[u], buf.at[u], send.at[0, t, 0], recv.at[s, t], partner).wait_recv()

        @pl.when(s == 1)
        def _():
            gather_send(buf, sems, t, s, 1, u)

        @pl.when((s > 1) & (s < 4))
        def _():
            gather_send(buf, sems, t, s, 2, u)
        gather_hand(buf, sems, t, s, u)

    @pl.when(s == 1)
    def _():
        for t in range(TREES):
            gather_send(buf, sems, t, 0, 2, me * TREES + t)
        for t, u in enumerate(units):
            gather_send(buf, sems, t, s, 2, u)


def gather_take(buf, sems, s):
    send, recv, dsend, drecv = sems
    me, core, chip, partner = place()
    others = [unit_at(t, s, 1 - core, chip) for t in range(TREES)]
    for t, u in enumerate(others):
        remote(buf.at[u], buf.at[u], dsend.at[0, t], drecv.at[s, t], partner).wait_recv()
    return [unit_at(t, s, core, chip) for t in range(TREES)] + others


def gather_drain(buf, sems):
    send, recv, dsend, drecv = sems
    me, core, chip, partner = place()

    def step(s, carry):
        for t in range(TREES):
            for k in range(3):
                @pl.when(s < 2 ** k)
                def _():
                    remote(buf.at[0], buf.at[0], send.at[s, t, k], recv.at[0, t], partner).wait_send()
            remote(buf.at[0], buf.at[0], dsend.at[s, t], drecv.at[0, t], partner).wait_send()
        return carry

    lax.fori_loop(0, STEPS, step, 0)


def gather_sems():
    dma = pltpu.SemaphoreType.DMA
    return [dma((4, TREES, 3)), dma((STEPS, TREES)), dma((STEPS, TREES)), dma((STEPS, TREES))]


def barrier_all(n):
    me = lax.axis_index(AXIS)
    sem = pltpu.get_barrier_semaphore()
    for i in range(1, n):
        pl.semaphore_signal(sem, inc=1, device_id=(lax.rem(me + i, n),), device_id_type=MESH)
    pl.semaphore_wait(sem, n - 1)


def send_all(n, src, dst, send_sem, recv_sem):
    me = lax.axis_index(AXIS)
    for i in range(1, n):
        to = lax.rem(me + i, n)
        remote(src(to), dst, send_sem.at[i], recv_sem.at[i], to).start()


def wait_all(n, src, dst, send_sem, recv_sem):
    me = lax.axis_index(AXIS)
    for i in range(1, n):
        to = lax.rem(me + i, n)
        copy = remote(src(to), dst, send_sem.at[i], recv_sem.at[i], to)
        copy.wait_send()
        copy.wait_recv()


def step_kernel(n, x_ref, w_hbm, w2t_ref, y_ref, m_ref, adj, loss_ref, dw_ref, dw2_ref,
                ring, buf, acc, h_buf, s_one, z_one, u_two, w_v, small, count, stage, mine, total, child, part, parts, whole,
                ring_sem, x_sem, w_sem, count_send, count_recv, dsend, drecv, csend, crecv, fsend, frecv, gsend, grecv, *sems):
    me, core, chip, partner = place()
    sems_x, sems_h = sems[:4], sems[4:]
    width = buf.shape[2]
    feats, rows = acc.shape
    hidden = h_buf.shape[1]
    chunks = [slice(t * width, (t + 1) * width) for t in range(TREES)]

    def slab(s, slot, j):
        u = unit_at(j % TREES, s, core if j < TREES else 1 - core, chip)
        return pltpu.make_async_copy(adj.at[:, pl.ds(pl.multiple_of(u * width, width), width)], ring.at[slot * 8 + j], ring_sem.at[slot, j])

    def load(s, slot, order=range(8)):
        for j in order:
            slab(s, slot, j).start()

    with jax.named_scope('start'):
        fetch = [pltpu.make_async_copy(x_ref.at[:, pl.ds(t * width, width)], buf.at[me * TREES + t], x_sem.at[t]) for t in range(TREES)]
        for copy in fetch:
            copy.start()
        weight = m_ref[...].astype(jnp.float32)
        count[me] = jnp.broadcast_to(jnp.sum(weight, axis=1, keepdims=True), count.shape[1:])
        barrier_all(n)
        for copy in fetch:
            copy.wait()
    gather_start(buf, sems_x)
    send_all(n, lambda to: count.at[me], count.at[me], count_send, count_recv)
    weights = pltpu.make_async_copy(w_hbm, w_v, w_sem)
    weights.start()
    for s in range(RING):
        load(s, s)
    acc[...] = jnp.zeros_like(acc)
    with jax.named_scope('arrive'):
        gather_arrive(buf, sems_x, 1)

    def aggregate(units_ref, units, slot, out):
        for j in range(8):
            slab(0, slot, j).wait()
        for cols in chunks:
            out[:, cols] += sum(lax.dot_general(units_ref[u], ring[slot * 8 + j, cols], COL_CONTRACT, preferred_element_type=jnp.float32) for j, u in enumerate(units))

    def step_one(s, carry):
        with jax.named_scope('arrive'):
            @pl.when(s > 1)
            def _():
                gather_arrive(buf, sems_x, s)
            units = gather_take(buf, sems_x, s)
        with jax.named_scope('consume'):
            slot = lax.rem(s, RING)
            aggregate(buf, units, slot, acc)
            load(lax.rem(s + RING, STEPS), slot)
        return carry

    lax.fori_loop(0, STEPS, step_one, 0)
    with jax.named_scope('mid'):
        weights.wait()
        s_one[...] = acc[...].astype(jnp.bfloat16)
        w_rows = w_v[...].astype(jnp.bfloat16)
        for t, cols in enumerate(chunks):
            z = lax.dot_general(w_rows, s_one[:, cols], ROW_CONTRACT, preferred_element_type=jnp.float32)
            z_one[:, cols] = z
            h_buf[me * TREES + t] = jnp.maximum(z, 0.0).astype(jnp.bfloat16)
    gather_start(h_buf, sems_h)
    two = acc.at[0:hidden]
    two[...] = jnp.zeros_like(two)
    with jax.named_scope('arrive'):
        gather_arrive(h_buf, sems_h, 1)

    def step_two(s, carry):
        with jax.named_scope('arrive'):
            @pl.when(s > 1)
            def _():
                gather_arrive(h_buf, sems_h, s)
            units = gather_take(h_buf, sems_h, s)
        with jax.named_scope('consume'):
            slot = lax.rem(s, RING)
            aggregate(h_buf, units, slot, two)
            late = s // RING
            load((1 - late) * (s + RING) + late * (STEPS + RING - 1 - s), slot)
        return carry

    lax.fori_loop(0, STEPS, step_two, 0)
    with jax.named_scope('soft'):
        wait_all(n, lambda to: count.at[me], count.at[me], count_send, count_recv)
        labelled = jnp.sum(count[...], axis=0)[0:1, 0:1]
        s_two = two[...].astype(jnp.bfloat16)
        w_two = w2t_ref[...].astype(jnp.bfloat16)
        logits = jnp.dot(w_two, s_two, preferred_element_type=jnp.float32)
        shifted = logits - jnp.max(logits, axis=0, keepdims=True)
        log_prob = shifted - jnp.log(jnp.sum(jnp.exp(shifted), axis=0, keepdims=True))
        hot = lax.broadcasted_iota(jnp.int32, logits.shape, 0) == y_ref[...]
        grad = (weight * (jnp.exp(log_prob) - hot.astype(jnp.float32)) / labelled).astype(jnp.bfloat16)
        u_two[...] = lax.dot_general(w_two, grad, ROW_CONTRACT, preferred_element_type=jnp.float32).astype(jnp.bfloat16)
        loss = -jnp.sum(weight * jnp.sum(jnp.where(hot, log_prob, 0.0), axis=0, keepdims=True), axis=1, keepdims=True)
        classes = logits.shape[0]
        edge = small.shape[0] - 8
        small[0:classes] = lax.dot_general(grad, s_two, COL_CONTRACT, preferred_element_type=jnp.float32)
        small[classes:edge] = jnp.zeros((edge - classes, hidden), jnp.float32)
        small[edge:] = jnp.broadcast_to(loss / labelled, (8, hidden))

    def to_partner(s, t):
        return remote(stage.at[s, t], total.at[s, t], dsend.at[s, t], drecv.at[s, t], partner)

    def to_parent(s, t, k):
        return remote(total.at[s, t], child.at[s - 1, t], csend.at[s, t], crecv.at[s, t], neighbour(t, k, core, chip))

    def step_back(i, carry):
        s = STEPS - 1 - i
        slot = lax.rem(i, RING)
        with jax.named_scope('give'):
            for j in range(8):
                slab(0, slot, j).wait()
            for t in range(TREES):
                stage[s, t] = jnp.dot(u_two[...], ring[slot * 8 + TREES + t], preferred_element_type=jnp.float32)
            for t in range(TREES):
                to_partner(s, t).start()
            for t in range(TREES):
                mine[t] = jnp.dot(u_two[...], ring[slot * 8 + t], preferred_element_type=jnp.float32)

            @pl.when(i + RING < STEPS)
            def _():
                load(s - RING, slot, (4, 5, 6, 7, 0, 1, 2, 3))
        with jax.named_scope('take'):
            for t in range(TREES):
                to_partner(s, t).wait_recv()
                total[s, t] = total[s, t] + mine[t]
                for k in range(3):
                    @pl.when(s < 2 ** k)
                    def _():
                        to_parent(s + 2 ** k, t, k).wait_recv()
                        total[s, t] = total[s, t] + child[s + 2 ** k - 1, t]
                for k in range(3):
                    @pl.when((s >= 2 ** k) & (s < 2 ** (k + 1)))
                    def _():
                        to_parent(s, t, k).start()
        return carry

    lax.fori_loop(0, STEPS, step_back, 0)
    start = -(-feats // 8) * 8
    extra = small.shape[0]
    with jax.named_scope('dw'):
        grads = [jnp.where(z_one[:, cols] > 0.0, total[0, t], 0.0).astype(jnp.bfloat16) for t, cols in enumerate(chunks)]
        part[0:feats] = lax.dot_general(s_one[...], jnp.concatenate(grads, axis=1), COL_CONTRACT, preferred_element_type=jnp.float32)
        part[feats:start] = jnp.zeros((start - feats, part.shape[1]), jnp.float32)
        part[start:start + extra] = small[...]
        part[start + extra:] = jnp.zeros_like(part[start + extra:])
    share = part.shape[0] // n

    def rows_of(to):
        return part.at[pl.ds(pl.multiple_of(to * share, 8), share)]

    send_all(n, rows_of, parts.at[me], fsend, frecv)
    parts[me] = part[pl.ds(pl.multiple_of(me * share, 8), share)]

    def drain(s, carry):
        for t in range(TREES):
            to_partner(s, t).wait_send()

            @pl.when(s > 0)
            def _():
                to_parent(s, t, 0).wait_send()
        return carry

    with jax.named_scope('drain'):
        gather_drain(buf, sems_x)
        gather_drain(h_buf, sems_h)
        lax.fori_loop(0, STEPS, drain, 0)
    with jax.named_scope('red'):
        wait_all(n, rows_of, parts.at[me], fsend, frecv)
    own = whole.at[pl.ds(pl.multiple_of(me * share, 8), share)]
    own[...] = jnp.sum(parts[...], axis=0)
    send_all(n, lambda to: own, own, gsend, grecv)
    with jax.named_scope('spread'):
        wait_all(n, lambda to: own, own, gsend, grecv)
    dw_ref[...] = whole[0:feats]
    dw2_ref[...] = whole[start:start + dw2_ref.shape[0]]
    loss_ref[...] = whole[start + extra - 8:start + extra]


def finish_kernel(loss_in, dw_in, dw2_in, loss_ref, dw_ref, dw2_ref):
    loss_ref[...] = loss_in[0:1, 0:1]
    dw_ref[...] = dw_in[...]
    dw2_ref[...] = dw2_in[...]


def train_step(x_rows, w_one, w2t, labels, mask, adj):
    rows, nodes = adj.shape
    n = nodes // rows
    feats, width = x_rows.shape[0], rows // TREES
    classes, hidden = w2t.shape
    units = n * TREES
    small = -(-classes // 8) * 8 + 8
    share = -(-(-(-feats // 8) * 8 + small) // (8 * n)) * 8
    vmem, hbm = pl.BlockSpec(memory_space=pltpu.VMEM), pl.BlockSpec(memory_space=pl.ANY)
    dma, f32, bf16 = pltpu.SemaphoreType.DMA, jnp.float32, jnp.bfloat16
    block = (TREES, hidden, width)
    loss, dw_one, dw_two = pl.pallas_call(
        functools.partial(step_kernel, n),
        name='step',
        out_shape=(jax.ShapeDtypeStruct((8, hidden), f32), jax.ShapeDtypeStruct((feats, hidden), f32), jax.ShapeDtypeStruct((classes, hidden), f32)),
        in_specs=[hbm, hbm, vmem, vmem, vmem, hbm],
        out_specs=(vmem,) * 3,
        scratch_shapes=[
            pltpu.VMEM((RING * 8, rows, width), bf16), pltpu.VMEM((units, feats, width), bf16), pltpu.VMEM((feats, rows), f32),
            pltpu.VMEM((units, hidden, width), bf16), pltpu.VMEM((feats, rows), bf16), pltpu.VMEM((hidden, rows), f32),
            pltpu.VMEM((hidden, rows), bf16), pltpu.VMEM((feats, hidden), f32), pltpu.VMEM((small, hidden), f32), pltpu.VMEM((n, 8, 128), f32),
            pltpu.VMEM((STEPS, *block), f32), pltpu.VMEM(block, f32), pltpu.VMEM((STEPS, *block), f32), pltpu.VMEM((STEPS - 1, *block), f32),
            pltpu.VMEM((n * share, hidden), f32), pltpu.VMEM((n, share, hidden), f32), pltpu.VMEM((n * share, hidden), f32),
            dma((RING, 8)), dma((TREES,)), dma, dma((n,)), dma((n,)), dma((STEPS, TREES)), dma((STEPS, TREES)), dma((STEPS, TREES)), dma((STEPS, TREES)),
            dma((n,)), dma((n,)), dma((n,)), dma((n,)), *gather_sems(), *gather_sems()],
        compiler_params=pltpu.CompilerParams(collective_id=0, has_side_effects=True, vmem_limit_bytes=67043328),
        cost_estimate=pl.CostEstimate(flops=2 * rows * nodes * (feats + 2 * hidden), bytes_accessed=6 * rows * nodes, transcendentals=0),
    )(x_rows, w_one, w2t, labels, mask, adj)
    return pl.pallas_call(
        finish_kernel,
        name='finish',
        out_shape=(jax.ShapeDtypeStruct((1, 1), f32), jax.ShapeDtypeStruct((feats, hidden), f32), jax.ShapeDtypeStruct((classes, hidden), f32)),
        in_specs=[vmem] * 3,
        out_specs=(vmem,) * 3,
    )(loss, dw_one, dw_two)


def solution(mesh):
    axis_name = AXIS

    def local_step(adj_rows, feat_rows, w_one, w_two, label_rows, mask_rows):
        rows = adj_rows.shape[0]
        loss, dw_one, dw_two = train_step(feat_rows.T, w_one, w_two.T, label_rows.reshape(1, rows), mask_rows.reshape(1, rows), adj_rows)
        return loss.reshape(1), dw_one, dw_two.T

    return jax.shard_map(local_step, mesh=mesh, in_specs=(P(axis_name, None), P(axis_name, None), P(None, None), P(None, None), P(axis_name), P(axis_name)), out_specs=(P(None), P(None, None), P(None, None)), check_vma=False)
```

```python
import functools

import jax
import jax.numpy as jnp
from jax import lax
from jax.experimental import pallas as pl
from jax.experimental.pallas import tpu as pltpu
from jax.sharding import PartitionSpec as P

MESH = pl.DeviceIdType.MESH
AXIS = 'nodes'
TREES = 4
RING = 4
STEPS = 8
COL_CONTRACT = (((1,), (1,)), ((), ()))
ROW_CONTRACT = (((0,), (0,)), ((), ()))


def tree_axis(tree, k, core, chip):
    if tree < 3:
        weight = 2 ** ((tree + k) % 3)
        return weight, lax.rem(chip // weight, 2)
    weight = (1 - core) * 2 ** k + core * 2 ** (2 - k)
    low, high = lax.rem(chip // 2 ** k, 2), lax.rem(chip // 2 ** (2 - k), 2)
    return weight, (1 - core) * low + core * high


def chip_at(tree, offset, core, chip):
    out = chip
    for k in range(3):
        weight, bit = tree_axis(tree, k, core, chip)
        out = out + lax.rem(offset // 2 ** k, 2) * weight * (1 - 2 * bit)
    return out


def unit_at(tree, offset, core, chip):
    return (chip_at(tree, offset, core, chip) * 2 + core) * TREES + tree


def neighbour(tree, k, core, chip):
    weight, bit = tree_axis(tree, k, core, chip)
    return (chip + weight * (1 - 2 * bit)) * 2 + core


def remote(src, dst, send_sem, recv_sem, device):
    return pltpu.make_async_remote_copy(src_ref=src, dst_ref=dst, send_sem=send_sem, recv_sem=recv_sem, device_id=(device,), device_id_type=MESH)


def place():
    me = lax.axis_index(AXIS)
    core, chip = lax.rem(me, 2), me // 2
    return me, core, chip, chip * 2 + 1 - core


def gather_send(buf, sems, tree, offset, k, unit):
    send, recv, hand = sems
    me, core, chip, partner = place()
    remote(buf.at[unit], buf.at[unit], send, recv.at[offset + 2 ** k, tree], neighbour(tree, k, core, chip)).start()


def gather_hand(buf, sems, offset, unit):
    send, recv, hand = sems
    me, core, chip, partner = place()
    remote(buf.at[unit], buf.at[unit], send, hand.at[offset], partner).start()


def gather_start(buf, sems, links):
    me = lax.axis_index(AXIS)
    for k in range(links):
        for t in range(TREES):
            gather_send(buf, sems, t, 0, k, me * TREES + t)
        if k == 0:
            for t in range(TREES):
                gather_hand(buf, sems, 0, me * TREES + t)


def gather_arrive(buf, sems, s, links):
    send, recv, hand = sems
    me, core, chip, partner = place()
    units = [unit_at(t, s, core, chip) for t in range(TREES)]
    for t, u in enumerate(units):
        remote(buf.at[u], buf.at[u], send, recv.at[s, t], partner).wait_recv()

        @pl.when(s == 1)
        def _():
            gather_send(buf, sems, t, s, 1, u)

        @pl.when((s > 1) & (s < 4))
        def _():
            gather_send(buf, sems, t, s, 2, u)
        gather_hand(buf, sems, s, u)

    @pl.when(s == 1)
    def _():
        if links < 3:
            for t in range(TREES):
                gather_send(buf, sems, t, 0, 2, me * TREES + t)
        for t, u in enumerate(units):
            gather_send(buf, sems, t, s, 2, u)


def gather_take(buf, sems, s):
    send, recv, hand = sems
    me, core, chip, partner = place()
    four = buf.at[pl.ds(0, TREES)]
    remote(four, four, send, hand.at[s], partner).wait_recv()


def gather_drain(buf, sems):
    send, recv, hand = sems
    me, core, chip, partner = place()
    sent = buf.at[pl.ds(0, TREES * (STEPS - 1 + STEPS))]
    remote(sent, sent, send, hand.at[0], partner).wait_send()


def gather_sems():
    dma = pltpu.SemaphoreType.DMA
    return [dma, dma((STEPS, TREES)), dma((STEPS,))]


def barrier_near():
    me, core, chip, partner = place()
    sem = pltpu.get_barrier_semaphore()
    pl.semaphore_signal(sem, inc=1, device_id=(partner,), device_id_type=MESH)
    for k in range(3):
        pl.semaphore_signal(sem, inc=1, device_id=(neighbour(0, k, core, chip),), device_id_type=MESH)
    pl.semaphore_wait(sem, 4)


def send_all(n, src, dst, send_sem, recv_sem):
    me = lax.axis_index(AXIS)
    for i in range(1, n):
        to = lax.rem(me + i, n)
        remote(src(to), dst, send_sem, recv_sem, to).start()


def wait_all(ref, send_sem, recv_sem):
    me, core, chip, partner = place()
    copy = remote(ref, ref, send_sem, recv_sem, partner)
    copy.wait_send()
    copy.wait_recv()


def step_kernel(n, x_ref, w_hbm, w2t_ref, y_ref, m_ref, adj, loss_ref, dw_ref, dw2_ref,
                ring, buf, acc, h_buf, s_one, z_one, u_two, w_v, small, count, stage, mine, total, child, part, parts, whole,
                ring_sem, x_sem, w_sem, count_send, count_recv, dsend, drecv, csend, crecv, fsend, frecv, gsend, grecv, *sems):
    me, core, chip, partner = place()
    sems_x, sems_h = sems[:3], sems[3:]
    width = buf.shape[2]
    feats, rows = acc.shape
    hidden = h_buf.shape[1]
    chunks = [slice(t * width, (t + 1) * width) for t in range(TREES)]

    def slab(s, slot, j):
        u = unit_at(j % TREES, s, core if j < TREES else 1 - core, chip)
        return pltpu.make_async_copy(adj.at[:, pl.ds(pl.multiple_of(u * width, width), width)], ring.at[slot * 8 + j], ring_sem.at[slot, j // TREES])

    def load(s, slot, half):
        for t in range(TREES):
            slab(s, slot, half * TREES + t).start()

    def loaded(slot, half):
        four = ring.at[pl.ds(0, TREES)]
        pltpu.make_async_copy(four, four, ring_sem.at[slot, half]).wait()

    with jax.named_scope('start'):
        fetch = [pltpu.make_async_copy(x_ref.at[:, pl.ds(t * width, width)], buf.at[me * TREES + t], x_sem) for t in range(TREES)]
        for copy in fetch:
            copy.start()
        weight = m_ref[...].astype(jnp.float32)
        count[me] = jnp.broadcast_to(jnp.sum(weight, axis=1, keepdims=True), count.shape[1:])
        barrier_near()
        four = buf.at[pl.ds(0, TREES)]
        pltpu.make_async_copy(four, four, x_sem).wait()
    gather_start(buf, sems_x, 2)
    weights = pltpu.make_async_copy(w_hbm, w_v, w_sem)
    weights.start()
    for s in range(RING):
        for half in range(2):
            load(s, s, half)
    acc[...] = jnp.zeros_like(acc)

    def terms(units_ref, s, half):
        slot = lax.rem(s, RING)
        loaded(slot, half)
        which = core if half == 0 else 1 - core
        return [(units_ref, unit_at(t, s, which, chip), slot * 8 + half * TREES + t) for t in range(TREES)]

    def aggregate(out, pairs):
        for cols in chunks:
            out[:, cols] += sum(lax.dot_general(ref[u], ring[j, cols], COL_CONTRACT, preferred_element_type=jnp.float32) for ref, u, j in pairs)

    def step_one(s, carry):
        with jax.named_scope('arrive'):
            @pl.when(s > 0)
            def _():
                gather_arrive(buf, sems_x, s, 2)
        for half in range(2):
            with jax.named_scope('consume'):
                if half == 1:
                    gather_take(buf, sems_x, s)
                aggregate(acc, terms(buf, s, half))
                load(lax.rem(s + RING, STEPS), lax.rem(s, RING), half)
        return carry

    lax.fori_loop(0, STEPS, step_one, 0)
    with jax.named_scope('mid'):
        weights.wait()
        s_one[...] = acc[...].astype(jnp.bfloat16)
        w_rows = w_v[...].astype(jnp.bfloat16)
        for t, cols in enumerate(chunks):
            z = lax.dot_general(w_rows, s_one[:, cols], ROW_CONTRACT, preferred_element_type=jnp.float32)
            z_one[:, cols] = z
            h_buf[me * TREES + t] = jnp.maximum(z, 0.0).astype(jnp.bfloat16)
    gather_start(h_buf, sems_h, 3)
    send_all(n, lambda to: count.at[me], count.at[me], count_send, count_recv)
    two = acc.at[0:hidden]

    def load_two(s, half):
        late = s // RING
        load((1 - late) * (s + RING) + late * (STEPS + RING - 1 - s), lax.rem(s, RING), half)

    two[...] = jnp.zeros_like(two)
    with jax.named_scope('consume'):
        aggregate(two, terms(h_buf, 0, 0))
        load_two(0, 0)

    def step_two(s, carry):
        with jax.named_scope('arrive'):
            gather_arrive(h_buf, sems_h, s, 3)
            gather_take(h_buf, sems_h, s - 1)
        with jax.named_scope('consume'):
            aggregate(two, terms(h_buf, s - 1, 1) + terms(h_buf, s, 0))
            load_two(s - 1, 1)
            load_two(s, 0)
        return carry

    lax.fori_loop(1, STEPS, step_two, 0)
    with jax.named_scope('last'):
        gather_take(h_buf, sems_h, STEPS - 1)
        aggregate(two, terms(h_buf, STEPS - 1, 1))
        load_two(STEPS - 1, 1)
    with jax.named_scope('soft'):
        wait_all(count.at[pl.ds(0, n - 1)], count_send, count_recv)
        labelled = jnp.sum(count[...], axis=0)[0:1, 0:1]
        s_two = two[...].astype(jnp.bfloat16)
        w_two = w2t_ref[...].astype(jnp.bfloat16)
        logits = jnp.dot(w_two, s_two, preferred_element_type=jnp.float32)
        shifted = logits - jnp.max(logits, axis=0, keepdims=True)
        log_prob = shifted - jnp.log(jnp.sum(jnp.exp(shifted), axis=0, keepdims=True))
        hot = lax.broadcasted_iota(jnp.int32, logits.shape, 0) == y_ref[...]
        grad = (weight * (jnp.exp(log_prob) - hot.astype(jnp.float32)) / labelled).astype(jnp.bfloat16)
        u_two[...] = lax.dot_general(w_two, grad, ROW_CONTRACT, preferred_element_type=jnp.float32).astype(jnp.bfloat16)
        loss = -jnp.sum(weight * jnp.sum(jnp.where(hot, log_prob, 0.0), axis=0, keepdims=True), axis=1, keepdims=True)
        classes = logits.shape[0]
        edge = small.shape[0] - 8
        small[0:classes] = lax.dot_general(grad, s_two, COL_CONTRACT, preferred_element_type=jnp.float32)
        small[classes:edge] = jnp.zeros((edge - classes, hidden), jnp.float32)
        small[edge:] = jnp.broadcast_to(loss / labelled, (8, hidden))

    def to_partner(s, t):
        return remote(stage.at[s, t], total.at[s, t], dsend, drecv.at[s], partner)

    def to_parent(s, t, k):
        return remote(total.at[s, t], child.at[s - 1, t], csend, crecv.at[s, t], neighbour(t, k, core, chip))

    def step_back(i, carry):
        s = STEPS - 1 - i
        slot = lax.rem(i, RING)
        with jax.named_scope('give'):
            loaded(slot, 1)
            for t in range(TREES):
                stage[s, t] = jnp.dot(u_two[...], ring[slot * 8 + TREES + t], preferred_element_type=jnp.float32)
            for t in range(TREES):
                to_partner(s, t).start()
            loaded(slot, 0)
            for t in range(TREES):
                mine[t] = jnp.dot(u_two[...], ring[slot * 8 + t], preferred_element_type=jnp.float32)

            @pl.when(i + RING < STEPS)
            def _():
                load(s - RING, slot, 1)
                load(s - RING, slot, 0)
        with jax.named_scope('take'):
            remote(total.at[s], total.at[s], dsend, drecv.at[s], partner).wait_recv()
            for t in range(TREES):
                total[s, t] = total[s, t] + mine[t]
                for k in range(3):
                    @pl.when(s < 2 ** k)
                    def _():
                        to_parent(s + 2 ** k, t, k).wait_recv()
                        total[s, t] = total[s, t] + child[s + 2 ** k - 1, t]
                for k in range(3):
                    @pl.when((s >= 2 ** k) & (s < 2 ** (k + 1)))
                    def _():
                        to_parent(s, t, k).start()
        return carry

    lax.fori_loop(0, STEPS, step_back, 0)
    start = -(-feats // 8) * 8
    extra = small.shape[0]
    with jax.named_scope('dw'):
        grads = [jnp.where(z_one[:, cols] > 0.0, total[0, t], 0.0).astype(jnp.bfloat16) for t, cols in enumerate(chunks)]
        part[0:feats] = lax.dot_general(s_one[...], jnp.concatenate(grads, axis=1), COL_CONTRACT, preferred_element_type=jnp.float32)
        part[feats:start] = jnp.zeros((start - feats, part.shape[1]), jnp.float32)
        part[start:start + extra] = small[...]
        part[start + extra:] = jnp.zeros_like(part[start + extra:])
    share = part.shape[0] // n

    def rows_of(to):
        return part.at[pl.ds(pl.multiple_of(to * share, 8), share)]

    send_all(n, rows_of, parts.at[me], fsend, frecv)
    parts[me] = part[pl.ds(pl.multiple_of(me * share, 8), share)]

    with jax.named_scope('drain'):
        gather_drain(buf, sems_x)
        gather_drain(h_buf, sems_h)
        remote(stage, stage, dsend, drecv.at[0], partner).wait_send()
        remote(child, child, csend, crecv.at[0, 0], partner).wait_send()
    with jax.named_scope('red'):
        wait_all(parts.at[pl.ds(0, n - 1)], fsend, frecv)
    own = whole.at[pl.ds(pl.multiple_of(me * share, 8), share)]
    own[...] = jnp.sum(parts[...], axis=0)
    send_all(n, lambda to: own, own, gsend, grecv)
    with jax.named_scope('spread'):
        wait_all(whole.at[pl.ds(0, (n - 1) * share)], gsend, grecv)
    dw_ref[...] = whole[0:feats]
    dw2_ref[...] = whole[start:start + dw2_ref.shape[0]]
    loss_ref[...] = whole[start + extra - 8:start + extra]


def finish_kernel(loss_in, dw_in, dw2_in, loss_ref, dw_ref, dw2_ref):
    loss_ref[...] = loss_in[0:1, 0:1]
    dw_ref[...] = dw_in[...]
    dw2_ref[...] = dw2_in[...]


def train_step(x_rows, w_one, w2t, labels, mask, adj):
    rows, nodes = adj.shape
    n = nodes // rows
    feats, width = x_rows.shape[0], rows // TREES
    classes, hidden = w2t.shape
    units = n * TREES
    small = -(-classes // 8) * 8 + 8
    share = -(-(-(-feats // 8) * 8 + small) // (8 * n)) * 8
    vmem, hbm = pl.BlockSpec(memory_space=pltpu.VMEM), pl.BlockSpec(memory_space=pl.ANY)
    dma, f32, bf16 = pltpu.SemaphoreType.DMA, jnp.float32, jnp.bfloat16
    block = (TREES, hidden, width)
    loss, dw_one, dw_two = pl.pallas_call(
        functools.partial(step_kernel, n),
        name='step',
        out_shape=(jax.ShapeDtypeStruct((8, hidden), f32), jax.ShapeDtypeStruct((feats, hidden), f32), jax.ShapeDtypeStruct((classes, hidden), f32)),
        in_specs=[hbm, hbm, vmem, vmem, vmem, hbm],
        out_specs=(vmem,) * 3,
        scratch_shapes=[
            pltpu.VMEM((RING * 8, rows, width), bf16), pltpu.VMEM((units, feats, width), bf16), pltpu.VMEM((feats, rows), f32),
            pltpu.VMEM((units, hidden, width), bf16), pltpu.VMEM((feats, rows), bf16), pltpu.VMEM((hidden, rows), f32),
            pltpu.VMEM((hidden, rows), bf16), pltpu.VMEM((feats, hidden), f32), pltpu.VMEM((small, hidden), f32), pltpu.VMEM((n, 8, 128), f32),
            pltpu.VMEM((STEPS, *block), f32), pltpu.VMEM(block, f32), pltpu.VMEM((STEPS, *block), f32), pltpu.VMEM((STEPS - 1, *block), f32),
            pltpu.VMEM((n * share, hidden), f32), pltpu.VMEM((n, share, hidden), f32), pltpu.VMEM((n * share, hidden), f32),
            dma((RING, 2)), dma, dma, dma, dma, dma, dma((STEPS,)), dma, dma((STEPS, TREES)), dma, dma, dma, dma, *gather_sems(), *gather_sems()],
        compiler_params=pltpu.CompilerParams(collective_id=0, has_side_effects=True, vmem_limit_bytes=67043328),
        cost_estimate=pl.CostEstimate(flops=2 * rows * nodes * (feats + 2 * hidden), bytes_accessed=6 * rows * nodes, transcendentals=0),
    )(x_rows, w_one, w2t, labels, mask, adj)
    return pl.pallas_call(
        finish_kernel,
        name='finish',
        out_shape=(jax.ShapeDtypeStruct((1, 1), f32), jax.ShapeDtypeStruct((feats, hidden), f32), jax.ShapeDtypeStruct((classes, hidden), f32)),
        in_specs=[vmem] * 3,
        out_specs=(vmem,) * 3,
    )(loss, dw_one, dw_two)


def solution(mesh):
    axis_name = AXIS

    def local_step(adj_rows, feat_rows, w_one, w_two, label_rows, mask_rows):
        rows = adj_rows.shape[0]
        loss, dw_one, dw_two = train_step(feat_rows.T, w_one, w_two.T, label_rows.reshape(1, rows), mask_rows.reshape(1, rows), adj_rows)
        return loss.reshape(1), dw_one, dw_two.T

    return jax.shard_map(local_step, mesh=mesh, in_specs=(P(axis_name, None), P(axis_name, None), P(None, None), P(None, None), P(axis_name), P(axis_name)), out_specs=(P(None), P(None, None), P(None, None)), check_vma=False)
```

```python
import functools

import jax
import jax.numpy as jnp
from jax import lax
from jax.experimental import pallas as pl
from jax.experimental.pallas import tpu as pltpu
from jax.sharding import PartitionSpec as P

MESH = pl.DeviceIdType.MESH
AXIS = 'nodes'
TREES = 4
RING = 4
STEPS = 8
COL_CONTRACT = (((1,), (1,)), ((), ()))
ROW_CONTRACT = (((0,), (0,)), ((), ()))


def tree_axis(tree, k, core, chip):
    if tree < 3:
        weight = 2 ** ((tree + k) % 3)
        return weight, lax.rem(chip // weight, 2)
    weight = (1 - core) * 2 ** k + core * 2 ** (2 - k)
    low, high = lax.rem(chip // 2 ** k, 2), lax.rem(chip // 2 ** (2 - k), 2)
    return weight, (1 - core) * low + core * high


def chip_at(tree, offset, core, chip):
    out = chip
    for k in range(3):
        weight, bit = tree_axis(tree, k, core, chip)
        out = out + lax.rem(offset // 2 ** k, 2) * weight * (1 - 2 * bit)
    return out


def early_order(place):
    pair = (place + 1) // 2
    return place + (pair * (4 - pair)) // 4 * (7 - 2 * place)


def unit_at(tree, offset, core, chip):
    return (chip_at(tree, offset, core, chip) * 2 + core) * TREES + tree


def neighbour(tree, k, core, chip):
    weight, bit = tree_axis(tree, k, core, chip)
    return (chip + weight * (1 - 2 * bit)) * 2 + core


def remote(src, dst, send_sem, recv_sem, device):
    return pltpu.make_async_remote_copy(src_ref=src, dst_ref=dst, send_sem=send_sem, recv_sem=recv_sem, device_id=(device,), device_id_type=MESH)


def place():
    me = lax.axis_index(AXIS)
    core, chip = lax.rem(me, 2), me // 2
    return me, core, chip, chip * 2 + 1 - core


def gather_send(buf, sems, tree, offset, k, unit):
    send, recv, hand = sems
    me, core, chip, partner = place()
    remote(buf.at[unit], buf.at[unit], send, recv.at[offset + 2 ** k, tree], neighbour(tree, k, core, chip)).start()


def gather_hand(buf, sems, offset, unit):
    send, recv, hand = sems
    me, core, chip, partner = place()
    remote(buf.at[unit], buf.at[unit], send, hand.at[offset], partner).start()


def gather_start(buf, sems, links):
    me = lax.axis_index(AXIS)
    for k in range(links):
        for t in range(TREES):
            gather_send(buf, sems, t, 0, k, me * TREES + t)
        if k == 0:
            for t in range(TREES):
                gather_hand(buf, sems, 0, me * TREES + t)


def gather_arrive(buf, sems, s, links):
    send, recv, hand = sems
    me, core, chip, partner = place()
    units = [unit_at(t, s, core, chip) for t in range(TREES)]
    for t, u in enumerate(units):
        remote(buf.at[u], buf.at[u], send, recv.at[s, t], partner).wait_recv()

        @pl.when(s == 1)
        def _():
            gather_send(buf, sems, t, s, 1, u)

        @pl.when((s > 1) & (s < 4))
        def _():
            gather_send(buf, sems, t, s, 2, u)
        gather_hand(buf, sems, s, u)

    @pl.when(s == 1)
    def _():
        if links < 3:
            for t in range(TREES):
                gather_send(buf, sems, t, 0, 2, me * TREES + t)
        for t, u in enumerate(units):
            gather_send(buf, sems, t, s, 2, u)


def gather_take(buf, sems, s):
    send, recv, hand = sems
    me, core, chip, partner = place()
    four = buf.at[pl.ds(0, TREES)]
    remote(four, four, send, hand.at[s], partner).wait_recv()


def gather_drain(buf, sems):
    send, recv, hand = sems
    me, core, chip, partner = place()
    sent = buf.at[pl.ds(0, TREES * (STEPS - 1 + STEPS))]
    remote(sent, sent, send, hand.at[0], partner).wait_send()


def gather_sems():
    dma = pltpu.SemaphoreType.DMA
    return [dma, dma((STEPS, TREES)), dma((STEPS,))]


def barrier_near():
    me, core, chip, partner = place()
    sem = pltpu.get_barrier_semaphore()
    pl.semaphore_signal(sem, inc=1, device_id=(partner,), device_id_type=MESH)
    for k in range(3):
        pl.semaphore_signal(sem, inc=1, device_id=(neighbour(0, k, core, chip),), device_id_type=MESH)
    pl.semaphore_wait(sem, 4)


def send_all(n, src, dst, send_sem, recv_sem):
    me = lax.axis_index(AXIS)
    for i in range(1, n):
        to = lax.rem(me + i, n)
        remote(src(to), dst, send_sem, recv_sem, to).start()


def wait_all(ref, send_sem, recv_sem):
    me, core, chip, partner = place()
    copy = remote(ref, ref, send_sem, recv_sem, partner)
    copy.wait_send()
    copy.wait_recv()


def step_kernel(n, x_ref, w_hbm, w2t_ref, y_ref, m_ref, adj, loss_ref, dw_ref, dw2_ref,
                ring, buf, acc, h_buf, s_one, z_one, u_two, w_v, small, count, stage, mine, total, child, part, parts, whole,
                small_parts, small_whole, pair,
                ring_sem, x_sem, w_sem, count_send, count_recv, dsend, drecv, csend, crecv, fsend, frecv, gsend, grecv,
                ssend, srecv, bsend, brecv, psend, precv, qsend, qrecv, *sems):
    me, core, chip, partner = place()
    sems_x, sems_h = sems[:3], sems[3:]
    width = buf.shape[2]
    feats, rows = acc.shape
    hidden = h_buf.shape[1]
    chunks = [slice(t * width, (t + 1) * width) for t in range(TREES)]

    def slab(s, slot, j):
        u = unit_at(j % TREES, s, core if j < TREES else 1 - core, chip)
        return pltpu.make_async_copy(adj.at[:, pl.ds(pl.multiple_of(u * width, width), width)], ring.at[slot * 8 + j], ring_sem.at[slot, j // TREES])

    def load(s, slot, half):
        for t in range(TREES):
            slab(s, slot, half * TREES + t).start()

    def loaded(slot, half):
        four = ring.at[pl.ds(0, TREES)]
        pltpu.make_async_copy(four, four, ring_sem.at[slot, half]).wait()

    with jax.named_scope('start'):
        fetch = [pltpu.make_async_copy(x_ref.at[:, pl.ds(t * width, width)], buf.at[me * TREES + t], x_sem) for t in range(TREES)]
        for copy in fetch:
            copy.start()
        weight = m_ref[...].astype(jnp.float32)
        count[me] = jnp.broadcast_to(jnp.sum(weight, axis=1, keepdims=True), count.shape[1:])
        barrier_near()
        four = buf.at[pl.ds(0, TREES)]
        pltpu.make_async_copy(four, four, x_sem).wait()
    gather_start(buf, sems_x, 2)
    weights = pltpu.make_async_copy(w_hbm, w_v, w_sem)
    weights.start()
    for s in range(RING):
        for half in range(2):
            load(s, s, half)
    acc[...] = jnp.zeros_like(acc)

    def terms(units_ref, s, slot, half):
        loaded(slot, half)
        which = core if half == 0 else 1 - core
        return [(units_ref, unit_at(t, s, which, chip), slot * 8 + half * TREES + t) for t in range(TREES)]

    def aggregate(out, pairs):
        for cols in chunks:
            out[:, cols] += sum(lax.dot_general(ref[u], ring[j, cols], COL_CONTRACT, preferred_element_type=jnp.float32) for ref, u, j in pairs)

    def step_one(s, carry):
        with jax.named_scope('arrive'):
            @pl.when(s > 0)
            def _():
                gather_arrive(buf, sems_x, s, 2)
        for half in range(2):
            with jax.named_scope('consume'):
                if half == 1:
                    gather_take(buf, sems_x, s)
                slot = lax.rem(s, RING)
                aggregate(acc, terms(buf, s, slot, half))
                late = s // RING
                load((1 - late) * (s + RING) + late * early_order(s - late * RING), slot, half)
        return carry

    lax.fori_loop(0, STEPS, step_one, 0)
    with jax.named_scope('mid'):
        weights.wait()
        s_one[...] = acc[...].astype(jnp.bfloat16)
        w_rows = w_v[...].astype(jnp.bfloat16)
        for t, cols in enumerate(chunks):
            z = lax.dot_general(w_rows, s_one[:, cols], ROW_CONTRACT, preferred_element_type=jnp.float32)
            z_one[:, cols] = z
            h_buf[me * TREES + t] = jnp.maximum(z, 0.0).astype(jnp.bfloat16)
    gather_start(h_buf, sems_h, 3)
    send_all(n, lambda to: count.at[me], count.at[me], count_send, count_recv)
    two = acc.at[0:hidden]

    def take_two(p, half):
        return terms(h_buf, early_order(p), lax.rem(p, RING), half)

    def load_two(p, half):
        late = p // RING
        load((1 - late) * early_order(p + RING - late * RING) + late * (STEPS + RING - 1 - p), lax.rem(p, RING), half)

    two[...] = jnp.zeros_like(two)
    with jax.named_scope('consume'):
        aggregate(two, take_two(0, 0))
        load_two(0, 0)
        gather_take(h_buf, sems_h, 0)
        aggregate(two, take_two(0, 1))
        load_two(0, 1)
    with jax.named_scope('arrive'):
        gather_arrive(h_buf, sems_h, 1, 3)
    with jax.named_scope('consume'):
        aggregate(two, take_two(1, 0))
        load_two(1, 0)

    def step_two(p, carry):
        with jax.named_scope('arrive'):
            gather_arrive(h_buf, sems_h, early_order(p), 3)
            gather_take(h_buf, sems_h, early_order(p - 1))
        with jax.named_scope('consume'):
            aggregate(two, take_two(p - 1, 1) + take_two(p, 0))
            load_two(p - 1, 1)
            load_two(p, 0)
        return carry

    lax.fori_loop(2, STEPS, step_two, 0)
    with jax.named_scope('last'):
        gather_take(h_buf, sems_h, STEPS - 1)
        aggregate(two, take_two(STEPS - 1, 1))
        load_two(STEPS - 1, 1)
    with jax.named_scope('soft'):
        wait_all(count.at[pl.ds(0, n - 1)], count_send, count_recv)
        labelled = jnp.sum(count[...], axis=0)[0:1, 0:1]
        s_two = two[...].astype(jnp.bfloat16)
        w_two = w2t_ref[...].astype(jnp.bfloat16)
        logits = jnp.dot(w_two, s_two, preferred_element_type=jnp.float32)
        shifted = logits - jnp.max(logits, axis=0, keepdims=True)
        log_prob = shifted - jnp.log(jnp.sum(jnp.exp(shifted), axis=0, keepdims=True))
        hot = lax.broadcasted_iota(jnp.int32, logits.shape, 0) == y_ref[...]
        grad = (weight * (jnp.exp(log_prob) - hot.astype(jnp.float32)) / labelled).astype(jnp.bfloat16)
        u_two[...] = lax.dot_general(w_two, grad, ROW_CONTRACT, preferred_element_type=jnp.float32).astype(jnp.bfloat16)
        loss = -jnp.sum(weight * jnp.sum(jnp.where(hot, log_prob, 0.0), axis=0, keepdims=True), axis=1, keepdims=True)
        classes = logits.shape[0]
        edge = small.shape[0] - 8
        small[0:classes] = lax.dot_general(grad, s_two, COL_CONTRACT, preferred_element_type=jnp.float32)
        small[classes:edge] = jnp.zeros((edge - classes, hidden), jnp.float32)
        small[edge:] = jnp.broadcast_to(loss / labelled, (8, hidden))
        owners = small.shape[0] // 8
        tile = pl.ds(pl.multiple_of(me * 8, 8), 8)
        for o in range(owners):
            @pl.when(me != o)
            def _():
                remote(small.at[pl.ds(o * 8, 8)], small_parts.at[me], ssend, srecv, o).start()

    def to_partner(s, t):
        return remote(stage.at[s, t], total.at[s, t], dsend, drecv.at[s], partner)

    def to_parent(s, t, k):
        return remote(total.at[s, t], child.at[s - 1, t], csend, crecv.at[s, t], neighbour(t, k, core, chip))

    def reduce_small():
        @pl.when(me < owners)
        def _():
            small_parts[me] = small[tile]
            got = small_parts.at[pl.ds(0, n - 1)]
            remote(got, got, ssend, srecv, partner).wait_recv()
            small_whole[tile] = jnp.sum(small_parts[...], axis=0)
            for i in range(1, n):
                remote(small_whole.at[tile], small_whole.at[tile], bsend, brecv, lax.rem(me + i, n)).start()

    def finish_small():
        sent = small_parts.at[pl.ds(0, n - 1)]
        fewer, every = small_whole.at[pl.ds(0, owners * 8 - 8)], small_whole.at[pl.ds(0, owners * 8)]

        @pl.when(me < owners)
        def _():
            remote(sent, sent, bsend, brecv, partner).wait_send()
            remote(fewer, fewer, ssend, brecv, partner).wait_send()
            remote(fewer, fewer, ssend, brecv, partner).wait_recv()

        @pl.when(me >= owners)
        def _():
            remote(every, every, ssend, brecv, partner).wait_send()
            remote(every, every, ssend, brecv, partner).wait_recv()

    def step_back(i, carry):
        @pl.when(i == STEPS - 3)
        def _():
            reduce_small()

        s = STEPS - 1 - i
        slot = lax.rem(i, RING)
        with jax.named_scope('give'):
            loaded(slot, 1)
            for t in range(TREES):
                stage[s, t] = jnp.dot(u_two[...], ring[slot * 8 + TREES + t], preferred_element_type=jnp.float32)
            for t in range(TREES):
                to_partner(s, t).start()
            loaded(slot, 0)
            for t in range(TREES):
                mine[t] = jnp.dot(u_two[...], ring[slot * 8 + t], preferred_element_type=jnp.float32)

            @pl.when(i + RING < STEPS)
            def _():
                load(s - RING, slot, 1)
                load(s - RING, slot, 0)
        with jax.named_scope('take'):
            remote(total.at[s], total.at[s], dsend, drecv.at[s], partner).wait_recv()
            for t in range(TREES):
                total[s, t] = total[s, t] + mine[t]
                for k in range(3):
                    @pl.when(s < 2 ** k)
                    def _():
                        to_parent(s + 2 ** k, t, k).wait_recv()
                        total[s, t] = total[s, t] + child[s + 2 ** k - 1, t]
                for k in range(3):
                    @pl.when((s >= 2 ** k) & (s < 2 ** (k + 1)))
                    def _():
                        to_parent(s, t, k).start()
        return carry

    lax.fori_loop(0, STEPS, step_back, 0)
    chips = n // 2
    half, share = part.shape[0] // 2, part.shape[0] // n
    mine_rows = pl.ds(pl.multiple_of(core * half, 8), half)
    their_rows = pl.ds(pl.multiple_of((1 - core) * half, 8), half)
    with jax.named_scope('dw'):
        grads = [jnp.where(z_one[:, cols] > 0.0, total[0, t], 0.0).astype(jnp.bfloat16) for t, cols in enumerate(chunks)]
        part[0:feats] = lax.dot_general(s_one[...], jnp.concatenate(grads, axis=1), COL_CONTRACT, preferred_element_type=jnp.float32)
        part[feats:] = jnp.zeros_like(part[feats:])
    over = remote(part.at[their_rows], pair, psend, precv, partner)
    over.start()
    with jax.named_scope('drain'):
        gather_drain(buf, sems_x)
        gather_drain(h_buf, sems_h)
        remote(stage, stage, dsend, drecv.at[0], partner).wait_send()
        remote(child, child, csend, crecv.at[0, 0], partner).wait_send()
        finish_small()
    with jax.named_scope('pair'):
        over.wait()
        pair[...] = pair[...] + part[mine_rows]

    def share_of(q):
        return pl.ds(pl.multiple_of(q * share, 8), share)

    for i in range(1, chips):
        to = lax.rem(chip + i, chips)
        remote(pair.at[share_of(to)], parts.at[chip], fsend, frecv, to * 2 + core).start()
    parts[chip] = pair[share_of(chip)]
    with jax.named_scope('red'):
        wait_all(parts.at[pl.ds(0, chips - 1)], fsend, frecv)
    own = whole.at[pl.ds(pl.multiple_of(core * half + chip * share, 8), share)]
    own[...] = jnp.sum(parts[...], axis=0)
    for i in range(1, chips):
        remote(own, own, gsend, grecv, lax.rem(chip + i, chips) * 2 + core).start()
    with jax.named_scope('spread'):
        wait_all(whole.at[pl.ds(0, (chips - 1) * share)], gsend, grecv)
    swap = remote(whole.at[mine_rows], whole.at[mine_rows], qsend, qrecv, partner)
    swap.start()
    dw2_ref[...] = small_whole[0:dw2_ref.shape[0]]
    loss_ref[...] = small_whole[edge:edge + 8]
    with jax.named_scope('swap'):
        swap.wait()
    dw_ref[...] = whole[0:feats]


def finish_kernel(loss_in, dw_in, dw2_in, loss_ref, dw_ref, dw2_ref):
    loss_ref[...] = loss_in[0:1, 0:1]
    dw_ref[...] = dw_in[...]
    dw2_ref[...] = dw2_in[...]


def train_step(x_rows, w_one, w2t, labels, mask, adj):
    rows, nodes = adj.shape
    n = nodes // rows
    feats, width = x_rows.shape[0], rows // TREES
    classes, hidden = w2t.shape
    units = n * TREES
    small = -(-classes // 8) * 8 + 8
    share = -(-feats // (8 * n)) * 8
    vmem, hbm = pl.BlockSpec(memory_space=pltpu.VMEM), pl.BlockSpec(memory_space=pl.ANY)
    dma, f32, bf16 = pltpu.SemaphoreType.DMA, jnp.float32, jnp.bfloat16
    block = (TREES, hidden, width)
    loss, dw_one, dw_two = pl.pallas_call(
        functools.partial(step_kernel, n),
        name='step',
        out_shape=(pltpu.VMEM((8, hidden), f32), pltpu.VMEM((feats, hidden), f32), pltpu.VMEM((classes, hidden), f32)),
        in_specs=[hbm, hbm, vmem, vmem, vmem, hbm],
        out_specs=(vmem,) * 3,
        scratch_shapes=[
            pltpu.VMEM((RING * 8, rows, width), bf16), pltpu.VMEM((units, feats, width), bf16), pltpu.VMEM((feats, rows), f32),
            pltpu.VMEM((units, hidden, width), bf16), pltpu.VMEM((feats, rows), bf16), pltpu.VMEM((hidden, rows), f32),
            pltpu.VMEM((hidden, rows), bf16), pltpu.VMEM((feats, hidden), f32), pltpu.VMEM((small, hidden), f32), pltpu.VMEM((n, 8, 128), f32),
            pltpu.VMEM((STEPS, *block), f32), pltpu.VMEM(block, f32), pltpu.VMEM((STEPS, *block), f32), pltpu.VMEM((STEPS - 1, *block), f32),
            pltpu.VMEM((n * share, hidden), f32), pltpu.VMEM((n // 2, share, hidden), f32), pltpu.VMEM((n * share, hidden), f32),
            pltpu.VMEM((n, 8, hidden), f32), pltpu.VMEM((small, hidden), f32), pltpu.VMEM((n // 2 * share, hidden), f32),
            dma((RING, 2)), dma, dma, dma, dma, dma, dma((STEPS,)), dma, dma((STEPS, TREES)), *[dma] * 12, *gather_sems(), *gather_sems()],
        compiler_params=pltpu.CompilerParams(collective_id=0, has_side_effects=True, vmem_limit_bytes=62000000),
        cost_estimate=pl.CostEstimate(flops=2 * rows * nodes * (feats + 2 * hidden), bytes_accessed=6 * rows * nodes, transcendentals=0),
    )(x_rows, w_one, w2t, labels, mask, adj)
    return pl.pallas_call(
        finish_kernel,
        name='finish',
        out_shape=(jax.ShapeDtypeStruct((1, 1), f32), jax.ShapeDtypeStruct((feats, hidden), f32), jax.ShapeDtypeStruct((classes, hidden), f32)),
        in_specs=[vmem] * 3,
        out_specs=(vmem,) * 3,
    )(*[pltpu.with_memory_space_constraint(x, pltpu.VMEM) for x in (loss, dw_one, dw_two)])


def solution(mesh):
    axis_name = AXIS

    def local_step(adj_rows, feat_rows, w_one, w_two, label_rows, mask_rows):
        rows = adj_rows.shape[0]
        loss, dw_one, dw_two = train_step(feat_rows.T, w_one, w_two.T, label_rows.reshape(1, rows), mask_rows.reshape(1, rows), adj_rows)
        return loss.reshape(1), dw_one, dw_two.T

    return jax.shard_map(local_step, mesh=mesh, in_specs=(P(axis_name, None), P(axis_name, None), P(None, None), P(None, None), P(axis_name), P(axis_name)), out_specs=(P(None), P(None, None), P(None, None)), check_vma=False)
```

```python
import functools

import jax
import jax.numpy as jnp
from jax import lax
from jax.experimental import pallas as pl
from jax.experimental.pallas import tpu as pltpu
from jax.sharding import PartitionSpec as P

MESH = pl.DeviceIdType.MESH
AXIS = 'nodes'
TREES = 4
RING = 4
STEPS = 8
COL_CONTRACT = (((1,), (1,)), ((), ()))
ROW_CONTRACT = (((0,), (0,)), ((), ()))


def tree_axis(tree, k, core, chip):
    if tree < 3:
        weight = 2 ** ((tree + k) % 3)
        return weight, lax.rem(chip // weight, 2)
    weight = (1 - core) * 2 ** k + core * 2 ** (2 - k)
    low, high = lax.rem(chip // 2 ** k, 2), lax.rem(chip // 2 ** (2 - k), 2)
    return weight, (1 - core) * low + core * high


def chip_at(tree, offset, core, chip):
    out = chip
    for k in range(3):
        weight, bit = tree_axis(tree, k, core, chip)
        out = out + lax.rem(offset // 2 ** k, 2) * weight * (1 - 2 * bit)
    return out


def early_order(place):
    pair = (place + 1) // 2
    return place + (pair * (4 - pair)) // 4 * (7 - 2 * place)


def unit_at(tree, offset, core, chip):
    return (chip_at(tree, offset, core, chip) * 2 + core) * TREES + tree


def neighbour(tree, k, core, chip):
    weight, bit = tree_axis(tree, k, core, chip)
    return (chip + weight * (1 - 2 * bit)) * 2 + core


def remote(src, dst, send_sem, recv_sem, device):
    return pltpu.make_async_remote_copy(src_ref=src, dst_ref=dst, send_sem=send_sem, recv_sem=recv_sem, device_id=(device,), device_id_type=MESH)


def place():
    me = lax.axis_index(AXIS)
    core, chip = lax.rem(me, 2), me // 2
    return me, core, chip, chip * 2 + 1 - core


def gather_send(buf, sems, tree, offset, k, unit, rows=slice(None)):
    send, recv, hand = sems
    me, core, chip, partner = place()
    ref = buf.at[unit, rows]
    remote(ref, ref, send, recv.at[offset + 2 ** k - 1, tree], neighbour(tree, k, core, chip)).start()


def gather_hand(buf, sems, slot, unit):
    send, recv, hand = sems
    me, core, chip, partner = place()
    remote(buf.at[unit], buf.at[unit], send, hand.at[slot], partner).start()


def gather_start(buf, sems, links):
    me = lax.axis_index(AXIS)
    for k in range(links):
        for t in range(TREES):
            gather_send(buf, sems, t, 0, k, me * TREES + t)
        if k == 0:
            for t in range(TREES):
                gather_hand(buf, sems, 0, me * TREES + t)


def gather_arrive(buf, sems, s, links, trees=range(TREES), slot=None, cut=None):
    send, recv, hand = sems
    me, core, chip, partner = place()
    units = {t: unit_at(t, s, core, chip) for t in trees}
    for t, u in units.items():
        remote(buf.at[u], buf.at[u], send, recv.at[s - 1, t], partner).wait_recv()
        split = cut is not None and t == TREES - 1

        @pl.when(s == 1)
        def _():
            gather_send(buf, sems, t, s, 1, u)

        @pl.when((s > 1) & (s < (3 if split else 4)))
        def _():
            gather_send(buf, sems, t, s, 2, u)
        if split:
            @pl.when(s == 3)
            def _():
                gather_send(buf, sems, t, s, 2, u, slice(0, cut))

            @pl.when(s == 5)
            def _():
                gather_send(buf, sems, t, s, 1, u, slice(cut, None))
        gather_hand(buf, sems, s if slot is None else slot, u)

    @pl.when(s == 1)
    def _():
        if links < 3:
            for t in range(TREES):
                gather_send(buf, sems, t, 0, 2, me * TREES + t)
        for t, u in units.items():
            gather_send(buf, sems, t, s, 2, u)


def gather_take(buf, sems, slot, count=TREES):
    send, recv, hand = sems
    me, core, chip, partner = place()
    units = buf.at[pl.ds(0, count)]
    remote(units, units, send, hand.at[slot], partner).wait_recv()


def gather_drain(buf, sems):
    send, recv, hand = sems
    me, core, chip, partner = place()
    sent = buf.at[pl.ds(0, TREES * (STEPS - 1 + STEPS))]
    remote(sent, sent, send, hand.at[0], partner).wait_send()


def gather_sems():
    dma = pltpu.SemaphoreType.DMA
    return [dma, dma((STEPS - 1, TREES)), dma((STEPS + 1,))]


def barrier_near():
    me, core, chip, partner = place()
    sem = pltpu.get_barrier_semaphore()
    pl.semaphore_signal(sem, inc=1, device_id=(partner,), device_id_type=MESH)
    for k in range(3):
        pl.semaphore_signal(sem, inc=1, device_id=(neighbour(0, k, core, chip),), device_id_type=MESH)
    pl.semaphore_wait(sem, 4)


def send_all(n, src, dst, send_sem, recv_sem):
    me = lax.axis_index(AXIS)
    for i in range(1, n):
        to = lax.rem(me + i, n)
        remote(src(to), dst, send_sem, recv_sem, to).start()


def wait_all(ref, send_sem, recv_sem):
    me, core, chip, partner = place()
    copy = remote(ref, ref, send_sem, recv_sem, partner)
    copy.wait_send()
    copy.wait_recv()


def step_kernel(n, x_ref, w_hbm, w2t_ref, y_ref, m_ref, adj, loss_ref, dw_ref, dw2_ref,
                ring, buf, acc, h_buf, s_one, z_one, u_two, w_v, small, count, stage, mine, total, child, part, parts, whole,
                small_parts, small_whole, pair,
                ring_sem, x_sem, w_sem, count_send, count_recv, dsend, drecv, csend, crecv, fsend, frecv, gsend, grecv,
                ssend, srecv, bsend, brecv, psend, precv, qsend, qrecv, *sems):
    me, core, chip, partner = place()
    sems_x, sems_h = sems[:3], sems[3:]
    width = buf.shape[2]
    feats, rows = acc.shape
    hidden = h_buf.shape[1]
    chunks = [slice(t * width, (t + 1) * width) for t in range(TREES)]

    def slab(s, slot, j):
        u = unit_at(j % TREES, s, core if j < TREES else 1 - core, chip)
        return pltpu.make_async_copy(adj.at[:, pl.ds(pl.multiple_of(u * width, width), width)], ring.at[slot * 8 + j], ring_sem.at[slot, j // TREES])

    def load(s, slot, half):
        for t in range(TREES):
            slab(s, slot, half * TREES + t).start()

    def loaded(slot, half):
        four = ring.at[pl.ds(0, TREES)]
        pltpu.make_async_copy(four, four, ring_sem.at[slot, half]).wait()

    with jax.named_scope('start'):
        fetch = [pltpu.make_async_copy(x_ref.at[:, pl.ds(t * width, width)], buf.at[me * TREES + t], x_sem) for t in range(TREES)]
        for copy in fetch:
            copy.start()
        weight = m_ref[...].astype(jnp.float32)
        count[me] = jnp.broadcast_to(jnp.sum(weight, axis=1, keepdims=True), count.shape[1:])
        barrier_near()
        four = buf.at[pl.ds(0, TREES)]
        pltpu.make_async_copy(four, four, x_sem).wait()
    gather_start(buf, sems_x, 2)
    weights = pltpu.make_async_copy(w_hbm, w_v, w_sem)
    weights.start()
    for s in range(RING):
        for half in range(2):
            load(s, s, half)
    acc[...] = jnp.zeros_like(acc)

    def terms(units_ref, s, slot, half, trees=range(TREES)):
        which = core if half == 0 else 1 - core
        return [(units_ref, unit_at(t, s, which, chip), slot * 8 + half * TREES + t) for t in trees]

    def aggregate(out, pairs):
        for cols in chunks:
            out[:, cols] += sum(lax.dot_general(ref[u], ring[j, cols], COL_CONTRACT, preferred_element_type=jnp.float32) for ref, u, j in pairs)

    def step_one(s, carry):
        with jax.named_scope('arrive'):
            @pl.when(s > 0)
            def _():
                gather_arrive(buf, sems_x, s, 2, cut=cut)
        for half in range(2):
            with jax.named_scope('consume'):
                if half == 1:
                    gather_take(buf, sems_x, s)
                slot = lax.rem(s, RING)
                loaded(slot, half)
                aggregate(acc, terms(buf, s, slot, half))
                late = s // RING
                load((1 - late) * (s + RING) + late * early_order(s - late * RING), slot, half)
        return carry

    cut = feats * 2 // 3 // 16 * 16
    final, slot = STEPS - 1, (STEPS - 1) % RING
    lax.fori_loop(0, final, step_one, 0)
    for trees, hand in ((range(TREES - 1), final), (range(TREES - 1, TREES), STEPS)):
        with jax.named_scope('arrive'):
            gather_arrive(buf, sems_x, final, 2, trees, hand, cut)
        for half in range(2):
            with jax.named_scope('consume'):
                if half == 1:
                    gather_take(buf, sems_x, hand, len(trees))
                if hand == final:
                    loaded(slot, half)
                aggregate(acc, terms(buf, final, slot, half, trees))
    for half in range(2):
        load(early_order(final - RING), slot, half)
    with jax.named_scope('mid'):
        weights.wait()
        s_one[...] = acc[...].astype(jnp.bfloat16)
        w_rows = w_v[...].astype(jnp.bfloat16)
        for t, cols in enumerate(chunks):
            z = lax.dot_general(w_rows, s_one[:, cols], ROW_CONTRACT, preferred_element_type=jnp.float32)
            z_one[:, cols] = z
            h_buf[me * TREES + t] = jnp.maximum(z, 0.0).astype(jnp.bfloat16)
    gather_start(h_buf, sems_h, 3)
    send_all(n, lambda to: count.at[me], count.at[me], count_send, count_recv)
    two = acc.at[0:hidden]

    def take_two(p, half):
        loaded(lax.rem(p, RING), half)
        return terms(h_buf, early_order(p), lax.rem(p, RING), half)

    def back_order(i):
        return early_order(STEPS - 1 - i)

    def load_two(p, half):
        late = p // RING
        load((1 - late) * early_order(p + RING - late * RING) + late * back_order(p - late * RING), lax.rem(p, RING), half)

    two[...] = jnp.zeros_like(two)
    with jax.named_scope('consume'):
        aggregate(two, take_two(0, 0))
        load_two(0, 0)
        gather_take(h_buf, sems_h, 0)
        aggregate(two, take_two(0, 1))
        load_two(0, 1)
    with jax.named_scope('arrive'):
        gather_arrive(h_buf, sems_h, 1, 3)
    with jax.named_scope('consume'):
        aggregate(two, take_two(1, 0))
        load_two(1, 0)

    def step_two(p, carry):
        with jax.named_scope('arrive'):
            gather_arrive(h_buf, sems_h, early_order(p), 3)
            gather_take(h_buf, sems_h, early_order(p - 1))
        with jax.named_scope('consume'):
            aggregate(two, take_two(p - 1, 1) + take_two(p, 0))
            load_two(p - 1, 1)
            load_two(p, 0)
        return carry

    lax.fori_loop(2, STEPS, step_two, 0)
    with jax.named_scope('last'):
        gather_take(h_buf, sems_h, STEPS - 1)
        aggregate(two, take_two(STEPS - 1, 1))
        load_two(STEPS - 1, 1)
    with jax.named_scope('soft'):
        wait_all(count.at[pl.ds(0, n - 1)], count_send, count_recv)
        labelled = jnp.sum(count[...], axis=0)[0:1, 0:1]
        s_two = two[...].astype(jnp.bfloat16)
        w_two = w2t_ref[...].astype(jnp.bfloat16)
        logits = jnp.dot(w_two, s_two, preferred_element_type=jnp.float32)
        shifted = logits - jnp.max(logits, axis=0, keepdims=True)
        log_prob = shifted - jnp.log(jnp.sum(jnp.exp(shifted), axis=0, keepdims=True))
        hot = lax.broadcasted_iota(jnp.int32, logits.shape, 0) == y_ref[...]
        grad = (weight * (jnp.exp(log_prob) - hot.astype(jnp.float32)) / labelled).astype(jnp.bfloat16)
        u_two[...] = lax.dot_general(w_two, grad, ROW_CONTRACT, preferred_element_type=jnp.float32).astype(jnp.bfloat16)
        loss = -jnp.sum(weight * jnp.sum(jnp.where(hot, log_prob, 0.0), axis=0, keepdims=True), axis=1, keepdims=True)
        classes = logits.shape[0]
        edge = small.shape[0] - 8
        small[0:classes] = lax.dot_general(grad, s_two, COL_CONTRACT, preferred_element_type=jnp.float32)
        small[classes:edge] = jnp.zeros((edge - classes, hidden), jnp.float32)
        small[edge:] = jnp.broadcast_to(loss / labelled, (8, hidden))
        owners = small.shape[0] // 8
        tile = pl.ds(pl.multiple_of(me * 8, 8), 8)
        for o in range(owners):
            @pl.when(me != o)
            def _():
                remote(small.at[pl.ds(o * 8, 8)], small_parts.at[me], ssend, srecv, o).start()

    def to_partner(s, t):
        return remote(stage.at[s, t], total.at[s, t], dsend, drecv.at[s], partner)

    def to_parent(s, t, k):
        return remote(total.at[s, t], child.at[s - 1, t], csend, crecv.at[s - 1, t], neighbour(t, k, core, chip))

    def reduce_small():
        @pl.when(me < owners)
        def _():
            small_parts[me] = small[tile]
            got = small_parts.at[pl.ds(0, n - 1)]
            remote(got, got, ssend, srecv, partner).wait_recv()
            small_whole[tile] = jnp.sum(small_parts[...], axis=0)
            for i in range(1, n):
                remote(small_whole.at[tile], small_whole.at[tile], bsend, brecv, lax.rem(me + i, n)).start()

    def finish_small():
        sent = small_parts.at[pl.ds(0, n - 1)]
        fewer, every = small_whole.at[pl.ds(0, owners * 8 - 8)], small_whole.at[pl.ds(0, owners * 8)]

        @pl.when(me < owners)
        def _():
            remote(sent, sent, bsend, brecv, partner).wait_send()
            remote(fewer, fewer, ssend, brecv, partner).wait_send()
            remote(fewer, fewer, ssend, brecv, partner).wait_recv()

        @pl.when(me >= owners)
        def _():
            remote(every, every, ssend, brecv, partner).wait_send()
            remote(every, every, ssend, brecv, partner).wait_recv()

    def step_back(i, carry):
        s = back_order(i)
        slot = lax.rem(i, RING)
        with jax.named_scope('give'):
            loaded(slot, 1)
            for t in range(TREES):
                stage[s, t] = jnp.dot(u_two[...], ring[slot * 8 + TREES + t], preferred_element_type=jnp.float32)
            for t in range(TREES):
                to_partner(s, t).start()
            loaded(slot, 0)
            for t in range(TREES):
                mine[t] = jnp.dot(u_two[...], ring[slot * 8 + t], preferred_element_type=jnp.float32)

            @pl.when(i + RING < STEPS)
            def _():
                load(back_order(i + RING), slot, 1)
                load(back_order(i + RING), slot, 0)
        with jax.named_scope('take'):
            remote(total.at[s], total.at[s], dsend, drecv.at[s], partner).wait_recv()
            for t in range(TREES):
                total[s, t] = total[s, t] + mine[t]
                for k in range(3):
                    @pl.when(s < 2 ** k)
                    def _():
                        to_parent(s + 2 ** k, t, k).wait_recv()
                        total[s, t] = total[s, t] + child[s + 2 ** k - 1, t]
                for k in range(3):
                    @pl.when((s >= 2 ** k) & (s < 2 ** (k + 1)))
                    def _():
                        to_parent(s, t, k).start()
        return carry

    lax.fori_loop(0, STEPS, step_back, 0)
    reduce_small()
    chips = n // 2
    half, share = part.shape[0] // 2, part.shape[0] // n
    mine_rows = pl.ds(pl.multiple_of(core * half, 8), half)
    their_rows = pl.ds(pl.multiple_of((1 - core) * half, 8), half)
    with jax.named_scope('dw'):
        grads = [jnp.where(z_one[:, cols] > 0.0, total[0, t], 0.0).astype(jnp.bfloat16) for t, cols in enumerate(chunks)]
        part[0:feats] = lax.dot_general(s_one[...], jnp.concatenate(grads, axis=1), COL_CONTRACT, preferred_element_type=jnp.float32)
        part[feats:] = jnp.zeros_like(part[feats:])
    over = remote(part.at[their_rows], pair, psend, precv, partner)
    over.start()
    with jax.named_scope('drain'):
        gather_drain(buf, sems_x)
        gather_drain(h_buf, sems_h)
        remote(stage, stage, dsend, drecv.at[0], partner).wait_send()
        remote(child, child, csend, crecv.at[0, 0], partner).wait_send()
        finish_small()
    with jax.named_scope('pair'):
        over.wait()
        pair[...] = pair[...] + part[mine_rows]

    def share_of(q):
        return pl.ds(pl.multiple_of(q * share, 8), share)

    for i in range(1, chips):
        to = lax.rem(chip + i, chips)
        remote(pair.at[share_of(to)], parts.at[chip], fsend, frecv, to * 2 + core).start()
    parts[chip] = pair[share_of(chip)]
    with jax.named_scope('red'):
        wait_all(parts.at[pl.ds(0, chips - 1)], fsend, frecv)
    own = whole.at[pl.ds(pl.multiple_of(core * half + chip * share, 8), share)]
    own[...] = jnp.sum(parts[...], axis=0)
    for i in range(1, chips):
        remote(own, own, gsend, grecv, lax.rem(chip + i, chips) * 2 + core).start()
    with jax.named_scope('spread'):
        wait_all(whole.at[pl.ds(0, (chips - 1) * share)], gsend, grecv)
    swap = remote(whole.at[mine_rows], whole.at[mine_rows], qsend, qrecv, partner)
    swap.start()
    dw2_ref[...] = small_whole[0:dw2_ref.shape[0]]
    loss_ref[...] = small_whole[edge:edge + 8]
    with jax.named_scope('swap'):
        swap.wait()
    dw_ref[...] = whole[0:feats]


def finish_kernel(loss_in, dw_in, dw2_in, loss_ref, dw_ref, dw2_ref):
    loss_ref[...] = loss_in[0:1, 0:1]
    dw_ref[...] = dw_in[...]
    dw2_ref[...] = dw2_in[...]


def train_step(x_rows, w_one, w2t, labels, mask, adj):
    rows, nodes = adj.shape
    n = nodes // rows
    feats, width = x_rows.shape[0], rows // TREES
    classes, hidden = w2t.shape
    units = n * TREES
    small = -(-classes // 8) * 8 + 8
    share = -(-feats // (8 * n)) * 8
    vmem, hbm = pl.BlockSpec(memory_space=pltpu.VMEM), pl.BlockSpec(memory_space=pl.ANY)
    dma, f32, bf16 = pltpu.SemaphoreType.DMA, jnp.float32, jnp.bfloat16
    block = (TREES, hidden, width)
    loss, dw_one, dw_two = pl.pallas_call(
        functools.partial(step_kernel, n),
        name='step',
        out_shape=(pltpu.VMEM((8, hidden), f32), pltpu.VMEM((feats, hidden), f32), pltpu.VMEM((classes, hidden), f32)),
        in_specs=[hbm, hbm, vmem, vmem, vmem, hbm],
        out_specs=(vmem,) * 3,
        scratch_shapes=[
            pltpu.VMEM((RING * 8, rows, width), bf16), pltpu.VMEM((units, feats, width), bf16), pltpu.VMEM((feats, rows), f32),
            pltpu.VMEM((units, hidden, width), bf16), pltpu.VMEM((feats, rows), bf16), pltpu.VMEM((hidden, rows), f32),
            pltpu.VMEM((hidden, rows), bf16), pltpu.VMEM((feats, hidden), f32), pltpu.VMEM((small, hidden), f32), pltpu.VMEM((n, 8, 128), f32),
            pltpu.VMEM((STEPS, *block), f32), pltpu.VMEM(block, f32), pltpu.VMEM((STEPS, *block), f32), pltpu.VMEM((STEPS - 1, *block), f32),
            pltpu.VMEM((n * share, hidden), f32), pltpu.VMEM((n // 2, share, hidden), f32), pltpu.VMEM((n * share, hidden), f32),
            pltpu.VMEM((n, 8, hidden), f32), pltpu.VMEM((small, hidden), f32), pltpu.VMEM((n // 2 * share, hidden), f32),
            dma((RING, 2)), dma, dma, dma, dma, dma, dma((STEPS,)), dma, dma((STEPS - 1, TREES)), *[dma] * 12, *gather_sems(), *gather_sems()],
        compiler_params=pltpu.CompilerParams(collective_id=0, has_side_effects=True, vmem_limit_bytes=62000000),
        cost_estimate=pl.CostEstimate(flops=2 * rows * nodes * (feats + 2 * hidden), bytes_accessed=6 * rows * nodes, transcendentals=0),
    )(x_rows, w_one, w2t, labels, mask, adj)
    return pl.pallas_call(
        finish_kernel,
        name='finish',
        out_shape=(jax.ShapeDtypeStruct((1, 1), f32), jax.ShapeDtypeStruct((feats, hidden), f32), jax.ShapeDtypeStruct((classes, hidden), f32)),
        in_specs=[vmem] * 3,
        out_specs=(vmem,) * 3,
    )(*[pltpu.with_memory_space_constraint(x, pltpu.VMEM) for x in (loss, dw_one, dw_two)])


def solution(mesh):
    axis_name = AXIS

    def local_step(adj_rows, feat_rows, w_one, w_two, label_rows, mask_rows):
        rows = adj_rows.shape[0]
        loss, dw_one, dw_two = train_step(feat_rows.T, w_one, w_two.T, label_rows.reshape(1, rows), mask_rows.reshape(1, rows), adj_rows)
        return loss.reshape(1), dw_one, dw_two.T

    return jax.shard_map(local_step, mesh=mesh, in_specs=(P(axis_name, None), P(axis_name, None), P(None, None), P(None, None), P(axis_name), P(axis_name)), out_specs=(P(None), P(None, None), P(None, None)), check_vma=False)
```

```python
import functools

import jax
import jax.numpy as jnp
from jax import lax
from jax.experimental import pallas as pl
from jax.experimental.pallas import tpu as pltpu
from jax.sharding import PartitionSpec as P

MESH = pl.DeviceIdType.MESH
AXIS = 'nodes'
TREES = 4
RING = 4
STEPS = 8
COL_CONTRACT = (((1,), (1,)), ((), ()))
ROW_CONTRACT = (((0,), (0,)), ((), ()))


def tree_axis(tree, k, core, chip):
    if tree < 3:
        weight = 2 ** ((tree + k) % 3)
        return weight, lax.rem(chip // weight, 2)
    weight = (1 - core) * 2 ** k + core * 2 ** (2 - k)
    low, high = lax.rem(chip // 2 ** k, 2), lax.rem(chip // 2 ** (2 - k), 2)
    return weight, (1 - core) * low + core * high


def chip_at(tree, offset, core, chip):
    out = chip
    for k in range(3):
        weight, bit = tree_axis(tree, k, core, chip)
        out = out + lax.rem(offset // 2 ** k, 2) * weight * (1 - 2 * bit)
    return out


def early_order(place):
    pair = (place + 1) // 2
    return place + (pair * (4 - pair)) // 4 * (7 - 2 * place)


def unit_at(tree, offset, core, chip):
    return (chip_at(tree, offset, core, chip) * 2 + core) * TREES + tree


def neighbour(tree, k, core, chip):
    weight, bit = tree_axis(tree, k, core, chip)
    return (chip + weight * (1 - 2 * bit)) * 2 + core


def remote(src, dst, send_sem, recv_sem, device):
    return pltpu.make_async_remote_copy(src_ref=src, dst_ref=dst, send_sem=send_sem, recv_sem=recv_sem, device_id=(device,), device_id_type=MESH)


def place():
    me = lax.axis_index(AXIS)
    core, chip = lax.rem(me, 2), me // 2
    return me, core, chip, chip * 2 + 1 - core


def gather_send(buf, sems, tree, offset, k, unit, rows=slice(None)):
    send, recv, hand = sems
    me, core, chip, partner = place()
    ref = buf.at[unit, rows]
    remote(ref, ref, send, recv.at[offset + 2 ** k - 1, tree], neighbour(tree, k, core, chip)).start()


def gather_hand(buf, sems, slot, unit):
    send, recv, hand = sems
    me, core, chip, partner = place()
    remote(buf.at[unit], buf.at[unit], send, hand.at[slot], partner).start()


def gather_start(buf, sems, links):
    me = lax.axis_index(AXIS)
    for k in range(links):
        for t in range(TREES):
            gather_send(buf, sems, t, 0, k, me * TREES + t)
        if k == 0:
            for t in range(TREES):
                gather_hand(buf, sems, 0, me * TREES + t)


def gather_arrive(buf, sems, s, links, trees=range(TREES), slot=None, cut=None):
    send, recv, hand = sems
    me, core, chip, partner = place()
    units = {t: unit_at(t, s, core, chip) for t in trees}
    for t, u in units.items():
        remote(buf.at[u], buf.at[u], send, recv.at[s - 1, t], partner).wait_recv()
        split = cut is not None and t == TREES - 1

        @pl.when(s == 1)
        def _():
            gather_send(buf, sems, t, s, 1, u)

        @pl.when((s > 1) & (s < (3 if split else 4)))
        def _():
            gather_send(buf, sems, t, s, 2, u)
        if split:
            @pl.when(s == 3)
            def _():
                gather_send(buf, sems, t, s, 2, u, slice(0, cut))

            @pl.when(s == 5)
            def _():
                gather_send(buf, sems, t, s, 1, u, slice(cut, None))
        gather_hand(buf, sems, s if slot is None else slot, u)

    @pl.when(s == 1)
    def _():
        if links < 3:
            for t in range(TREES):
                gather_send(buf, sems, t, 0, 2, me * TREES + t)
        for t, u in units.items():
            gather_send(buf, sems, t, s, 2, u)


def gather_take(buf, sems, slot, count=TREES):
    send, recv, hand = sems
    me, core, chip, partner = place()
    units = buf.at[pl.ds(0, count)]
    remote(units, units, send, hand.at[slot], partner).wait_recv()


def gather_drain(buf, sems):
    send, recv, hand = sems
    me, core, chip, partner = place()
    sent = buf.at[pl.ds(0, TREES * (STEPS - 1 + STEPS))]
    remote(sent, sent, send, hand.at[0], partner).wait_send()


def gather_sems():
    dma = pltpu.SemaphoreType.DMA
    return [dma, dma((STEPS - 1, TREES)), dma((STEPS + 1,))]


def barrier_near():
    me, core, chip, partner = place()
    sem = pltpu.get_barrier_semaphore()
    pl.semaphore_signal(sem, inc=1, device_id=(partner,), device_id_type=MESH)
    for k in range(3):
        pl.semaphore_signal(sem, inc=1, device_id=(neighbour(0, k, core, chip),), device_id_type=MESH)
    pl.semaphore_wait(sem, 4)


def send_all(n, src, dst, send_sem, recv_sem):
    me = lax.axis_index(AXIS)
    for i in range(1, n):
        to = lax.rem(me + i, n)
        remote(src(to), dst, send_sem, recv_sem, to).start()


def wait_all(ref, send_sem, recv_sem):
    me, core, chip, partner = place()
    copy = remote(ref, ref, send_sem, recv_sem, partner)
    copy.wait_send()
    copy.wait_recv()


def step_kernel(n, x_ref, w_hbm, w2t_ref, y_ref, m_ref, adj, loss_ref, dw_ref, dw2_ref,
                ring, buf, acc, h_buf, s_one, z_one, u_two, w_v, small, count, stage, mine, total, child, part, parts, whole,
                small_parts, small_whole, pair,
                ring_sem, x_sem, w_sem, count_send, count_recv, dsend, drecv, csend, crecv, fsend, frecv, gsend, grecv,
                ssend, srecv, bsend, brecv, psend, precv, qsend, qrecv, *sems):
    me, core, chip, partner = place()
    sems_x, sems_h = sems[:3], sems[3:]
    width = buf.shape[2]
    feats, rows = acc.shape
    hidden = h_buf.shape[1]
    chunks = [slice(t * width, (t + 1) * width) for t in range(TREES)]

    def slab(s, slot, j):
        u = unit_at(j % TREES, s, core if j < TREES else 1 - core, chip)
        return pltpu.make_async_copy(adj.at[:, pl.ds(pl.multiple_of(u * width, width), width)], ring.at[slot * 8 + j], ring_sem.at[slot, j // TREES])

    def load(s, slot, half):
        for t in range(TREES):
            slab(s, slot, half * TREES + t).start()

    def loaded(slot, half):
        four = ring.at[pl.ds(0, TREES)]
        pltpu.make_async_copy(four, four, ring_sem.at[slot, half]).wait()

    with jax.named_scope('start'):
        fetch = [pltpu.make_async_copy(x_ref.at[:, pl.ds(t * width, width)], buf.at[me * TREES + t], x_sem) for t in range(TREES)]
        for copy in fetch:
            copy.start()
        weight = m_ref[...].astype(jnp.float32)
        count[me] = jnp.broadcast_to(jnp.sum(weight, axis=1, keepdims=True), count.shape[1:])
        barrier_near()
        four = buf.at[pl.ds(0, TREES)]
        pltpu.make_async_copy(four, four, x_sem).wait()
    gather_start(buf, sems_x, 2)
    weights = pltpu.make_async_copy(w_hbm, w_v, w_sem)
    weights.start()
    for s in range(RING):
        for half in range(2):
            load(s, s, half)
    acc[...] = jnp.zeros_like(acc)

    def terms(units_ref, s, slot, half, trees=range(TREES)):
        which = core if half == 0 else 1 - core
        return [(units_ref, unit_at(t, s, which, chip), slot * 8 + half * TREES + t) for t in trees]

    def aggregate(out, pairs):
        for cols in chunks:
            out[:, cols] += sum(lax.dot_general(ref[u], ring[j, cols], COL_CONTRACT, preferred_element_type=jnp.float32) for ref, u, j in pairs)

    def step_one(s, carry):
        with jax.named_scope('arrive'):
            @pl.when(s > 0)
            def _():
                gather_arrive(buf, sems_x, s, 2, cut=cut)
        for half in range(2):
            with jax.named_scope('consume'):
                if half == 1:
                    gather_take(buf, sems_x, s)
                slot = lax.rem(s, RING)
                loaded(slot, half)
                aggregate(acc, terms(buf, s, slot, half))
                late = s // RING
                load((1 - late) * (s + RING) + late * early_order(s - late * RING), slot, half)
        return carry

    cut = feats * 2 // 3 // 16 * 16
    final, slot = STEPS - 1, (STEPS - 1) % RING
    lax.fori_loop(0, final, step_one, 0)
    early, late = (range(TREES - 1), final), (range(TREES - 1, TREES), STEPS)
    for half in range(2):
        for trees, hand in (early, late):
            with jax.named_scope('consume'):
                if half == 0:
                    gather_arrive(buf, sems_x, final, 2, trees, hand, cut)
                else:
                    gather_take(buf, sems_x, hand, len(trees))
                if hand == final:
                    loaded(slot, half)
                aggregate(acc, terms(buf, final, slot, half, trees))
    for half in range(2):
        load(early_order(final - RING), slot, half)
    with jax.named_scope('mid'):
        weights.wait()
        s_one[0:feats] = acc[...].astype(jnp.bfloat16)
        s_one[feats:] = jnp.zeros_like(s_one[feats:])
        w_rows = w_v[...].astype(jnp.bfloat16)
        for t, cols in enumerate(chunks):
            z = lax.dot_general(w_rows, s_one[0:feats, cols], ROW_CONTRACT, preferred_element_type=jnp.float32)
            z_one[:, cols] = z
            h_buf[me * TREES + t] = jnp.maximum(z, 0.0).astype(jnp.bfloat16)
    gather_start(h_buf, sems_h, 3)
    send_all(n, lambda to: count.at[me], count.at[me], count_send, count_recv)
    two = acc.at[0:hidden]

    def take_two(p, half):
        loaded(lax.rem(p, RING), half)
        return terms(h_buf, early_order(p), lax.rem(p, RING), half)

    def back_order(i):
        return early_order(STEPS - 1 - i)

    def load_two(p, half):
        late = p // RING
        load((1 - late) * early_order(p + RING - late * RING) + late * back_order(p - late * RING), lax.rem(p, RING), half)

    two[...] = jnp.zeros_like(two)
    with jax.named_scope('consume'):
        aggregate(two, take_two(0, 0))
        load_two(0, 0)
        gather_take(h_buf, sems_h, 0)
        aggregate(two, take_two(0, 1))
        load_two(0, 1)
    with jax.named_scope('arrive'):
        gather_arrive(h_buf, sems_h, 1, 3)
    with jax.named_scope('consume'):
        aggregate(two, take_two(1, 0))
        load_two(1, 0)

    def step_two(p, carry):
        with jax.named_scope('arrive'):
            gather_arrive(h_buf, sems_h, early_order(p), 3)
            gather_take(h_buf, sems_h, early_order(p - 1))
        with jax.named_scope('consume'):
            aggregate(two, take_two(p - 1, 1) + take_two(p, 0))
            load_two(p - 1, 1)
            load_two(p, 0)
        return carry

    lax.fori_loop(2, STEPS, step_two, 0)
    with jax.named_scope('last'):
        gather_take(h_buf, sems_h, STEPS - 1)
        aggregate(two, take_two(STEPS - 1, 1))
        load_two(STEPS - 1, 1)
    with jax.named_scope('soft'):
        wait_all(count.at[pl.ds(0, n - 1)], count_send, count_recv)
        labelled = jnp.sum(count[...], axis=0)[0:1, 0:1]
        s_two = two[...].astype(jnp.bfloat16)
        w_two = w2t_ref[...].astype(jnp.bfloat16)
        logits = jnp.dot(w_two, s_two, preferred_element_type=jnp.float32)
        shifted = logits - jnp.max(logits, axis=0, keepdims=True)
        log_prob = shifted - jnp.log(jnp.sum(jnp.exp(shifted), axis=0, keepdims=True))
        hot = lax.broadcasted_iota(jnp.int32, logits.shape, 0) == y_ref[...]
        grad = (weight * (jnp.exp(log_prob) - hot.astype(jnp.float32)) / labelled).astype(jnp.bfloat16)
        u_two[...] = lax.dot_general(w_two, grad, ROW_CONTRACT, preferred_element_type=jnp.float32).astype(jnp.bfloat16)
        loss = -jnp.sum(weight * jnp.sum(jnp.where(hot, log_prob, 0.0), axis=0, keepdims=True), axis=1, keepdims=True)
        classes = logits.shape[0]
        edge = small.shape[0] - 8
        small[0:classes] = lax.dot_general(grad, s_two, COL_CONTRACT, preferred_element_type=jnp.float32)
        small[classes:edge] = jnp.zeros((edge - classes, hidden), jnp.float32)
        small[edge:] = jnp.broadcast_to(loss / labelled, (8, hidden))
        owners = small.shape[0] // 8
        tile = pl.ds(pl.multiple_of(me * 8, 8), 8)
        for o in range(owners):
            @pl.when(me != o)
            def _():
                remote(small.at[pl.ds(o * 8, 8)], small_parts.at[me], ssend, srecv, o).start()

    def to_partner(s, t):
        return remote(stage.at[s, t], total.at[s, t], dsend, drecv.at[s], partner)

    def to_parent(s, t, k):
        return remote(total.at[s, t], child.at[s - 1, t], csend, crecv.at[s - 1, t], neighbour(t, k, core, chip))

    def reduce_small():
        @pl.when(me < owners)
        def _():
            small_parts[me] = small[tile]
            got = small_parts.at[pl.ds(0, n - 1)]
            remote(got, got, ssend, srecv, partner).wait_recv()
            small_whole[tile] = jnp.sum(small_parts[...], axis=0)
            for i in range(1, n):
                remote(small_whole.at[tile], small_whole.at[tile], bsend, brecv, lax.rem(me + i, n)).start()

    def finish_small():
        sent = small_parts.at[pl.ds(0, n - 1)]
        fewer, every = small_whole.at[pl.ds(0, owners * 8 - 8)], small_whole.at[pl.ds(0, owners * 8)]

        @pl.when(me < owners)
        def _():
            remote(sent, sent, bsend, brecv, partner).wait_send()
            remote(fewer, fewer, ssend, brecv, partner).wait_send()
            remote(fewer, fewer, ssend, brecv, partner).wait_recv()

        @pl.when(me >= owners)
        def _():
            remote(every, every, ssend, brecv, partner).wait_send()
            remote(every, every, ssend, brecv, partner).wait_recv()

    def step_back(i, carry):
        s = back_order(i)
        slot = lax.rem(i, RING)
        with jax.named_scope('give'):
            loaded(slot, 1)
            for t in range(TREES):
                stage[s, t] = jnp.dot(u_two[...], ring[slot * 8 + TREES + t], preferred_element_type=jnp.float32)
            for t in range(TREES):
                to_partner(s, t).start()
            loaded(slot, 0)
            for t in range(TREES):
                mine[t] = jnp.dot(u_two[...], ring[slot * 8 + t], preferred_element_type=jnp.float32)

            @pl.when(i + RING < STEPS)
            def _():
                load(back_order(i + RING), slot, 1)
                load(back_order(i + RING), slot, 0)
        with jax.named_scope('take'):
            remote(total.at[s], total.at[s], dsend, drecv.at[s], partner).wait_recv()
            for t in range(TREES):
                total[s, t] = total[s, t] + mine[t]
                for k in range(3):
                    @pl.when(s < 2 ** k)
                    def _():
                        to_parent(s + 2 ** k, t, k).wait_recv()
                        total[s, t] = total[s, t] + child[s + 2 ** k - 1, t]
                for k in range(3):
                    @pl.when((s >= 2 ** k) & (s < 2 ** (k + 1)))
                    def _():
                        to_parent(s, t, k).start()
        return carry

    lax.fori_loop(0, STEPS, step_back, 0)
    reduce_small()
    chips = n // 2
    half, share = part.shape[0] // 2, part.shape[0] // n
    mine_rows = pl.ds(pl.multiple_of(core * half, 8), half)
    their_rows = pl.ds(pl.multiple_of((1 - core) * half, 8), half)
    with jax.named_scope('dw'):
        grads = [jnp.where(z_one[:, cols] > 0.0, total[0, t], 0.0).astype(jnp.bfloat16) for t, cols in enumerate(chunks)]
        grads = jnp.concatenate(grads, axis=1)
        part[their_rows] = lax.dot_general(s_one[their_rows], grads, COL_CONTRACT, preferred_element_type=jnp.float32)
        over = remote(part.at[their_rows], pair, psend, precv, partner)
        over.start()
        part[mine_rows] = lax.dot_general(s_one[mine_rows], grads, COL_CONTRACT, preferred_element_type=jnp.float32)
    with jax.named_scope('drain'):
        gather_drain(buf, sems_x)
        gather_drain(h_buf, sems_h)
        remote(stage, stage, dsend, drecv.at[0], partner).wait_send()
        remote(child, child, csend, crecv.at[0, 0], partner).wait_send()
    with jax.named_scope('pair'):
        over.wait()
        pair[...] = pair[...] + part[mine_rows]

    def share_of(q):
        return pl.ds(pl.multiple_of(q * share, 8), share)

    for i in range(1, chips):
        to = lax.rem(chip + i, chips)
        remote(pair.at[share_of(to)], parts.at[chip], fsend, frecv, to * 2 + core).start()
    parts[chip] = pair[share_of(chip)]
    with jax.named_scope('red'):
        wait_all(parts.at[pl.ds(0, chips - 1)], fsend, frecv)
    own = whole.at[pl.ds(pl.multiple_of(core * half + chip * share, 8), share)]
    own[...] = jnp.sum(parts[...], axis=0)
    for i in range(1, chips):
        remote(own, own, gsend, grecv, lax.rem(chip + i, chips) * 2 + core).start()
    with jax.named_scope('spread'):
        wait_all(whole.at[pl.ds(0, (chips - 1) * share)], gsend, grecv)
    swap = remote(whole.at[mine_rows], whole.at[mine_rows], qsend, qrecv, partner)
    swap.start()
    finish_small()
    dw2_ref[...] = small_whole[0:dw2_ref.shape[0]]
    loss_ref[...] = small_whole[edge:edge + 8]
    with jax.named_scope('swap'):
        swap.wait()
    dw_ref[...] = whole[0:feats]


def finish_kernel(loss_in, dw_in, dw2_in, loss_ref, dw_ref, dw2_ref):
    loss_ref[...] = loss_in[0:1, 0:1]
    dw_ref[...] = dw_in[...]
    dw2_ref[...] = dw2_in[...]


def train_step(x_rows, w_one, w2t, labels, mask, adj):
    rows, nodes = adj.shape
    n = nodes // rows
    feats, width = x_rows.shape[0], rows // TREES
    classes, hidden = w2t.shape
    units = n * TREES
    small = -(-classes // 8) * 8 + 8
    share = -(-feats // (8 * n)) * 8
    vmem, hbm = pl.BlockSpec(memory_space=pltpu.VMEM), pl.BlockSpec(memory_space=pl.ANY)
    dma, f32, bf16 = pltpu.SemaphoreType.DMA, jnp.float32, jnp.bfloat16
    block = (TREES, hidden, width)
    loss, dw_one, dw_two = pl.pallas_call(
        functools.partial(step_kernel, n),
        name='step',
        out_shape=(pltpu.VMEM((8, hidden), f32), pltpu.VMEM((feats, hidden), f32), pltpu.VMEM((classes, hidden), f32)),
        in_specs=[hbm, hbm, vmem, vmem, vmem, hbm],
        out_specs=(vmem,) * 3,
        scratch_shapes=[
            pltpu.VMEM((RING * 8, rows, width), bf16), pltpu.VMEM((units, feats, width), bf16), pltpu.VMEM((feats, rows), f32),
            pltpu.VMEM((units, hidden, width), bf16), pltpu.VMEM((n * share, rows), bf16), pltpu.VMEM((hidden, rows), f32),
            pltpu.VMEM((hidden, rows), bf16), pltpu.VMEM((feats, hidden), f32), pltpu.VMEM((small, hidden), f32), pltpu.VMEM((n, 8, 128), f32),
            pltpu.VMEM((STEPS, *block), f32), pltpu.VMEM(block, f32), pltpu.VMEM((STEPS, *block), f32), pltpu.VMEM((STEPS - 1, *block), f32),
            pltpu.VMEM((n * share, hidden), f32), pltpu.VMEM((n // 2, share, hidden), f32), pltpu.VMEM((n * share, hidden), f32),
            pltpu.VMEM((n, 8, hidden), f32), pltpu.VMEM((small, hidden), f32), pltpu.VMEM((n // 2 * share, hidden), f32),
            dma((RING, 2)), dma, dma, dma, dma, dma, dma((STEPS,)), dma, dma((STEPS - 1, TREES)), *[dma] * 12, *gather_sems(), *gather_sems()],
        compiler_params=pltpu.CompilerParams(collective_id=0, has_side_effects=True, vmem_limit_bytes=62000000),
        cost_estimate=pl.CostEstimate(flops=2 * rows * nodes * (feats + 2 * hidden), bytes_accessed=6 * rows * nodes, transcendentals=0),
    )(x_rows, w_one, w2t, labels, mask, adj)
    return pl.pallas_call(
        finish_kernel,
        name='finish',
        out_shape=(jax.ShapeDtypeStruct((1, 1), f32), jax.ShapeDtypeStruct((feats, hidden), f32), jax.ShapeDtypeStruct((classes, hidden), f32)),
        in_specs=[vmem] * 3,
        out_specs=(vmem,) * 3,
    )(*[pltpu.with_memory_space_constraint(x, pltpu.VMEM) for x in (loss, dw_one, dw_two)])


def solution(mesh):
    axis_name = AXIS

    def local_step(adj_rows, feat_rows, w_one, w_two, label_rows, mask_rows):
        rows = adj_rows.shape[0]
        loss, dw_one, dw_two = train_step(feat_rows.T, w_one, w_two.T, label_rows.reshape(1, rows), mask_rows.reshape(1, rows), adj_rows)
        return loss.reshape(1), dw_one, dw_two.T

    return jax.shard_map(local_step, mesh=mesh, in_specs=(P(axis_name, None), P(axis_name, None), P(None, None), P(None, None), P(axis_name), P(axis_name)), out_specs=(P(None), P(None, None), P(None, None)), check_vma=False)
```

```python
import functools

import jax
import jax.numpy as jnp
from jax import lax
from jax.experimental import pallas as pl
from jax.experimental.pallas import tpu as pltpu
from jax.sharding import PartitionSpec as P

MESH = pl.DeviceIdType.MESH
AXIS = 'nodes'
TREES = 4
EARLY = 2
RING = 4
STEPS = 8
COL_CONTRACT = (((1,), (1,)), ((), ()))
ROW_CONTRACT = (((0,), (0,)), ((), ()))


def tree_axis(tree, k, core, chip):
    if tree < 3:
        weight = 2 ** ((tree + k) % 3)
        return weight, lax.rem(chip // weight, 2)
    weight = (1 - core) * 2 ** k + core * 2 ** (2 - k)
    low, high = lax.rem(chip // 2 ** k, 2), lax.rem(chip // 2 ** (2 - k), 2)
    return weight, (1 - core) * low + core * high


def chip_at(tree, offset, core, chip):
    out = chip
    for k in range(3):
        weight, bit = tree_axis(tree, k, core, chip)
        out = out + lax.rem(offset // 2 ** k, 2) * weight * (1 - 2 * bit)
    return out


def early_order(place):
    pair = (place + 1) // 2
    return place + (pair * (4 - pair)) // 4 * (7 - 2 * place)


def unit_at(tree, offset, core, chip):
    return (chip_at(tree, offset, core, chip) * 2 + core) * TREES + tree


def neighbour(tree, k, core, chip):
    weight, bit = tree_axis(tree, k, core, chip)
    return (chip + weight * (1 - 2 * bit)) * 2 + core


def remote(src, dst, send_sem, recv_sem, device):
    return pltpu.make_async_remote_copy(src_ref=src, dst_ref=dst, send_sem=send_sem, recv_sem=recv_sem, device_id=(device,), device_id_type=MESH)


def place():
    me = lax.axis_index(AXIS)
    core, chip = lax.rem(me, 2), me // 2
    return me, core, chip, chip * 2 + 1 - core


def gather_send(buf, sems, tree, offset, k, unit, rows=slice(None)):
    send, recv, hand = sems
    me, core, chip, partner = place()
    ref = buf.at[unit, rows]
    remote(ref, ref, send, recv.at[offset + 2 ** k - 1, tree], neighbour(tree, k, core, chip)).start()


def gather_hand(buf, sems, slot, unit):
    send, recv, hand = sems
    me, core, chip, partner = place()
    remote(buf.at[unit], buf.at[unit], send, hand.at[slot], partner).start()


def gather_start(buf, sems, early):
    me = lax.axis_index(AXIS)
    for k in range(3):
        for t in range(TREES if k < 2 else early):
            gather_send(buf, sems, t, 0, k, me * TREES + t)
        if k == 0:
            for t in range(TREES):
                gather_hand(buf, sems, 0, me * TREES + t)


def gather_arrive(buf, sems, s, early, trees=range(TREES), slot=None, cut=None):
    send, recv, hand = sems
    me, core, chip, partner = place()
    units = {t: unit_at(t, s, core, chip) for t in trees}
    for t, u in units.items():
        remote(buf.at[u], buf.at[u], send, recv.at[s - 1, t], partner).wait_recv()
        split = cut is not None and t == TREES - 1

        @pl.when(s == 1)
        def _():
            gather_send(buf, sems, t, s, 1, u)

        @pl.when((s > 1) & (s < (3 if split else 4)))
        def _():
            gather_send(buf, sems, t, s, 2, u)
        if split:
            @pl.when(s == 3)
            def _():
                gather_send(buf, sems, t, s, 2, u, slice(0, cut))

            @pl.when(s == 5)
            def _():
                gather_send(buf, sems, t, s, 1, u, slice(cut, None))
        gather_hand(buf, sems, s if slot is None else slot, u)

    @pl.when(s == 1)
    def _():
        for t in range(early, TREES):
            gather_send(buf, sems, t, 0, 2, me * TREES + t)
        for t, u in units.items():
            gather_send(buf, sems, t, s, 2, u)


def gather_take(buf, sems, slot, count=TREES):
    send, recv, hand = sems
    me, core, chip, partner = place()
    units = buf.at[pl.ds(0, count)]
    remote(units, units, send, hand.at[slot], partner).wait_recv()


def gather_drain(buf, sems):
    send, recv, hand = sems
    me, core, chip, partner = place()
    sent = buf.at[pl.ds(0, TREES * (STEPS - 1 + STEPS))]
    remote(sent, sent, send, hand.at[0], partner).wait_send()


def gather_sems():
    dma = pltpu.SemaphoreType.DMA
    return [dma, dma((STEPS - 1, TREES)), dma((STEPS + 1,))]


def barrier_near():
    me, core, chip, partner = place()
    sem = pltpu.get_barrier_semaphore()
    pl.semaphore_signal(sem, inc=1, device_id=(partner,), device_id_type=MESH)
    for k in range(3):
        pl.semaphore_signal(sem, inc=1, device_id=(neighbour(0, k, core, chip),), device_id_type=MESH)
    pl.semaphore_wait(sem, 4)


def send_all(n, src, dst, send_sem, recv_sem):
    me = lax.axis_index(AXIS)
    for i in range(1, n):
        to = lax.rem(me + i, n)
        remote(src(to), dst, send_sem, recv_sem, to).start()


def wait_all(ref, send_sem, recv_sem):
    me, core, chip, partner = place()
    copy = remote(ref, ref, send_sem, recv_sem, partner)
    copy.wait_send()
    copy.wait_recv()


def step_kernel(n, x_ref, w_hbm, w2t_ref, y_ref, m_ref, adj, loss_ref, dw_ref, dw2_ref,
                ring, buf, acc, h_buf, s_one, z_one, u_two, w_v, small, count, stage, mine, total, child, part, parts, whole,
                small_parts, small_whole, pair, g_two, g_one, picked,
                ring_sem, x_sem, w_sem, count_send, count_recv, dsend, drecv, csend, crecv, fsend, frecv, gsend, grecv,
                ssend, srecv, bsend, brecv, psend, precv, qsend, qrecv, cut_sem, *sems):
    me, core, chip, partner = place()
    sems_x, sems_h = sems[:3], sems[3:]
    width = buf.shape[2]
    feats, rows = acc.shape
    hidden = h_buf.shape[1]
    chunks = [slice(t * width, (t + 1) * width) for t in range(TREES)]

    def slab(s, slot, j):
        u = unit_at(j % TREES, s, core if j < TREES else 1 - core, chip)
        return pltpu.make_async_copy(adj.at[:, pl.ds(pl.multiple_of(u * width, width), width)], ring.at[slot * 8 + j], ring_sem.at[slot, j // TREES])

    def load(s, slot, half):
        for t in range(TREES):
            slab(s, slot, half * TREES + t).start()

    def loaded(slot, half):
        four = ring.at[pl.ds(0, TREES)]
        pltpu.make_async_copy(four, four, ring_sem.at[slot, half]).wait()

    with jax.named_scope('start'):
        fetch = [pltpu.make_async_copy(x_ref.at[:, pl.ds(t * width, width)], buf.at[me * TREES + t], x_sem) for t in range(TREES)]
        for copy in fetch:
            copy.start()
        weight = m_ref[...].astype(jnp.float32)
        count[me] = jnp.broadcast_to(jnp.sum(weight, axis=1, keepdims=True), count.shape[1:])
        barrier_near()
        four = buf.at[pl.ds(0, TREES)]
        pltpu.make_async_copy(four, four, x_sem).wait()
    gather_start(buf, sems_x, 0)
    weights = pltpu.make_async_copy(w_hbm, w_v, w_sem)
    weights.start()
    for s in range(RING):
        for half in range(2):
            load(s, s, half)
    acc[...] = jnp.zeros_like(acc)

    def terms(units_ref, s, slot, half, trees=range(TREES)):
        which = core if half == 0 else 1 - core
        return [(units_ref, unit_at(t, s, which, chip), slot * 8 + half * TREES + t) for t in trees]

    def aggregate(out, pairs):
        for cols in chunks:
            out[:, cols] += sum(lax.dot_general(ref[u], ring[j, cols], COL_CONTRACT, preferred_element_type=jnp.float32) for ref, u, j in pairs)

    def step_one(s, carry):
        with jax.named_scope('arrive'):
            @pl.when(s > 0)
            def _():
                gather_arrive(buf, sems_x, s, 0, cut=cut)
        for half in range(2):
            with jax.named_scope('consume'):
                if half == 1:
                    gather_take(buf, sems_x, s)
                slot = lax.rem(s, RING)
                loaded(slot, half)
                aggregate(acc, terms(buf, s, slot, half))
                late = s // RING
                load((1 - late) * (s + RING) + late * (s - RING), slot, half)
        return carry

    cut = feats * 2 // 3 // 16 * 16
    final, slot = STEPS - 1, (STEPS - 1) % RING
    lax.fori_loop(0, final, step_one, 0)
    early, late = (range(TREES - 1), final), (range(TREES - 1, TREES), STEPS)
    for half in range(2):
        for trees, hand in (early, late):
            with jax.named_scope('consume'):
                if half == 0:
                    gather_arrive(buf, sems_x, final, 0, trees, hand, cut)
                else:
                    gather_take(buf, sems_x, hand, len(trees))
                if hand == final:
                    loaded(slot, half)
                aggregate(acc, terms(buf, final, slot, half, trees))
    for half in range(2):
        load(final - RING, slot, half)
    with jax.named_scope('mid'):
        weights.wait()
        s_one[0:feats] = acc[...].astype(jnp.bfloat16)
        s_one[feats:] = jnp.zeros_like(s_one[feats:])
        w_rows = w_v[...].astype(jnp.bfloat16)
        for t, cols in enumerate(chunks):
            z = lax.dot_general(w_rows, s_one[0:feats, cols], ROW_CONTRACT, preferred_element_type=jnp.float32)
            z_one[:, cols] = z
            h_buf[me * TREES + t] = jnp.maximum(z, 0.0).astype(jnp.bfloat16)
    gather_start(h_buf, sems_h, EARLY)
    send_all(n, lambda to: count.at[me], count.at[me], count_send, count_recv)
    two = acc.at[0:hidden]

    def take_two(p, half):
        loaded(lax.rem(p, RING), half)
        return terms(h_buf, p, lax.rem(p, RING), half)

    def back_order(i):
        return early_order(STEPS - 1 - i)

    def load_two(p, half):
        late = p // RING
        load((1 - late) * (p + RING) + late * back_order(p - late * RING), lax.rem(p, RING), half)

    two[...] = jnp.zeros_like(two)
    with jax.named_scope('consume'):
        aggregate(two, take_two(0, 0))
        load_two(0, 0)
        gather_take(h_buf, sems_h, 0)
        aggregate(two, take_two(0, 1))
        load_two(0, 1)
    with jax.named_scope('arrive'):
        gather_arrive(h_buf, sems_h, 1, EARLY)
    with jax.named_scope('consume'):
        aggregate(two, take_two(1, 0))
        load_two(1, 0)

    def step_two(p, carry):
        with jax.named_scope('arrive'):
            gather_arrive(h_buf, sems_h, p, EARLY)
            gather_take(h_buf, sems_h, p - 1)
        with jax.named_scope('consume'):
            aggregate(two, take_two(p - 1, 1) + take_two(p, 0))
            load_two(p - 1, 1)
            load_two(p, 0)
        return carry

    lax.fori_loop(2, STEPS, step_two, 0)
    with jax.named_scope('last'):
        gather_take(h_buf, sems_h, STEPS - 1)
        aggregate(two, take_two(STEPS - 1, 1))
        load_two(STEPS - 1, 1)
    with jax.named_scope('soft'):
        wait_all(count.at[pl.ds(0, n - 1)], count_send, count_recv)
        labelled = jnp.sum(count[...], axis=0)[0:1, 0:1]
        s_two = two[...].astype(jnp.bfloat16)
        w_two = w2t_ref[...].astype(jnp.bfloat16)
        logits = jnp.dot(w_two, s_two, preferred_element_type=jnp.float32)
        shifted = logits - jnp.max(logits, axis=0, keepdims=True)
        log_prob = shifted - jnp.log(jnp.sum(jnp.exp(shifted), axis=0, keepdims=True))
        hot = lax.broadcasted_iota(jnp.int32, logits.shape, 0) == y_ref[...]
        grad = (weight * (jnp.exp(log_prob) - hot.astype(jnp.float32)) / labelled).astype(jnp.bfloat16)
        u_two[...] = lax.dot_general(w_two, grad, ROW_CONTRACT, preferred_element_type=jnp.float32).astype(jnp.bfloat16)
        g_two[...] = grad
        picked[...] = -weight * jnp.sum(jnp.where(hot, log_prob, 0.0), axis=0, keepdims=True)
    classes = g_two.shape[0]
    edge = small.shape[0] - 8
    owners = small.shape[0] // 8
    tile = pl.ds(pl.multiple_of(me * 8, 8), 8)

    def send_small():
        loss = jnp.sum(picked[...], axis=1, keepdims=True)
        labelled = jnp.sum(count[...], axis=0)[0:1, 0:1]
        small[0:classes] = lax.dot_general(g_two[...], two[...].astype(jnp.bfloat16), COL_CONTRACT, preferred_element_type=jnp.float32)
        small[classes:edge] = jnp.zeros((edge - classes, hidden), jnp.float32)
        small[edge:] = jnp.broadcast_to(loss / labelled, (8, hidden))
        for o in range(owners):
            @pl.when(me != o)
            def _():
                remote(small.at[pl.ds(o * 8, 8)], small_parts.at[me], ssend, srecv, o).start()

    def to_partner(s, t):
        return remote(stage.at[s, t], total.at[s, t], dsend, drecv.at[s], partner)

    def to_parent(s, t, k):
        return remote(total.at[s, t], child.at[s - 1, t], csend, crecv.at[s - 1, t], neighbour(t, k, core, chip))

    far, cut = STEPS - 1, hidden * 2 // 3 // 8 * 8 + 8
    parts_of_far = ((slice(0, cut), 2, (far - 1, TREES - 1)), (slice(cut, hidden), 1, (0, 0)))

    def to_parents(which):
        rows, k, sem = parts_of_far[which]
        ref = (STEPS - 1, TREES - 1, rows)
        got = (STEPS - 2, TREES - 1, rows)
        sems_far = crecv.at[sem] if which == 0 else cut_sem
        return remote(total.at[ref], child.at[got], csend, sems_far, neighbour(TREES - 1, k, core, chip))

    def from_far(s, which):
        to_parents(which).wait_recv()
        rows = parts_of_far[which][0]
        total[s, TREES - 1, rows] = total[s, TREES - 1, rows] + child[STEPS - 2, TREES - 1, rows]

    def give(s, slot):
        loaded(slot, 1)
        for t in range(TREES):
            stage[s, t] = jnp.dot(u_two[...], ring[slot * 8 + TREES + t], preferred_element_type=jnp.float32)
        for t in range(TREES):
            to_partner(s, t).start()
        loaded(slot, 0)
        for t in range(TREES):
            mine[t] = jnp.dot(u_two[...], ring[slot * 8 + t], preferred_element_type=jnp.float32)

    def join(s):
        remote(total.at[s], total.at[s], dsend, drecv.at[s], partner).wait_recv()

    def gather_children(s, t):
        total[s, t] = total[s, t] + mine[t]
        for k in range(3):
            last = k == 2 and t == TREES - 1

            @pl.when((s < 2 ** k) & (s != (3 if last else STEPS)))
            def _():
                to_parent(s + 2 ** k, t, k).wait_recv()
                total[s, t] = total[s, t] + child[s + 2 ** k - 1, t]
        if t == TREES - 1:
            @pl.when(s == 3)
            def _():
                from_far(s, 0)

            @pl.when(s == 5)
            def _():
                from_far(s, 1)

    def reduce_small():
        @pl.when(me < owners)
        def _():
            small_parts[me] = small[tile]
            got = small_parts.at[pl.ds(0, n - 1)]
            remote(got, got, ssend, srecv, partner).wait_recv()
            small_whole[tile] = jnp.sum(small_parts[...], axis=0)
            for i in range(1, n):
                remote(small_whole.at[tile], small_whole.at[tile], bsend, brecv, lax.rem(me + i, n)).start()

    def finish_small():
        sent = small_parts.at[pl.ds(0, n - 1)]
        fewer, every = small_whole.at[pl.ds(0, owners * 8 - 8)], small_whole.at[pl.ds(0, owners * 8)]

        @pl.when(me < owners)
        def _():
            remote(sent, sent, bsend, brecv, partner).wait_send()
            remote(fewer, fewer, ssend, brecv, partner).wait_send()
            remote(fewer, fewer, ssend, brecv, partner).wait_recv()

        @pl.when(me >= owners)
        def _():
            remote(every, every, ssend, brecv, partner).wait_send()
            remote(every, every, ssend, brecv, partner).wait_recv()

    def step_back(i, carry):
        s = back_order(i)
        slot = lax.rem(i, RING)

        @pl.when(i == STEPS - 2)
        def _():
            send_small()

        with jax.named_scope('give'):
            give(s, slot)

            @pl.when(i + RING < STEPS)
            def _():
                load(back_order(i + RING), slot, 1)
                load(back_order(i + RING), slot, 0)
        with jax.named_scope('take'):
            join(s)
            for t in range(TREES):
                gather_children(s, t)
                for k in range(3):
                    top = STEPS - 1 if k == 2 and t == TREES - 1 else 2 ** (k + 1)

                    @pl.when((s >= 2 ** k) & (s < top))
                    def _():
                        to_parent(s, t, k).start()
                if t == TREES - 1:
                    @pl.when(s == STEPS - 1)
                    def _():
                        to_parents(0).start()
                        to_parents(1).start()
        return carry

    lax.fori_loop(0, STEPS - 1, step_back, 0)
    chips = n // 2
    half, share = part.shape[0] // 2, part.shape[0] // n
    mine_rows = pl.ds(pl.multiple_of(core * half, 8), half)
    their_rows = pl.ds(pl.multiple_of((1 - core) * half, 8), half)
    most = slice(0, (TREES - 1) * width)
    with jax.named_scope('give'):
        give(0, (STEPS - 1) % RING)
        join(0)

    def hidden_grad(t):
        gather_children(0, t)
        g_one[:, chunks[t]] = jnp.where(z_one[:, chunks[t]] > 0.0, total[0, t], 0.0).astype(jnp.bfloat16)

    def weight_grad(out_rows, cols):
        return lax.dot_general(s_one[out_rows, cols], g_one[:, cols], COL_CONTRACT, preferred_element_type=jnp.float32)

    with jax.named_scope('take'):
        for t in range(TREES - 1):
            hidden_grad(t)
        part[...] = weight_grad(slice(None), most)
        hidden_grad(TREES - 1)
    with jax.named_scope('dw'):
        part[their_rows] = part[their_rows] + weight_grad(their_rows, chunks[-1])
        over = remote(part.at[their_rows], pair, psend, precv, partner)
        over.start()
        part[mine_rows] = part[mine_rows] + weight_grad(mine_rows, chunks[-1])
    reduce_small()
    with jax.named_scope('drain'):
        gather_drain(buf, sems_x)
        gather_drain(h_buf, sems_h)
        remote(stage, stage, dsend, drecv.at[0], partner).wait_send()
        remote(child, child, csend, crecv.at[0, 0], partner).wait_send()
    with jax.named_scope('pair'):
        over.wait()
        pair[...] = pair[...] + part[mine_rows]

    def share_of(q):
        return pl.ds(pl.multiple_of(q * share, 8), share)

    for i in range(1, chips):
        to = lax.rem(chip + i, chips)
        remote(pair.at[share_of(to)], parts.at[chip], fsend, frecv, to * 2 + core).start()
    parts[chip] = pair[share_of(chip)]
    with jax.named_scope('red'):
        wait_all(parts.at[pl.ds(0, chips - 1)], fsend, frecv)
    own = whole.at[pl.ds(pl.multiple_of(core * half + chip * share, 8), share)]
    own[...] = jnp.sum(parts[...], axis=0)
    for i in range(1, chips):
        remote(own, own, gsend, grecv, lax.rem(chip + i, chips) * 2 + core).start()
    with jax.named_scope('spread'):
        wait_all(whole.at[pl.ds(0, (chips - 1) * share)], gsend, grecv)
    swap = remote(whole.at[mine_rows], whole.at[mine_rows], qsend, qrecv, partner)
    swap.start()
    finish_small()
    dw2_ref[...] = small_whole[0:dw2_ref.shape[0]]
    loss_ref[...] = small_whole[edge:edge + 8]
    with jax.named_scope('swap'):
        swap.wait()
    dw_ref[...] = whole[0:feats]


def finish_kernel(loss_in, dw_in, dw2_in, loss_ref, dw_ref, dw2_ref):
    loss_ref[...] = loss_in[0:1, 0:1]
    dw_ref[...] = dw_in[...]
    dw2_ref[...] = dw2_in[...]


def train_step(x_rows, w_one, w2t, labels, mask, adj):
    rows, nodes = adj.shape
    n = nodes // rows
    feats, width = x_rows.shape[0], rows // TREES
    classes, hidden = w2t.shape
    units = n * TREES
    small = -(-classes // 8) * 8 + 8
    share = -(-feats // (8 * n)) * 8
    vmem, hbm = pl.BlockSpec(memory_space=pltpu.VMEM), pl.BlockSpec(memory_space=pl.ANY)
    dma, f32, bf16 = pltpu.SemaphoreType.DMA, jnp.float32, jnp.bfloat16
    block = (TREES, hidden, width)
    loss, dw_one, dw_two = pl.pallas_call(
        functools.partial(step_kernel, n),
        name='step',
        out_shape=(pltpu.VMEM((8, hidden), f32), pltpu.VMEM((feats, hidden), f32), pltpu.VMEM((classes, hidden), f32)),
        in_specs=[hbm, hbm, vmem, vmem, vmem, hbm],
        out_specs=(vmem,) * 3,
        scratch_shapes=[
            pltpu.VMEM((RING * 8, rows, width), bf16), pltpu.VMEM((units, feats, width), bf16), pltpu.VMEM((feats, rows), f32),
            pltpu.VMEM((units, hidden, width), bf16), pltpu.VMEM((n * share, rows), bf16), pltpu.VMEM((hidden, rows), f32),
            pltpu.VMEM((hidden, rows), bf16), pltpu.VMEM((feats, hidden), f32), pltpu.VMEM((small, hidden), f32), pltpu.VMEM((n, 8, 128), f32),
            pltpu.VMEM((STEPS, *block), f32), pltpu.VMEM(block, f32), pltpu.VMEM((STEPS, *block), f32), pltpu.VMEM((STEPS - 1, *block), f32),
            pltpu.VMEM((n * share, hidden), f32), pltpu.VMEM((n // 2, share, hidden), f32), pltpu.VMEM((n * share, hidden), f32),
            pltpu.VMEM((n, 8, hidden), f32), pltpu.VMEM((small, hidden), f32), pltpu.VMEM((n // 2 * share, hidden), f32),
            pltpu.VMEM((classes, rows), bf16), pltpu.VMEM((hidden, rows), bf16), pltpu.VMEM((1, rows), f32),
            dma((RING, 2)), dma, dma, dma, dma, dma, dma((STEPS,)), dma, dma((STEPS - 1, TREES)), *[dma] * 13, *gather_sems(), *gather_sems()],
        compiler_params=pltpu.CompilerParams(collective_id=0, has_side_effects=True, vmem_limit_bytes=62000000),
        cost_estimate=pl.CostEstimate(flops=2 * rows * nodes * (feats + 2 * hidden), bytes_accessed=6 * rows * nodes, transcendentals=0),
    )(x_rows, w_one, w2t, labels, mask, adj)
    return pl.pallas_call(
        finish_kernel,
        name='finish',
        out_shape=(jax.ShapeDtypeStruct((1, 1), f32), jax.ShapeDtypeStruct((feats, hidden), f32), jax.ShapeDtypeStruct((classes, hidden), f32)),
        in_specs=[vmem] * 3,
        out_specs=(vmem,) * 3,
    )(*[pltpu.with_memory_space_constraint(x, pltpu.VMEM) for x in (loss, dw_one, dw_two)])


def solution(mesh):
    axis_name = AXIS

    def local_step(adj_rows, feat_rows, w_one, w_two, label_rows, mask_rows):
        rows = adj_rows.shape[0]
        loss, dw_one, dw_two = train_step(feat_rows.T, w_one, w_two.T, label_rows.reshape(1, rows), mask_rows.reshape(1, rows), adj_rows)
        return loss.reshape(1), dw_one, dw_two.T

    return jax.shard_map(local_step, mesh=mesh, in_specs=(P(axis_name, None), P(axis_name, None), P(None, None), P(None, None), P(axis_name), P(axis_name)), out_specs=(P(None), P(None, None), P(None, None)), check_vma=False)
```

```python
import functools

import jax
import jax.numpy as jnp
from jax import lax
from jax.experimental import pallas as pl
from jax.experimental.pallas import tpu as pltpu
from jax.sharding import PartitionSpec as P

MESH = pl.DeviceIdType.MESH
AXIS = 'nodes'
TREES = 4
EARLY = 2
RING = 4
STEPS = 8
COL_CONTRACT = (((1,), (1,)), ((), ()))
ROW_CONTRACT = (((0,), (0,)), ((), ()))


def tree_axis(tree, k, core, chip):
    if tree < 3:
        weight = 2 ** ((tree + k) % 3)
        return weight, lax.rem(chip // weight, 2)
    weight = (1 - core) * 2 ** k + core * 2 ** (2 - k)
    low, high = lax.rem(chip // 2 ** k, 2), lax.rem(chip // 2 ** (2 - k), 2)
    return weight, (1 - core) * low + core * high


def chip_at(tree, offset, core, chip):
    out = chip
    for k in range(3):
        weight, bit = tree_axis(tree, k, core, chip)
        out = out + lax.rem(offset // 2 ** k, 2) * weight * (1 - 2 * bit)
    return out


def back_order(i):
    pair = i // 2
    swap = lax.rem(pair, 2) * (1 - pair // 2)
    return STEPS - 1 - i - swap * (1 - 2 * lax.rem(i, 2))


def unit_at(tree, offset, core, chip):
    return (chip_at(tree, offset, core, chip) * 2 + core) * TREES + tree


def neighbour(tree, k, core, chip):
    weight, bit = tree_axis(tree, k, core, chip)
    return (chip + weight * (1 - 2 * bit)) * 2 + core


def remote(src, dst, send_sem, recv_sem, device):
    return pltpu.make_async_remote_copy(src_ref=src, dst_ref=dst, send_sem=send_sem, recv_sem=recv_sem, device_id=(device,), device_id_type=MESH)


def place():
    me = lax.axis_index(AXIS)
    core, chip = lax.rem(me, 2), me // 2
    return me, core, chip, chip * 2 + 1 - core


def gather_send(buf, sems, tree, offset, k, unit, rows=slice(None)):
    send, recv, hand = sems
    me, core, chip, partner = place()
    ref = buf.at[unit, rows]
    remote(ref, ref, send, recv.at[offset + 2 ** k - 1, tree], neighbour(tree, k, core, chip)).start()


def gather_hand(buf, sems, slot, unit):
    send, recv, hand = sems
    me, core, chip, partner = place()
    remote(buf.at[unit], buf.at[unit], send, hand.at[slot], partner).start()


def gather_start(buf, sems, early):
    me = lax.axis_index(AXIS)
    for k in range(3):
        for t in range(TREES if k < 2 else early):
            gather_send(buf, sems, t, 0, k, me * TREES + t)
        if k == 0:
            for t in range(TREES):
                gather_hand(buf, sems, 0, me * TREES + t)


def gather_arrive(buf, sems, s, early, trees=range(TREES), slot=None, cut=None):
    send, recv, hand = sems
    me, core, chip, partner = place()
    units = {t: unit_at(t, s, core, chip) for t in trees}
    for t, u in units.items():
        remote(buf.at[u], buf.at[u], send, recv.at[s - 1, t], partner).wait_recv()
        split = cut is not None and t == TREES - 1

        @pl.when(s == 1)
        def _():
            gather_send(buf, sems, t, s, 1, u)

        @pl.when((s > 1) & (s < (3 if split else 4)))
        def _():
            gather_send(buf, sems, t, s, 2, u)
        if split:
            @pl.when(s == 3)
            def _():
                gather_send(buf, sems, t, s, 2, u, slice(0, cut))

            @pl.when(s == 5)
            def _():
                gather_send(buf, sems, t, s, 1, u, slice(cut, None))
        gather_hand(buf, sems, s if slot is None else slot, u)

    @pl.when(s == 1)
    def _():
        for t in range(early, TREES):
            gather_send(buf, sems, t, 0, 2, me * TREES + t)
        for t, u in units.items():
            gather_send(buf, sems, t, s, 2, u)


def gather_take(buf, sems, slot, count=TREES):
    send, recv, hand = sems
    me, core, chip, partner = place()
    units = buf.at[pl.ds(0, count)]
    remote(units, units, send, hand.at[slot], partner).wait_recv()


def gather_drain(buf, sems):
    send, recv, hand = sems
    me, core, chip, partner = place()
    sent = buf.at[pl.ds(0, TREES * (STEPS - 1 + STEPS))]
    remote(sent, sent, send, hand.at[0], partner).wait_send()


def gather_sems():
    dma = pltpu.SemaphoreType.DMA
    return [dma, dma((STEPS - 1, TREES)), dma((STEPS + 1,))]


def barrier_near():
    me, core, chip, partner = place()
    sem = pltpu.get_barrier_semaphore()
    pl.semaphore_signal(sem, inc=1, device_id=(partner,), device_id_type=MESH)
    for k in range(3):
        pl.semaphore_signal(sem, inc=1, device_id=(neighbour(0, k, core, chip),), device_id_type=MESH)
    pl.semaphore_wait(sem, 4)


def send_all(n, src, dst, send_sem, recv_sem):
    me = lax.axis_index(AXIS)
    for i in range(1, n):
        to = lax.rem(me + i, n)
        remote(src(to), dst, send_sem, recv_sem, to).start()


def wait_all(ref, send_sem, recv_sem):
    me, core, chip, partner = place()
    copy = remote(ref, ref, send_sem, recv_sem, partner)
    copy.wait_send()
    copy.wait_recv()


def step_kernel(n, x_ref, w_hbm, w2t_ref, y_ref, m_ref, adj, loss_ref, dw_ref, dw2_ref,
                ring, buf, acc, h_buf, s_one, z_one, u_two, w_v, small, count, stage, mine, total, child, part, parts, whole,
                small_parts, small_whole, pair, g_two, g_one, picked,
                ring_sem, x_sem, w_sem, count_send, count_recv, dsend, drecv, csend, crecv, fsend, frecv, gsend, grecv,
                ssend, srecv, bsend, brecv, psend, precv, qsend, qrecv, cut_sem, *sems):
    me, core, chip, partner = place()
    sems_x, sems_h = sems[:3], sems[3:]
    width = buf.shape[2]
    feats, rows = acc.shape
    hidden = h_buf.shape[1]
    chunks = [slice(t * width, (t + 1) * width) for t in range(TREES)]

    def slab(s, slot, j):
        u = unit_at(j % TREES, s, core if j < TREES else 1 - core, chip)
        return pltpu.make_async_copy(adj.at[:, pl.ds(pl.multiple_of(u * width, width), width)], ring.at[slot * 8 + j], ring_sem.at[slot, j // TREES])

    def load(s, slot, half):
        for t in range(TREES):
            slab(s, slot, half * TREES + t).start()

    def loaded(slot, half):
        four = ring.at[pl.ds(0, TREES)]
        pltpu.make_async_copy(four, four, ring_sem.at[slot, half]).wait()

    with jax.named_scope('start'):
        fetch = [pltpu.make_async_copy(x_ref.at[:, pl.ds(t * width, width)], buf.at[me * TREES + t], x_sem) for t in range(TREES)]
        for copy in fetch:
            copy.start()
        weight = m_ref[...].astype(jnp.float32)
        count[me] = jnp.broadcast_to(jnp.sum(weight, axis=1, keepdims=True), count.shape[1:])
        barrier_near()
        four = buf.at[pl.ds(0, TREES)]
        pltpu.make_async_copy(four, four, x_sem).wait()
    gather_start(buf, sems_x, 0)
    weights = pltpu.make_async_copy(w_hbm, w_v, w_sem)
    weights.start()
    for s in range(RING):
        for half in range(2):
            load(s, s, half)
    acc[...] = jnp.zeros_like(acc)

    def terms(units_ref, s, slot, half, trees=range(TREES)):
        which = core if half == 0 else 1 - core
        return [(units_ref, unit_at(t, s, which, chip), slot * 8 + half * TREES + t) for t in trees]

    def aggregate(out, pairs):
        for cols in chunks:
            out[:, cols] += sum(lax.dot_general(ref[u], ring[j, cols], COL_CONTRACT, preferred_element_type=jnp.float32) for ref, u, j in pairs)

    def step_one(s, carry):
        with jax.named_scope('arrive'):
            @pl.when(s > 0)
            def _():
                gather_arrive(buf, sems_x, s, 0, cut=cut)
        for half in range(2):
            with jax.named_scope('consume'):
                if half == 1:
                    gather_take(buf, sems_x, s)
                slot = lax.rem(s, RING)
                loaded(slot, half)
                aggregate(acc, terms(buf, s, slot, half))
                late = s // RING
                load((1 - late) * (s + RING) + late * (s - RING), slot, half)
        return carry

    cut = feats * 2 // 3 // 16 * 16
    final, slot = STEPS - 1, (STEPS - 1) % RING
    lax.fori_loop(0, final, step_one, 0)
    early, late = (range(TREES - 1), final), (range(TREES - 1, TREES), STEPS)
    for half in range(2):
        for trees, hand in (early, late):
            with jax.named_scope('consume'):
                if half == 0:
                    gather_arrive(buf, sems_x, final, 0, trees, hand, cut)
                else:
                    gather_take(buf, sems_x, hand, len(trees))
                if hand == final:
                    loaded(slot, half)
                aggregate(acc, terms(buf, final, slot, half, trees))
    for half in range(2):
        load(final - RING, slot, half)
    with jax.named_scope('mid'):
        weights.wait()
        s_one[0:feats] = acc[...].astype(jnp.bfloat16)
        s_one[feats:] = jnp.zeros_like(s_one[feats:])
        w_rows = w_v[...].astype(jnp.bfloat16)
        for t, cols in enumerate(chunks):
            z = lax.dot_general(w_rows, s_one[0:feats, cols], ROW_CONTRACT, preferred_element_type=jnp.float32)
            z_one[:, cols] = z
            h_buf[me * TREES + t] = jnp.maximum(z, 0.0).astype(jnp.bfloat16)
    gather_start(h_buf, sems_h, EARLY)
    send_all(n, lambda to: count.at[me], count.at[me], count_send, count_recv)
    two = acc.at[0:hidden]

    def take_two(p, half):
        loaded(lax.rem(p, RING), half)
        return terms(h_buf, p, lax.rem(p, RING), half)

    def load_two(p, half):
        late = p // RING
        load((1 - late) * (p + RING) + late * back_order(p - late * RING), lax.rem(p, RING), half)

    two[...] = jnp.zeros_like(two)
    with jax.named_scope('consume'):
        aggregate(two, take_two(0, 0))
        load_two(0, 0)
        gather_take(h_buf, sems_h, 0)
        aggregate(two, take_two(0, 1))
        load_two(0, 1)
    with jax.named_scope('arrive'):
        gather_arrive(h_buf, sems_h, 1, EARLY)
    with jax.named_scope('consume'):
        aggregate(two, take_two(1, 0))
        load_two(1, 0)

    def block_two(first, count):
        with jax.named_scope('arrive'):
            for p in range(first, first + count):
                gather_arrive(h_buf, sems_h, p, EARLY)
                gather_take(h_buf, sems_h, p - 1)
        with jax.named_scope('consume'):
            aggregate(two, sum([take_two(p - 1, 1) + take_two(p, 0) for p in range(first, first + count)], []))
            for p in range(first, first + count):
                load_two(p - 1, 1)
                load_two(p, 0)

    for first, steps in ((2, 1), (3, 2), (5, 2), (7, 1)):
        block_two(first, steps)
    with jax.named_scope('last'):
        gather_take(h_buf, sems_h, STEPS - 1)
        aggregate(two, take_two(STEPS - 1, 1))
        load_two(STEPS - 1, 1)
    with jax.named_scope('soft'):
        wait_all(count.at[pl.ds(0, n - 1)], count_send, count_recv)
        labelled = jnp.sum(count[...], axis=0)[0:1, 0:1]
        s_two = two[...].astype(jnp.bfloat16)
        w_two = w2t_ref[...].astype(jnp.bfloat16)
        logits = jnp.dot(w_two, s_two, preferred_element_type=jnp.float32)
        shifted = logits - jnp.max(logits, axis=0, keepdims=True)
        log_prob = shifted - jnp.log(jnp.sum(jnp.exp(shifted), axis=0, keepdims=True))
        hot = lax.broadcasted_iota(jnp.int32, logits.shape, 0) == y_ref[...]
        grad = (weight * (jnp.exp(log_prob) - hot.astype(jnp.float32)) / labelled).astype(jnp.bfloat16)
        u_two[...] = lax.dot_general(w_two, grad, ROW_CONTRACT, preferred_element_type=jnp.float32).astype(jnp.bfloat16)
        g_two[...] = grad
        picked[...] = -weight * jnp.sum(jnp.where(hot, log_prob, 0.0), axis=0, keepdims=True)
    classes = g_two.shape[0]
    edge = small.shape[0] - 8
    owners = small.shape[0] // 8
    tile = pl.ds(pl.multiple_of(me * 8, 8), 8)

    def send_small():
        loss = jnp.sum(picked[...], axis=1, keepdims=True)
        labelled = jnp.sum(count[...], axis=0)[0:1, 0:1]
        small[0:classes] = lax.dot_general(g_two[...], two[...].astype(jnp.bfloat16), COL_CONTRACT, preferred_element_type=jnp.float32)
        small[classes:edge] = jnp.zeros((edge - classes, hidden), jnp.float32)
        small[edge:] = jnp.broadcast_to(loss / labelled, (8, hidden))
        for o in range(owners):
            @pl.when(me != o)
            def _():
                remote(small.at[pl.ds(o * 8, 8)], small_parts.at[me], ssend, srecv, o).start()

    send_small()

    def to_partner(s, t):
        return remote(stage.at[s, t], total.at[s, t], dsend, drecv.at[s], partner)

    def to_parent(s, t, k):
        return remote(total.at[s, t], child.at[s - 1, t], csend, crecv.at[s - 1, t], neighbour(t, k, core, chip))

    far, cut = STEPS - 1, hidden * 2 // 3 // 8 * 8 + 8
    parts_of_far = ((slice(0, cut), 2, (far - 1, TREES - 1)), (slice(cut, hidden), 1, (0, 0)))

    def to_parents(which):
        rows, k, sem = parts_of_far[which]
        ref = (STEPS - 1, TREES - 1, rows)
        got = (STEPS - 2, TREES - 1, rows)
        sems_far = crecv.at[sem] if which == 0 else cut_sem
        return remote(total.at[ref], child.at[got], csend, sems_far, neighbour(TREES - 1, k, core, chip))

    def from_far(s, which):
        to_parents(which).wait_recv()
        rows = parts_of_far[which][0]
        total[s, TREES - 1, rows] = total[s, TREES - 1, rows] + child[STEPS - 2, TREES - 1, rows]

    def give(s, slot):
        loaded(slot, 1)
        for t in range(TREES):
            stage[s, t] = jnp.dot(u_two[...], ring[slot * 8 + TREES + t], preferred_element_type=jnp.float32)
        for t in range(TREES):
            to_partner(s, t).start()
        loaded(slot, 0)
        for t in range(TREES):
            mine[t] = jnp.dot(u_two[...], ring[slot * 8 + t], preferred_element_type=jnp.float32)

    def join(s):
        remote(total.at[s], total.at[s], dsend, drecv.at[s], partner).wait_recv()

    def gather_children(s, t):
        total[s, t] = total[s, t] + mine[t]
        for k in range(3):
            last = k == 2 and t == TREES - 1

            @pl.when((s < 2 ** k) & (s != (3 if last else STEPS)))
            def _():
                to_parent(s + 2 ** k, t, k).wait_recv()
                total[s, t] = total[s, t] + child[s + 2 ** k - 1, t]
        if t == TREES - 1:
            @pl.when(s == 3)
            def _():
                from_far(s, 0)

            @pl.when(s == 5)
            def _():
                from_far(s, 1)

    def reduce_small():
        @pl.when(me < owners)
        def _():
            small_parts[me] = small[tile]
            got = small_parts.at[pl.ds(0, n - 1)]
            remote(got, got, ssend, srecv, partner).wait_recv()
            small_whole[tile] = jnp.sum(small_parts[...], axis=0)
            for i in range(1, n):
                remote(small_whole.at[tile], small_whole.at[tile], bsend, brecv, lax.rem(me + i, n)).start()

    def finish_small():
        sent = small_parts.at[pl.ds(0, n - 1)]
        fewer, every = small_whole.at[pl.ds(0, owners * 8 - 8)], small_whole.at[pl.ds(0, owners * 8)]

        @pl.when(me < owners)
        def _():
            remote(sent, sent, bsend, brecv, partner).wait_send()
            remote(fewer, fewer, ssend, brecv, partner).wait_send()
            remote(fewer, fewer, ssend, brecv, partner).wait_recv()

        @pl.when(me >= owners)
        def _():
            remote(every, every, ssend, brecv, partner).wait_send()
            remote(every, every, ssend, brecv, partner).wait_recv()

    def step_back(i, carry):
        s = back_order(i)
        slot = lax.rem(i, RING)

        with jax.named_scope('give'):
            give(s, slot)

            @pl.when(i + RING < STEPS)
            def _():
                load(back_order(i + RING), slot, 1)
                load(back_order(i + RING), slot, 0)
        with jax.named_scope('take'):
            join(s)
            for t in range(TREES):
                gather_children(s, t)
                for k in range(3):
                    top = STEPS - 1 if k == 2 and t == TREES - 1 else 2 ** (k + 1)

                    @pl.when((s >= 2 ** k) & (s < top))
                    def _():
                        to_parent(s, t, k).start()
                if t == TREES - 1:
                    @pl.when(s == STEPS - 1)
                    def _():
                        to_parents(0).start()
                        to_parents(1).start()
        return carry

    lax.fori_loop(0, STEPS - 1, step_back, 0)
    chips = n // 2
    half, share = part.shape[0] // 2, part.shape[0] // n
    mine_rows = pl.ds(pl.multiple_of(core * half, 8), half)
    their_rows = pl.ds(pl.multiple_of((1 - core) * half, 8), half)
    most = slice(0, (TREES - 1) * width)
    with jax.named_scope('give'):
        give(0, (STEPS - 1) % RING)
        join(0)

    def hidden_grad(t):
        gather_children(0, t)
        g_one[:, chunks[t]] = jnp.where(z_one[:, chunks[t]] > 0.0, total[0, t], 0.0).astype(jnp.bfloat16)

    def weight_grad(out_rows, cols):
        return lax.dot_general(s_one[out_rows, cols], g_one[:, cols], COL_CONTRACT, preferred_element_type=jnp.float32)

    with jax.named_scope('take'):
        for t in range(TREES - 1):
            hidden_grad(t)
        part[...] = weight_grad(slice(None), most)
        hidden_grad(TREES - 1)
    with jax.named_scope('dw'):
        part[their_rows] = part[their_rows] + weight_grad(their_rows, chunks[-1])
        over = remote(part.at[their_rows], pair, psend, precv, partner)
        over.start()
        part[mine_rows] = part[mine_rows] + weight_grad(mine_rows, chunks[-1])
    reduce_small()
    with jax.named_scope('drain'):
        gather_drain(buf, sems_x)
        gather_drain(h_buf, sems_h)
        remote(stage, stage, dsend, drecv.at[0], partner).wait_send()
        remote(child, child, csend, crecv.at[0, 0], partner).wait_send()
    with jax.named_scope('pair'):
        over.wait()
        pair[...] = pair[...] + part[mine_rows]

    def share_of(q):
        return pl.ds(pl.multiple_of(q * share, 8), share)

    for i in range(1, chips):
        to = lax.rem(chip + i, chips)
        remote(pair.at[share_of(to)], parts.at[chip], fsend, frecv, to * 2 + core).start()
    parts[chip] = pair[share_of(chip)]
    with jax.named_scope('red'):
        wait_all(parts.at[pl.ds(0, chips - 1)], fsend, frecv)
    own = whole.at[pl.ds(pl.multiple_of(core * half + chip * share, 8), share)]
    own[...] = jnp.sum(parts[...], axis=0)
    for i in range(1, chips):
        remote(own, own, gsend, grecv, lax.rem(chip + i, chips) * 2 + core).start()
    with jax.named_scope('spread'):
        wait_all(whole.at[pl.ds(0, (chips - 1) * share)], gsend, grecv)
    swap = remote(whole.at[mine_rows], whole.at[mine_rows], qsend, qrecv, partner)
    swap.start()
    finish_small()
    dw2_ref[...] = small_whole[0:dw2_ref.shape[0]]
    loss_ref[...] = small_whole[edge:edge + 8]
    with jax.named_scope('swap'):
        swap.wait()
    dw_ref[...] = whole[0:feats]


def finish_kernel(loss_in, dw_in, dw2_in, loss_ref, dw_ref, dw2_ref):
    loss_ref[...] = loss_in[0:1, 0:1]
    dw_ref[...] = dw_in[...]
    dw2_ref[...] = dw2_in[...]


def train_step(x_rows, w_one, w2t, labels, mask, adj):
    rows, nodes = adj.shape
    n = nodes // rows
    feats, width = x_rows.shape[0], rows // TREES
    classes, hidden = w2t.shape
    units = n * TREES
    small = -(-classes // 8) * 8 + 8
    share = -(-feats // (8 * n)) * 8
    vmem, hbm = pl.BlockSpec(memory_space=pltpu.VMEM), pl.BlockSpec(memory_space=pl.ANY)
    dma, f32, bf16 = pltpu.SemaphoreType.DMA, jnp.float32, jnp.bfloat16
    block = (TREES, hidden, width)
    loss, dw_one, dw_two = pl.pallas_call(
        functools.partial(step_kernel, n),
        name='step',
        out_shape=(pltpu.VMEM((8, hidden), f32), pltpu.VMEM((feats, hidden), f32), pltpu.VMEM((classes, hidden), f32)),
        in_specs=[hbm, hbm, vmem, vmem, vmem, hbm],
        out_specs=(vmem,) * 3,
        scratch_shapes=[
            pltpu.VMEM((RING * 8, rows, width), bf16), pltpu.VMEM((units, feats, width), bf16), pltpu.VMEM((feats, rows), f32),
            pltpu.VMEM((units, hidden, width), bf16), pltpu.VMEM((n * share, rows), bf16), pltpu.VMEM((hidden, rows), f32),
            pltpu.VMEM((hidden, rows), bf16), pltpu.VMEM((feats, hidden), f32), pltpu.VMEM((small, hidden), f32), pltpu.VMEM((n, 8, 128), f32),
            pltpu.VMEM((STEPS, *block), f32), pltpu.VMEM(block, f32), pltpu.VMEM((STEPS, *block), f32), pltpu.VMEM((STEPS - 1, *block), f32),
            pltpu.VMEM((n * share, hidden), f32), pltpu.VMEM((n // 2, share, hidden), f32), pltpu.VMEM((n * share, hidden), f32),
            pltpu.VMEM((n, 8, hidden), f32), pltpu.VMEM((small, hidden), f32), pltpu.VMEM((n // 2 * share, hidden), f32),
            pltpu.VMEM((classes, rows), bf16), pltpu.VMEM((hidden, rows), bf16), pltpu.VMEM((1, rows), f32),
            dma((RING, 2)), dma, dma, dma, dma, dma, dma((STEPS,)), dma, dma((STEPS - 1, TREES)), *[dma] * 13, *gather_sems(), *gather_sems()],
        compiler_params=pltpu.CompilerParams(collective_id=0, has_side_effects=True, vmem_limit_bytes=62000000),
        cost_estimate=pl.CostEstimate(flops=2 * rows * nodes * (feats + 2 * hidden), bytes_accessed=6 * rows * nodes, transcendentals=0),
    )(x_rows, w_one, w2t, labels, mask, adj)
    return pl.pallas_call(
        finish_kernel,
        name='finish',
        out_shape=(jax.ShapeDtypeStruct((1, 1), f32), jax.ShapeDtypeStruct((feats, hidden), f32), jax.ShapeDtypeStruct((classes, hidden), f32)),
        in_specs=[vmem] * 3,
        out_specs=(vmem,) * 3,
    )(*[pltpu.with_memory_space_constraint(x, pltpu.VMEM) for x in (loss, dw_one, dw_two)])


def solution(mesh):
    axis_name = AXIS

    def local_step(adj_rows, feat_rows, w_one, w_two, label_rows, mask_rows):
        rows = adj_rows.shape[0]
        loss, dw_one, dw_two = train_step(feat_rows.T, w_one, w_two.T, label_rows.reshape(1, rows), mask_rows.reshape(1, rows), adj_rows)
        return loss.reshape(1), dw_one, dw_two.T

    return jax.shard_map(local_step, mesh=mesh, in_specs=(P(axis_name, None), P(axis_name, None), P(None, None), P(None, None), P(axis_name), P(axis_name)), out_specs=(P(None), P(None, None), P(None, None)), check_vma=False)
```

```python
import functools

import jax
import jax.numpy as jnp
from jax import lax
from jax.experimental import pallas as pl
from jax.experimental.pallas import tpu as pltpu
from jax.sharding import PartitionSpec as P

MESH = pl.DeviceIdType.MESH
AXIS = 'nodes'
TREES = 4
RING = 4
STEPS = 8
COL_CONTRACT = (((1,), (1,)), ((), ()))
ROW_CONTRACT = (((0,), (0,)), ((), ()))


def tree_axis(tree, k, core, chip):
    if tree < 3:
        weight = 2 ** ((tree + k) % 3)
        return weight, lax.rem(chip // weight, 2)
    weight = (1 - core) * 2 ** k + core * 2 ** (2 - k)
    low, high = lax.rem(chip // 2 ** k, 2), lax.rem(chip // 2 ** (2 - k), 2)
    return weight, (1 - core) * low + core * high


def chip_at(tree, offset, core, chip):
    out = chip
    for k in range(3):
        weight, bit = tree_axis(tree, k, core, chip)
        out = out + lax.rem(offset // 2 ** k, 2) * weight * (1 - 2 * bit)
    return out


def early_order(place):
    pair = (place + 1) // 2
    return place + (pair * (4 - pair)) // 4 * (7 - 2 * place)


def unit_at(tree, offset, core, chip):
    return (chip_at(tree, offset, core, chip) * 2 + core) * TREES + tree


def neighbour(tree, k, core, chip):
    weight, bit = tree_axis(tree, k, core, chip)
    return (chip + weight * (1 - 2 * bit)) * 2 + core


def remote(src, dst, send_sem, recv_sem, device):
    return pltpu.make_async_remote_copy(src_ref=src, dst_ref=dst, send_sem=send_sem, recv_sem=recv_sem, device_id=(device,), device_id_type=MESH)


def place():
    me = lax.axis_index(AXIS)
    core, chip = lax.rem(me, 2), me // 2
    return me, core, chip, chip * 2 + 1 - core


def gather_send(buf, sems, tree, offset, k, unit, rows=slice(None)):
    send, recv, hand = sems
    me, core, chip, partner = place()
    ref = buf.at[unit, rows]
    remote(ref, ref, send, recv.at[offset + 2 ** k - 1, tree], neighbour(tree, k, core, chip)).start()


def gather_hand(buf, sems, slot, unit):
    send, recv, hand = sems
    me, core, chip, partner = place()
    remote(buf.at[unit], buf.at[unit], send, hand.at[slot], partner).start()


def gather_start(buf, sems, links):
    me = lax.axis_index(AXIS)
    for k in range(links):
        for t in range(TREES):
            gather_send(buf, sems, t, 0, k, me * TREES + t)
        if k == 0:
            for t in range(TREES):
                gather_hand(buf, sems, 0, me * TREES + t)


def gather_arrive(buf, sems, s, links, trees=range(TREES), slot=None, cut=None):
    send, recv, hand = sems
    me, core, chip, partner = place()
    units = {t: unit_at(t, s, core, chip) for t in trees}
    for t, u in units.items():
        remote(buf.at[u], buf.at[u], send, recv.at[s - 1, t], partner).wait_recv()
        split = cut is not None and t == TREES - 1

        @pl.when(s == 1)
        def _():
            gather_send(buf, sems, t, s, 1, u)

        @pl.when((s > 1) & (s < (3 if split else 4)))
        def _():
            gather_send(buf, sems, t, s, 2, u)
        if split:
            @pl.when(s == 3)
            def _():
                gather_send(buf, sems, t, s, 2, u, slice(0, cut))

            @pl.when(s == 5)
            def _():
                gather_send(buf, sems, t, s, 1, u, slice(cut, None))
        gather_hand(buf, sems, s if slot is None else slot, u)

    @pl.when(s == 1)
    def _():
        if links < 3:
            for t in range(TREES):
                gather_send(buf, sems, t, 0, 2, me * TREES + t)
        for t, u in units.items():
            gather_send(buf, sems, t, s, 2, u)


def gather_take(buf, sems, slot, count=TREES):
    send, recv, hand = sems
    me, core, chip, partner = place()
    units = buf.at[pl.ds(0, count)]
    remote(units, units, send, hand.at[slot], partner).wait_recv()


def gather_drain(buf, sems):
    send, recv, hand = sems
    me, core, chip, partner = place()
    sent = buf.at[pl.ds(0, TREES * (STEPS - 1 + STEPS))]
    remote(sent, sent, send, hand.at[0], partner).wait_send()


def gather_sems():
    dma = pltpu.SemaphoreType.DMA
    return [dma, dma((STEPS - 1, TREES)), dma((STEPS + 1,))]


def barrier_near():
    me, core, chip, partner = place()
    sem = pltpu.get_barrier_semaphore()
    pl.semaphore_signal(sem, inc=1, device_id=(partner,), device_id_type=MESH)
    for k in range(3):
        pl.semaphore_signal(sem, inc=1, device_id=(neighbour(0, k, core, chip),), device_id_type=MESH)
    pl.semaphore_wait(sem, 4)


def send_all(n, src, dst, send_sem, recv_sem):
    me = lax.axis_index(AXIS)
    for i in range(1, n):
        to = lax.rem(me + i, n)
        remote(src(to), dst, send_sem, recv_sem, to).start()


def wait_all(ref, send_sem, recv_sem):
    me, core, chip, partner = place()
    copy = remote(ref, ref, send_sem, recv_sem, partner)
    copy.wait_send()
    copy.wait_recv()


def step_kernel(n, x_ref, w_hbm, w2t_ref, y_ref, m_ref, adj, loss_ref, dw_ref, dw2_ref,
                ring, buf, acc, h_buf, s_one, z_one, u_two, w_v, small, count, stage, mine, total, child, part, parts, whole,
                small_parts, small_whole, pair, g_two, g_one, picked,
                ring_sem, x_sem, w_sem, count_send, count_recv, dsend, drecv, csend, crecv, fsend, frecv, gsend, grecv,
                ssend, srecv, bsend, brecv, psend, precv, qsend, qrecv, *sems):
    me, core, chip, partner = place()
    sems_x, sems_h = sems[:3], sems[3:]
    width = buf.shape[2]
    feats, rows = acc.shape
    hidden = h_buf.shape[1]
    chunks = [slice(t * width, (t + 1) * width) for t in range(TREES)]

    def slab(s, slot, j):
        u = unit_at(j % TREES, s, core if j < TREES else 1 - core, chip)
        return pltpu.make_async_copy(adj.at[:, pl.ds(pl.multiple_of(u * width, width), width)], ring.at[slot * 8 + j], ring_sem.at[slot, j // TREES])

    def load(s, slot, half):
        for t in range(TREES):
            slab(s, slot, half * TREES + t).start()

    def loaded(slot, half):
        four = ring.at[pl.ds(0, TREES)]
        pltpu.make_async_copy(four, four, ring_sem.at[slot, half]).wait()

    with jax.named_scope('start'):
        fetch = [pltpu.make_async_copy(x_ref.at[:, pl.ds(t * width, width)], buf.at[me * TREES + t], x_sem) for t in range(TREES)]
        for copy in fetch:
            copy.start()
        weight = m_ref[...].astype(jnp.float32)
        count[me] = jnp.broadcast_to(jnp.sum(weight, axis=1, keepdims=True), count.shape[1:])
        barrier_near()
        four = buf.at[pl.ds(0, TREES)]
        pltpu.make_async_copy(four, four, x_sem).wait()
    gather_start(buf, sems_x, 2)
    weights = pltpu.make_async_copy(w_hbm, w_v, w_sem)
    weights.start()
    for s in range(RING):
        for half in range(2):
            load(s, s, half)
    acc[...] = jnp.zeros_like(acc)

    def terms(units_ref, s, slot, half, trees=range(TREES)):
        which = core if half == 0 else 1 - core
        return [(units_ref, unit_at(t, s, which, chip), slot * 8 + half * TREES + t) for t in trees]

    def aggregate(out, pairs):
        for cols in chunks:
            out[:, cols] += sum(lax.dot_general(ref[u], ring[j, cols], COL_CONTRACT, preferred_element_type=jnp.float32) for ref, u, j in pairs)

    def step_one(s, carry):
        with jax.named_scope('arrive'):
            @pl.when(s > 0)
            def _():
                gather_arrive(buf, sems_x, s, 2, cut=cut)
        for half in range(2):
            with jax.named_scope('consume'):
                if half == 1:
                    gather_take(buf, sems_x, s)
                slot = lax.rem(s, RING)
                loaded(slot, half)
                aggregate(acc, terms(buf, s, slot, half))
                late = s // RING
                load((1 - late) * (s + RING) + late * early_order(s - late * RING), slot, half)
        return carry

    cut = feats * 2 // 3 // 16 * 16
    final, slot = STEPS - 1, (STEPS - 1) % RING
    lax.fori_loop(0, final, step_one, 0)
    early, late = (range(TREES - 1), final), (range(TREES - 1, TREES), STEPS)
    for half in range(2):
        for trees, hand in (early, late):
            with jax.named_scope('consume'):
                if half == 0:
                    gather_arrive(buf, sems_x, final, 2, trees, hand, cut)
                else:
                    gather_take(buf, sems_x, hand, len(trees))
                if hand == final:
                    loaded(slot, half)
                aggregate(acc, terms(buf, final, slot, half, trees))
    for half in range(2):
        load(early_order(final - RING), slot, half)
    with jax.named_scope('mid'):
        weights.wait()
        s_one[0:feats] = acc[...].astype(jnp.bfloat16)
        s_one[feats:] = jnp.zeros_like(s_one[feats:])
        w_rows = w_v[...].astype(jnp.bfloat16)
        for t, cols in enumerate(chunks):
            z = lax.dot_general(w_rows, s_one[0:feats, cols], ROW_CONTRACT, preferred_element_type=jnp.float32)
            z_one[:, cols] = z
            h_buf[me * TREES + t] = jnp.maximum(z, 0.0).astype(jnp.bfloat16)
    gather_start(h_buf, sems_h, 3)
    send_all(n, lambda to: count.at[me], count.at[me], count_send, count_recv)
    two = acc.at[0:hidden]

    def take_two(p, half):
        loaded(lax.rem(p, RING), half)
        return terms(h_buf, early_order(p), lax.rem(p, RING), half)

    def back_order(i):
        return early_order(STEPS - 1 - i)

    def load_two(p, half):
        late = p // RING
        load((1 - late) * early_order(p + RING - late * RING) + late * back_order(p - late * RING), lax.rem(p, RING), half)

    two[...] = jnp.zeros_like(two)
    with jax.named_scope('consume'):
        aggregate(two, take_two(0, 0))
        load_two(0, 0)
        gather_take(h_buf, sems_h, 0)
        aggregate(two, take_two(0, 1))
        load_two(0, 1)
    with jax.named_scope('arrive'):
        gather_arrive(h_buf, sems_h, 1, 3)
    with jax.named_scope('consume'):
        aggregate(two, take_two(1, 0))
        load_two(1, 0)

    for p in range(2, STEPS):
        with jax.named_scope('arrive'):
            gather_arrive(h_buf, sems_h, early_order(p), 3)
            gather_take(h_buf, sems_h, early_order(p - 1))
        with jax.named_scope('consume'):
            aggregate(two, take_two(p - 1, 1) + take_two(p, 0))
            load_two(p - 1, 1)
            load_two(p, 0)
    with jax.named_scope('last'):
        gather_take(h_buf, sems_h, STEPS - 1)
        aggregate(two, take_two(STEPS - 1, 1))
        load_two(STEPS - 1, 1)
    with jax.named_scope('soft'):
        wait_all(count.at[pl.ds(0, n - 1)], count_send, count_recv)
        labelled = jnp.sum(count[...], axis=0)[0:1, 0:1]
        s_two = two[...].astype(jnp.bfloat16)
        w_two = w2t_ref[...].astype(jnp.bfloat16)
        logits = jnp.dot(w_two, s_two, preferred_element_type=jnp.float32)
        shifted = logits - jnp.max(logits, axis=0, keepdims=True)
        log_prob = shifted - jnp.log(jnp.sum(jnp.exp(shifted), axis=0, keepdims=True))
        hot = lax.broadcasted_iota(jnp.int32, logits.shape, 0) == y_ref[...]
        grad = (weight * (jnp.exp(log_prob) - hot.astype(jnp.float32)) / labelled).astype(jnp.bfloat16)
        u_two[...] = lax.dot_general(w_two, grad, ROW_CONTRACT, preferred_element_type=jnp.float32).astype(jnp.bfloat16)
        g_two[...] = grad
        picked[...] = -weight * jnp.sum(jnp.where(hot, log_prob, 0.0), axis=0, keepdims=True)
    classes = g_two.shape[0]
    edge = small.shape[0] - 8
    owners = small.shape[0] // 8
    tile = pl.ds(pl.multiple_of(me * 8, 8), 8)

    def send_small():
        loss = jnp.sum(picked[...], axis=1, keepdims=True)
        labelled = jnp.sum(count[...], axis=0)[0:1, 0:1]
        small[0:classes] = lax.dot_general(g_two[...], two[...].astype(jnp.bfloat16), COL_CONTRACT, preferred_element_type=jnp.float32)
        small[classes:edge] = jnp.zeros((edge - classes, hidden), jnp.float32)
        small[edge:] = jnp.broadcast_to(loss / labelled, (8, hidden))
        for o in range(owners):
            @pl.when(me != o)
            def _():
                remote(small.at[pl.ds(o * 8, 8)], small_parts.at[me], ssend, srecv, o).start()

    def to_partner(s, t):
        return remote(stage.at[s, t], total.at[s, t], dsend, drecv.at[s], partner)

    def to_parent(s, t, k):
        return remote(total.at[s, t], child.at[s - 1, t], csend, crecv.at[s - 1, t], neighbour(t, k, core, chip))

    def reduce_small():
        @pl.when(me < owners)
        def _():
            small_parts[me] = small[tile]
            got = small_parts.at[pl.ds(0, n - 1)]
            remote(got, got, ssend, srecv, partner).wait_recv()
            small_whole[tile] = jnp.sum(small_parts[...], axis=0)
            for i in range(1, n):
                remote(small_whole.at[tile], small_whole.at[tile], bsend, brecv, lax.rem(me + i, n)).start()

    def finish_small():
        sent = small_parts.at[pl.ds(0, n - 1)]
        fewer, every = small_whole.at[pl.ds(0, owners * 8 - 8)], small_whole.at[pl.ds(0, owners * 8)]

        @pl.when(me < owners)
        def _():
            remote(sent, sent, bsend, brecv, partner).wait_send()
            remote(fewer, fewer, ssend, brecv, partner).wait_send()
            remote(fewer, fewer, ssend, brecv, partner).wait_recv()

        @pl.when(me >= owners)
        def _():
            remote(every, every, ssend, brecv, partner).wait_send()
            remote(every, every, ssend, brecv, partner).wait_recv()

    def give(s, slot):
        loaded(slot, 1)
        for t in range(TREES):
            stage[s, t] = jnp.dot(u_two[...], ring[slot * 8 + TREES + t], preferred_element_type=jnp.float32)
        for t in range(TREES):
            to_partner(s, t).start()
        loaded(slot, 0)
        for t in range(TREES):
            mine[t] = jnp.dot(u_two[...], ring[slot * 8 + t], preferred_element_type=jnp.float32)

    def join(s):
        remote(total.at[s], total.at[s], dsend, drecv.at[s], partner).wait_recv()

    def gather_children(s, t):
        total[s, t] = total[s, t] + mine[t]
        for k in range(3):
            @pl.when(s < 2 ** k)
            def _():
                to_parent(s + 2 ** k, t, k).wait_recv()
                total[s, t] = total[s, t] + child[s + 2 ** k - 1, t]

    def step_back(i, carry):
        s = back_order(i)
        slot = lax.rem(i, RING)
        with jax.named_scope('give'):
            give(s, slot)

            @pl.when(i + RING < STEPS)
            def _():
                load(back_order(i + RING), slot, 1)
                load(back_order(i + RING), slot, 0)

            @pl.when(i == 0)
            def _():
                send_small()
        with jax.named_scope('take'):
            join(s)
            for t in range(TREES):
                gather_children(s, t)
                for k in range(3):
                    @pl.when((s >= 2 ** k) & (s < 2 ** (k + 1)))
                    def _():
                        to_parent(s, t, k).start()
        return carry

    lax.fori_loop(0, STEPS - 1, step_back, 0)
    chips = n // 2
    half, share = part.shape[0] // 2, part.shape[0] // n
    mine_rows = pl.ds(pl.multiple_of(core * half, 8), half)
    their_rows = pl.ds(pl.multiple_of((1 - core) * half, 8), half)
    most = slice(0, (TREES - 1) * width)
    with jax.named_scope('give'):
        give(0, (STEPS - 1) % RING)
        join(0)

    def hidden_grad(t):
        gather_children(0, t)
        g_one[:, chunks[t]] = jnp.where(z_one[:, chunks[t]] > 0.0, total[0, t], 0.0).astype(jnp.bfloat16)

    def weight_grad(out_rows, cols):
        return lax.dot_general(s_one[out_rows, cols], g_one[:, cols], COL_CONTRACT, preferred_element_type=jnp.float32)

    with jax.named_scope('take'):
        for t in range(TREES - 1):
            hidden_grad(t)
        part[...] = weight_grad(slice(None), most)
        hidden_grad(TREES - 1)
    with jax.named_scope('dw'):
        part[their_rows] = part[their_rows] + weight_grad(their_rows, chunks[-1])
        over = remote(part.at[their_rows], pair, psend, precv, partner)
        over.start()
        part[mine_rows] = part[mine_rows] + weight_grad(mine_rows, chunks[-1])
    reduce_small()
    with jax.named_scope('drain'):
        gather_drain(buf, sems_x)
        gather_drain(h_buf, sems_h)
        remote(stage, stage, dsend, drecv.at[0], partner).wait_send()
        remote(child, child, csend, crecv.at[0, 0], partner).wait_send()
    with jax.named_scope('pair'):
        over.wait()
        pair[...] = pair[...] + part[mine_rows]

    def share_of(q):
        return pl.ds(pl.multiple_of(q * share, 8), share)

    for i in range(1, chips):
        to = lax.rem(chip + i, chips)
        remote(pair.at[share_of(to)], parts.at[chip], fsend, frecv, to * 2 + core).start()
    parts[chip] = pair[share_of(chip)]
    with jax.named_scope('red'):
        wait_all(parts.at[pl.ds(0, chips - 1)], fsend, frecv)
    own = whole.at[pl.ds(pl.multiple_of(core * half + chip * share, 8), share)]
    own[...] = jnp.sum(parts[...], axis=0)
    for i in range(1, chips):
        remote(own, own, gsend, grecv, lax.rem(chip + i, chips) * 2 + core).start()
    with jax.named_scope('spread'):
        wait_all(whole.at[pl.ds(0, (chips - 1) * share)], gsend, grecv)
    swap = remote(whole.at[mine_rows], whole.at[mine_rows], qsend, qrecv, partner)
    swap.start()
    finish_small()
    dw2_ref[...] = small_whole[0:dw2_ref.shape[0]]
    loss_ref[...] = small_whole[edge:edge + 8]
    with jax.named_scope('swap'):
        swap.wait()
    dw_ref[...] = whole[0:feats]


def finish_kernel(loss_in, dw_in, dw2_in, loss_ref, dw_ref, dw2_ref):
    loss_ref[...] = loss_in[0:1, 0:1]
    dw_ref[...] = dw_in[...]
    dw2_ref[...] = dw2_in[...]


def train_step(x_rows, w_one, w2t, labels, mask, adj):
    rows, nodes = adj.shape
    n = nodes // rows
    feats, width = x_rows.shape[0], rows // TREES
    classes, hidden = w2t.shape
    units = n * TREES
    small = -(-classes // 8) * 8 + 8
    share = -(-feats // (8 * n)) * 8
    vmem, hbm = pl.BlockSpec(memory_space=pltpu.VMEM), pl.BlockSpec(memory_space=pl.ANY)
    dma, f32, bf16 = pltpu.SemaphoreType.DMA, jnp.float32, jnp.bfloat16
    block = (TREES, hidden, width)
    loss, dw_one, dw_two = pl.pallas_call(
        functools.partial(step_kernel, n),
        name='step',
        out_shape=(pltpu.VMEM((8, hidden), f32), pltpu.VMEM((feats, hidden), f32), pltpu.VMEM((classes, hidden), f32)),
        in_specs=[hbm, hbm, vmem, vmem, vmem, hbm],
        out_specs=(vmem,) * 3,
        scratch_shapes=[
            pltpu.VMEM((RING * 8, rows, width), bf16), pltpu.VMEM((units, feats, width), bf16), pltpu.VMEM((feats, rows), f32),
            pltpu.VMEM((units, hidden, width), bf16), pltpu.VMEM((n * share, rows), bf16), pltpu.VMEM((hidden, rows), f32),
            pltpu.VMEM((hidden, rows), bf16), pltpu.VMEM((feats, hidden), f32), pltpu.VMEM((small, hidden), f32), pltpu.VMEM((n, 8, 128), f32),
            pltpu.VMEM((STEPS, *block), f32), pltpu.VMEM(block, f32), pltpu.VMEM((STEPS, *block), f32), pltpu.VMEM((STEPS - 1, *block), f32),
            pltpu.VMEM((n * share, hidden), f32), pltpu.VMEM((n // 2, share, hidden), f32), pltpu.VMEM((n * share, hidden), f32),
            pltpu.VMEM((n, 8, hidden), f32), pltpu.VMEM((small, hidden), f32), pltpu.VMEM((n // 2 * share, hidden), f32),
            pltpu.VMEM((classes, rows), bf16), pltpu.VMEM((hidden, rows), bf16), pltpu.VMEM((1, rows), f32),
            dma((RING, 2)), dma, dma, dma, dma, dma, dma((STEPS,)), dma, dma((STEPS - 1, TREES)), *[dma] * 12, *gather_sems(), *gather_sems()],
        compiler_params=pltpu.CompilerParams(collective_id=0, has_side_effects=True, vmem_limit_bytes=62000000),
        cost_estimate=pl.CostEstimate(flops=2 * rows * nodes * (feats + 2 * hidden), bytes_accessed=6 * rows * nodes, transcendentals=0),
    )(x_rows, w_one, w2t, labels, mask, adj)
    return pl.pallas_call(
        finish_kernel,
        name='finish',
        out_shape=(jax.ShapeDtypeStruct((1, 1), f32), jax.ShapeDtypeStruct((feats, hidden), f32), jax.ShapeDtypeStruct((classes, hidden), f32)),
        in_specs=[vmem] * 3,
        out_specs=(vmem,) * 3,
    )(*[pltpu.with_memory_space_constraint(x, pltpu.VMEM) for x in (loss, dw_one, dw_two)])


def solution(mesh):
    axis_name = AXIS

    def local_step(adj_rows, feat_rows, w_one, w_two, label_rows, mask_rows):
        rows = adj_rows.shape[0]
        loss, dw_one, dw_two = train_step(feat_rows.T, w_one, w_two.T, label_rows.reshape(1, rows), mask_rows.reshape(1, rows), adj_rows)
        return loss.reshape(1), dw_one, dw_two.T

    return jax.shard_map(local_step, mesh=mesh, in_specs=(P(axis_name, None), P(axis_name, None), P(None, None), P(None, None), P(axis_name), P(axis_name)), out_specs=(P(None), P(None, None), P(None, None)), check_vma=False)
```

```python
import functools

import jax
import jax.numpy as jnp
from jax import lax
from jax.experimental import pallas as pl
from jax.experimental.pallas import tpu as pltpu
from jax.sharding import PartitionSpec as P

MESH = pl.DeviceIdType.MESH
AXIS = 'nodes'
TREES = 4
RING = 4
STEPS = 8
COL_CONTRACT = (((1,), (1,)), ((), ()))
ROW_CONTRACT = (((0,), (0,)), ((), ()))


def tree_axis(tree, k, core, chip):
    if tree < 3:
        weight = 2 ** ((tree + k) % 3)
        return weight, lax.rem(chip // weight, 2)
    weight = (1 - core) * 2 ** k + core * 2 ** (2 - k)
    low, high = lax.rem(chip // 2 ** k, 2), lax.rem(chip // 2 ** (2 - k), 2)
    return weight, (1 - core) * low + core * high


def chip_at(tree, offset, core, chip):
    out = chip
    for k in range(3):
        weight, bit = tree_axis(tree, k, core, chip)
        out = out + lax.rem(offset // 2 ** k, 2) * weight * (1 - 2 * bit)
    return out


def early_order(place):
    pair = (place + 1) // 2
    return place + (pair * (4 - pair)) // 4 * (7 - 2 * place)


def unit_at(tree, offset, core, chip):
    return (chip_at(tree, offset, core, chip) * 2 + core) * TREES + tree


def neighbour(tree, k, core, chip):
    weight, bit = tree_axis(tree, k, core, chip)
    return (chip + weight * (1 - 2 * bit)) * 2 + core


def remote(src, dst, send_sem, recv_sem, device):
    return pltpu.make_async_remote_copy(src_ref=src, dst_ref=dst, send_sem=send_sem, recv_sem=recv_sem, device_id=(device,), device_id_type=MESH)


def place():
    me = lax.axis_index(AXIS)
    core, chip = lax.rem(me, 2), me // 2
    return me, core, chip, chip * 2 + 1 - core


def gather_send(buf, sems, tree, offset, k, unit, rows=slice(None)):
    send, recv, hand = sems
    me, core, chip, partner = place()
    ref = buf.at[unit, rows]
    remote(ref, ref, send, recv.at[offset + 2 ** k - 1, tree], neighbour(tree, k, core, chip)).start()


def gather_hand(buf, sems, slot, unit):
    send, recv, hand = sems
    me, core, chip, partner = place()
    remote(buf.at[unit], buf.at[unit], send, hand.at[slot], partner).start()


def gather_start(buf, sems, links):
    me = lax.axis_index(AXIS)
    for k in range(links):
        for t in range(TREES):
            gather_send(buf, sems, t, 0, k, me * TREES + t)
        if k == 0:
            for t in range(TREES):
                gather_hand(buf, sems, 0, me * TREES + t)


def gather_arrive(buf, sems, s, links, trees=range(TREES), slot=None, cut=None):
    send, recv, hand = sems
    me, core, chip, partner = place()
    units = {t: unit_at(t, s, core, chip) for t in trees}
    for t, u in units.items():
        remote(buf.at[u], buf.at[u], send, recv.at[s - 1, t], partner).wait_recv()
        split = cut is not None and t == TREES - 1

        @pl.when(s == 1)
        def _():
            gather_send(buf, sems, t, s, 1, u)

        @pl.when((s > 1) & (s < (3 if split else 4)))
        def _():
            gather_send(buf, sems, t, s, 2, u)
        if split:
            @pl.when(s == 3)
            def _():
                gather_send(buf, sems, t, s, 2, u, slice(0, cut))

            @pl.when(s == 5)
            def _():
                gather_send(buf, sems, t, s, 1, u, slice(cut, None))
        gather_hand(buf, sems, s if slot is None else slot, u)

    @pl.when(s == 1)
    def _():
        if links < 3:
            for t in range(TREES):
                gather_send(buf, sems, t, 0, 2, me * TREES + t)
        for t, u in units.items():
            gather_send(buf, sems, t, s, 2, u)


def gather_take(buf, sems, slot, count=TREES):
    send, recv, hand = sems
    me, core, chip, partner = place()
    units = buf.at[pl.ds(0, count)]
    remote(units, units, send, hand.at[slot], partner).wait_recv()


def gather_drain(buf, sems):
    send, recv, hand = sems
    me, core, chip, partner = place()
    sent = buf.at[pl.ds(0, TREES * (STEPS - 1 + STEPS))]
    remote(sent, sent, send, hand.at[0], partner).wait_send()


def gather_sems():
    dma = pltpu.SemaphoreType.DMA
    return [dma, dma((STEPS - 1, TREES)), dma((STEPS + 1,))]


def barrier_near():
    me, core, chip, partner = place()
    sem = pltpu.get_barrier_semaphore()
    pl.semaphore_signal(sem, inc=1, device_id=(partner,), device_id_type=MESH)
    for k in range(3):
        pl.semaphore_signal(sem, inc=1, device_id=(neighbour(0, k, core, chip),), device_id_type=MESH)
    pl.semaphore_wait(sem, 4)


def send_all(n, src, dst, send_sem, recv_sem):
    me = lax.axis_index(AXIS)
    for i in range(1, n):
        to = lax.rem(me + i, n)
        remote(src(to), dst, send_sem, recv_sem, to).start()


def wait_all(ref, send_sem, recv_sem):
    me, core, chip, partner = place()
    copy = remote(ref, ref, send_sem, recv_sem, partner)
    copy.wait_send()
    copy.wait_recv()


def step_kernel(n, x_ref, w_hbm, w2t_ref, y_ref, m_ref, adj, loss_ref, dw_ref, dw2_ref,
                ring, buf, acc, h_buf, s_one, z_one, u_two, w_v, small, count, stage, mine, total, child, part, parts, whole,
                small_parts, small_whole, pair, g_two, g_one, picked,
                ring_sem, x_sem, w_sem, count_send, count_recv, dsend, drecv, csend, crecv, fsend, frecv, gsend, grecv,
                ssend, srecv, bsend, brecv, psend, precv, qsend, qrecv, cut_sem, *sems):
    me, core, chip, partner = place()
    sems_x, sems_h = sems[:3], sems[3:]
    width = buf.shape[2]
    feats, rows = acc.shape
    hidden = h_buf.shape[1]
    chunks = [slice(t * width, (t + 1) * width) for t in range(TREES)]

    def slab(s, slot, j):
        u = unit_at(j % TREES, s, core if j < TREES else 1 - core, chip)
        return pltpu.make_async_copy(adj.at[:, pl.ds(pl.multiple_of(u * width, width), width)], ring.at[slot * 8 + j], ring_sem.at[slot, j // TREES])

    def load(s, slot, half):
        for t in range(TREES):
            slab(s, slot, half * TREES + t).start()

    def loaded(slot, half):
        four = ring.at[pl.ds(0, TREES)]
        pltpu.make_async_copy(four, four, ring_sem.at[slot, half]).wait()

    with jax.named_scope('start'):
        fetch = [pltpu.make_async_copy(x_ref.at[:, pl.ds(t * width, width)], buf.at[me * TREES + t], x_sem) for t in range(TREES)]
        for copy in fetch:
            copy.start()
        weight = m_ref[...].astype(jnp.float32)
        count[me] = jnp.broadcast_to(jnp.sum(weight, axis=1, keepdims=True), count.shape[1:])
        barrier_near()
        four = buf.at[pl.ds(0, TREES)]
        pltpu.make_async_copy(four, four, x_sem).wait()
    gather_start(buf, sems_x, 2)
    weights = pltpu.make_async_copy(w_hbm, w_v, w_sem)
    weights.start()
    for s in range(RING):
        for half in range(2):
            load(s, s, half)
    acc[...] = jnp.zeros_like(acc)

    def terms(units_ref, s, slot, half, trees=range(TREES)):
        which = core if half == 0 else 1 - core
        return [(units_ref, unit_at(t, s, which, chip), slot * 8 + half * TREES + t) for t in trees]

    def aggregate(out, pairs):
        for cols in chunks:
            out[:, cols] += sum(lax.dot_general(ref[u], ring[j, cols], COL_CONTRACT, preferred_element_type=jnp.float32) for ref, u, j in pairs)

    def step_one(s, carry):
        with jax.named_scope('arrive'):
            @pl.when(s > 0)
            def _():
                gather_arrive(buf, sems_x, s, 2, cut=cut)
        for half in range(2):
            with jax.named_scope('consume'):
                if half == 1:
                    gather_take(buf, sems_x, s)
                slot = lax.rem(s, RING)
                loaded(slot, half)
                aggregate(acc, terms(buf, s, slot, half))
                late = s // RING
                load((1 - late) * (s + RING) + late * early_order(s - late * RING), slot, half)
        return carry

    cut = feats * 2 // 3 // 16 * 16
    final, slot = STEPS - 1, (STEPS - 1) % RING
    lax.fori_loop(0, final, step_one, 0)
    early, late = (range(TREES - 1), final), (range(TREES - 1, TREES), STEPS)
    for half in range(2):
        for trees, hand in (early, late):
            with jax.named_scope('consume'):
                if half == 0:
                    gather_arrive(buf, sems_x, final, 2, trees, hand, cut)
                else:
                    gather_take(buf, sems_x, hand, len(trees))
                if hand == final:
                    loaded(slot, half)
                aggregate(acc, terms(buf, final, slot, half, trees))
    for half in range(2):
        load(early_order(final - RING), slot, half)
    with jax.named_scope('mid'):
        weights.wait()
        s_one[0:feats] = acc[...].astype(jnp.bfloat16)
        s_one[feats:] = jnp.zeros_like(s_one[feats:])
        w_rows = w_v[...].astype(jnp.bfloat16)
        for t, cols in enumerate(chunks):
            z = lax.dot_general(w_rows, s_one[0:feats, cols], ROW_CONTRACT, preferred_element_type=jnp.float32)
            z_one[:, cols] = z
            h_buf[me * TREES + t] = jnp.maximum(z, 0.0).astype(jnp.bfloat16)
    gather_start(h_buf, sems_h, 3)
    send_all(n, lambda to: count.at[me], count.at[me], count_send, count_recv)
    two = acc.at[0:hidden]

    def take_two(p, half):
        loaded(lax.rem(p, RING), half)
        return terms(h_buf, early_order(p), lax.rem(p, RING), half)

    def back_order(i):
        return early_order(STEPS - 1 - i)

    def load_two(p, half):
        late = p // RING
        load((1 - late) * early_order(p + RING - late * RING) + late * back_order(p - late * RING), lax.rem(p, RING), half)

    two[...] = jnp.zeros_like(two)
    with jax.named_scope('consume'):
        aggregate(two, take_two(0, 0))
        load_two(0, 0)
        gather_take(h_buf, sems_h, 0)
        aggregate(two, take_two(0, 1))
        load_two(0, 1)
    with jax.named_scope('arrive'):
        gather_arrive(h_buf, sems_h, 1, 3)
    with jax.named_scope('consume'):
        aggregate(two, take_two(1, 0))
        load_two(1, 0)

    for p in range(2, STEPS):
        with jax.named_scope('arrive'):
            gather_arrive(h_buf, sems_h, early_order(p), 3)
            gather_take(h_buf, sems_h, early_order(p - 1))
        with jax.named_scope('consume'):
            aggregate(two, take_two(p - 1, 1) + take_two(p, 0))
            load_two(p - 1, 1)
            load_two(p, 0)
    with jax.named_scope('last'):
        gather_take(h_buf, sems_h, STEPS - 1)
        aggregate(two, take_two(STEPS - 1, 1))
        load_two(STEPS - 1, 1)
    with jax.named_scope('soft'):
        wait_all(count.at[pl.ds(0, n - 1)], count_send, count_recv)
        labelled = jnp.sum(count[...], axis=0)[0:1, 0:1]
        s_two = two[...].astype(jnp.bfloat16)
        w_two = w2t_ref[...].astype(jnp.bfloat16)
        logits = jnp.dot(w_two, s_two, preferred_element_type=jnp.float32)
        shifted = logits - jnp.max(logits, axis=0, keepdims=True)
        log_prob = shifted - jnp.log(jnp.sum(jnp.exp(shifted), axis=0, keepdims=True))
        hot = lax.broadcasted_iota(jnp.int32, logits.shape, 0) == y_ref[...]
        grad = (weight * (jnp.exp(log_prob) - hot.astype(jnp.float32)) / labelled).astype(jnp.bfloat16)
        u_two[...] = lax.dot_general(w_two, grad, ROW_CONTRACT, preferred_element_type=jnp.float32).astype(jnp.bfloat16)
        g_two[...] = grad
        picked[...] = -weight * jnp.sum(jnp.where(hot, log_prob, 0.0), axis=0, keepdims=True)
    classes = g_two.shape[0]
    edge = small.shape[0] - 8
    owners = small.shape[0] // 8
    tile = pl.ds(pl.multiple_of(me * 8, 8), 8)

    def send_small():
        loss = jnp.sum(picked[...], axis=1, keepdims=True)
        labelled = jnp.sum(count[...], axis=0)[0:1, 0:1]
        small[0:classes] = lax.dot_general(g_two[...], two[...].astype(jnp.bfloat16), COL_CONTRACT, preferred_element_type=jnp.float32)
        small[classes:edge] = jnp.zeros((edge - classes, hidden), jnp.float32)
        small[edge:] = jnp.broadcast_to(loss / labelled, (8, hidden))
        for o in range(owners):
            @pl.when(me != o)
            def _():
                remote(small.at[pl.ds(o * 8, 8)], small_parts.at[me], ssend, srecv, o).start()

    def to_partner(s, t):
        return remote(stage.at[s, t], total.at[s, t], dsend, drecv.at[s], partner)

    def to_parent(s, t, k):
        return remote(total.at[s, t], child.at[s - 1, t], csend, crecv.at[s - 1, t], neighbour(t, k, core, chip))

    def reduce_small():
        @pl.when(me < owners)
        def _():
            small_parts[me] = small[tile]
            got = small_parts.at[pl.ds(0, n - 1)]
            remote(got, got, ssend, srecv, partner).wait_recv()
            small_whole[tile] = jnp.sum(small_parts[...], axis=0)
            for i in range(1, n):
                remote(small_whole.at[tile], small_whole.at[tile], bsend, brecv, lax.rem(me + i, n)).start()

    def finish_small():
        sent = small_parts.at[pl.ds(0, n - 1)]
        fewer, every = small_whole.at[pl.ds(0, owners * 8 - 8)], small_whole.at[pl.ds(0, owners * 8)]

        @pl.when(me < owners)
        def _():
            remote(sent, sent, bsend, brecv, partner).wait_send()
            remote(fewer, fewer, ssend, brecv, partner).wait_send()
            remote(fewer, fewer, ssend, brecv, partner).wait_recv()

        @pl.when(me >= owners)
        def _():
            remote(every, every, ssend, brecv, partner).wait_send()
            remote(every, every, ssend, brecv, partner).wait_recv()

    far, edge_row = STEPS - 2, hidden * 2 // 3 // 8 * 8 + 8

    def from_far_to(which):
        rows, k = ((slice(0, edge_row), 2), (slice(edge_row, hidden), 1))[which]
        sem = cut_sem if which else crecv.at[far - 1, TREES - 1]
        return remote(total.at[far, TREES - 1, rows], child.at[far - 1, TREES - 1, rows], csend, sem, neighbour(TREES - 1, k, core, chip))

    def add_far(s, which):
        from_far_to(which).wait_recv()
        rows = (slice(0, edge_row), slice(edge_row, hidden))[which]
        total[s, TREES - 1, rows] = total[s, TREES - 1, rows] + child[far - 1, TREES - 1, rows]

    def give(s, slot):
        loaded(slot, 1)
        for t in range(TREES):
            stage[s, t] = jnp.dot(u_two[...], ring[slot * 8 + TREES + t], preferred_element_type=jnp.float32)
        for t in range(TREES):
            to_partner(s, t).start()
        loaded(slot, 0)
        for t in range(TREES):
            mine[t] = jnp.dot(u_two[...], ring[slot * 8 + t], preferred_element_type=jnp.float32)

    def join(s):
        remote(total.at[s], total.at[s], dsend, drecv.at[s], partner).wait_recv()

    def gather_children(s, t):
        total[s, t] = total[s, t] + mine[t]
        for k in range(3):
            skip = far - 4 if k == 2 and t == TREES - 1 else STEPS

            @pl.when((s < 2 ** k) & (s != skip))
            def _():
                to_parent(s + 2 ** k, t, k).wait_recv()
                total[s, t] = total[s, t] + child[s + 2 ** k - 1, t]
        if t == TREES - 1:
            for which, parent in ((0, far - 4), (1, far - 2)):
                @pl.when(s == parent)
                def _():
                    add_far(s, which)

    def step_back(i, carry):
        s = back_order(i)
        slot = lax.rem(i, RING)
        with jax.named_scope('give'):
            give(s, slot)

            @pl.when(i + RING < STEPS)
            def _():
                load(back_order(i + RING), slot, 1)
                load(back_order(i + RING), slot, 0)

            @pl.when(i == 0)
            def _():
                send_small()
        with jax.named_scope('take'):
            join(s)
            for t in range(TREES):
                gather_children(s, t)
                for k in range(3):
                    skip = far if k == 2 and t == TREES - 1 else STEPS

                    @pl.when((s >= 2 ** k) & (s < 2 ** (k + 1)) & (s != skip))
                    def _():
                        to_parent(s, t, k).start()
                if t == TREES - 1:
                    @pl.when(s == far)
                    def _():
                        from_far_to(0).start()
                        from_far_to(1).start()
        return carry

    lax.fori_loop(0, STEPS - 1, step_back, 0)
    chips = n // 2
    half, share = part.shape[0] // 2, part.shape[0] // n
    mine_rows = pl.ds(pl.multiple_of(core * half, 8), half)
    their_rows = pl.ds(pl.multiple_of((1 - core) * half, 8), half)
    most = slice(0, (TREES - 1) * width)
    with jax.named_scope('give'):
        give(0, (STEPS - 1) % RING)
        join(0)

    def hidden_grad(t):
        gather_children(0, t)
        g_one[:, chunks[t]] = jnp.where(z_one[:, chunks[t]] > 0.0, total[0, t], 0.0).astype(jnp.bfloat16)

    def weight_grad(out_rows, cols):
        return lax.dot_general(s_one[out_rows, cols], g_one[:, cols], COL_CONTRACT, preferred_element_type=jnp.float32)

    with jax.named_scope('take'):
        for t in range(TREES - 1):
            hidden_grad(t)
        part[...] = weight_grad(slice(None), most)
        hidden_grad(TREES - 1)
    with jax.named_scope('dw'):
        part[their_rows] = part[their_rows] + weight_grad(their_rows, chunks[-1])
        over = remote(part.at[their_rows], pair, psend, precv, partner)
        over.start()
        part[mine_rows] = part[mine_rows] + weight_grad(mine_rows, chunks[-1])
    reduce_small()
    with jax.named_scope('drain'):
        gather_drain(buf, sems_x)
        gather_drain(h_buf, sems_h)
        remote(stage, stage, dsend, drecv.at[0], partner).wait_send()
        remote(child, child, csend, crecv.at[0, 0], partner).wait_send()
    with jax.named_scope('pair'):
        over.wait()
        pair[...] = pair[...] + part[mine_rows]

    def share_of(q):
        return pl.ds(pl.multiple_of(q * share, 8), share)

    for i in range(1, chips):
        to = lax.rem(chip + i, chips)
        remote(pair.at[share_of(to)], parts.at[chip], fsend, frecv, to * 2 + core).start()
    parts[chip] = pair[share_of(chip)]
    with jax.named_scope('red'):
        wait_all(parts.at[pl.ds(0, chips - 1)], fsend, frecv)
    own = whole.at[pl.ds(pl.multiple_of(core * half + chip * share, 8), share)]
    own[...] = jnp.sum(parts[...], axis=0)
    for i in range(1, chips):
        remote(own, own, gsend, grecv, lax.rem(chip + i, chips) * 2 + core).start()
    with jax.named_scope('spread'):
        wait_all(whole.at[pl.ds(0, (chips - 1) * share)], gsend, grecv)
    swap = remote(whole.at[mine_rows], whole.at[mine_rows], qsend, qrecv, partner)
    swap.start()
    finish_small()
    dw2_ref[...] = small_whole[0:dw2_ref.shape[0]]
    loss_ref[...] = small_whole[edge:edge + 8]
    with jax.named_scope('swap'):
        swap.wait()
    dw_ref[...] = whole[0:feats]


def finish_kernel(loss_in, dw_in, dw2_in, loss_ref, dw_ref, dw2_ref):
    loss_ref[...] = loss_in[0:1, 0:1]
    dw_ref[...] = dw_in[...]
    dw2_ref[...] = dw2_in[...]


def train_step(x_rows, w_one, w2t, labels, mask, adj):
    rows, nodes = adj.shape
    n = nodes // rows
    feats, width = x_rows.shape[0], rows // TREES
    classes, hidden = w2t.shape
    units = n * TREES
    small = -(-classes // 8) * 8 + 8
    share = -(-feats // (8 * n)) * 8
    vmem, hbm = pl.BlockSpec(memory_space=pltpu.VMEM), pl.BlockSpec(memory_space=pl.ANY)
    dma, f32, bf16 = pltpu.SemaphoreType.DMA, jnp.float32, jnp.bfloat16
    block = (TREES, hidden, width)
    loss, dw_one, dw_two = pl.pallas_call(
        functools.partial(step_kernel, n),
        name='step',
        out_shape=(pltpu.VMEM((8, hidden), f32), pltpu.VMEM((feats, hidden), f32), pltpu.VMEM((classes, hidden), f32)),
        in_specs=[hbm, hbm, vmem, vmem, vmem, hbm],
        out_specs=(vmem,) * 3,
        scratch_shapes=[
            pltpu.VMEM((RING * 8, rows, width), bf16), pltpu.VMEM((units, feats, width), bf16), pltpu.VMEM((feats, rows), f32),
            pltpu.VMEM((units, hidden, width), bf16), pltpu.VMEM((n * share, rows), bf16), pltpu.VMEM((hidden, rows), f32),
            pltpu.VMEM((hidden, rows), bf16), pltpu.VMEM((feats, hidden), f32), pltpu.VMEM((small, hidden), f32), pltpu.VMEM((n, 8, 128), f32),
            pltpu.VMEM((STEPS, *block), f32), pltpu.VMEM(block, f32), pltpu.VMEM((STEPS, *block), f32), pltpu.VMEM((STEPS - 1, *block), f32),
            pltpu.VMEM((n * share, hidden), f32), pltpu.VMEM((n // 2, share, hidden), f32), pltpu.VMEM((n * share, hidden), f32),
            pltpu.VMEM((n, 8, hidden), f32), pltpu.VMEM((small, hidden), f32), pltpu.VMEM((n // 2 * share, hidden), f32),
            pltpu.VMEM((classes, rows), bf16), pltpu.VMEM((hidden, rows), bf16), pltpu.VMEM((1, rows), f32),
            dma((RING, 2)), dma, dma, dma, dma, dma, dma((STEPS,)), dma, dma((STEPS - 1, TREES)), *[dma] * 13, *gather_sems(), *gather_sems()],
        compiler_params=pltpu.CompilerParams(collective_id=0, has_side_effects=True, vmem_limit_bytes=62000000),
        cost_estimate=pl.CostEstimate(flops=2 * rows * nodes * (feats + 2 * hidden), bytes_accessed=6 * rows * nodes, transcendentals=0),
    )(x_rows, w_one, w2t, labels, mask, adj)
    return pl.pallas_call(
        finish_kernel,
        name='finish',
        out_shape=(jax.ShapeDtypeStruct((1, 1), f32), jax.ShapeDtypeStruct((feats, hidden), f32), jax.ShapeDtypeStruct((classes, hidden), f32)),
        in_specs=[vmem] * 3,
        out_specs=(vmem,) * 3,
    )(*[pltpu.with_memory_space_constraint(x, pltpu.VMEM) for x in (loss, dw_one, dw_two)])


def solution(mesh):
    axis_name = AXIS

    def local_step(adj_rows, feat_rows, w_one, w_two, label_rows, mask_rows):
        rows = adj_rows.shape[0]
        loss, dw_one, dw_two = train_step(feat_rows.T, w_one, w_two.T, label_rows.reshape(1, rows), mask_rows.reshape(1, rows), adj_rows)
        return loss.reshape(1), dw_one, dw_two.T

    return jax.shard_map(local_step, mesh=mesh, in_specs=(P(axis_name, None), P(axis_name, None), P(None, None), P(None, None), P(axis_name), P(axis_name)), out_specs=(P(None), P(None, None), P(None, None)), check_vma=False)
```

```python
import functools

import jax
import jax.numpy as jnp
from jax import lax
from jax.experimental import pallas as pl
from jax.experimental.pallas import tpu as pltpu
from jax.sharding import PartitionSpec as P

MESH = pl.DeviceIdType.MESH
AXIS = 'nodes'
TREES = 4
RING = 4
STEPS = 8
COL_CONTRACT = (((1,), (1,)), ((), ()))
ROW_CONTRACT = (((0,), (0,)), ((), ()))


def tree_axis(tree, k, core, chip):
    if tree < 3:
        weight = 2 ** ((tree + k) % 3)
        return weight, lax.rem(chip // weight, 2)
    weight = (1 - core) * 2 ** k + core * 2 ** (2 - k)
    low, high = lax.rem(chip // 2 ** k, 2), lax.rem(chip // 2 ** (2 - k), 2)
    return weight, (1 - core) * low + core * high


def chip_at(tree, offset, core, chip):
    out = chip
    for k in range(3):
        weight, bit = tree_axis(tree, k, core, chip)
        out = out + lax.rem(offset // 2 ** k, 2) * weight * (1 - 2 * bit)
    return out


def early_order(place):
    pair = (place + 1) // 2
    return place + (pair * (4 - pair)) // 4 * (7 - 2 * place)


def unit_at(tree, offset, core, chip):
    return (chip_at(tree, offset, core, chip) * 2 + core) * TREES + tree


def neighbour(tree, k, core, chip):
    weight, bit = tree_axis(tree, k, core, chip)
    return (chip + weight * (1 - 2 * bit)) * 2 + core


def remote(src, dst, send_sem, recv_sem, device):
    return pltpu.make_async_remote_copy(src_ref=src, dst_ref=dst, send_sem=send_sem, recv_sem=recv_sem, device_id=(device,), device_id_type=MESH)


def place():
    me = lax.axis_index(AXIS)
    core, chip = lax.rem(me, 2), me // 2
    return me, core, chip, chip * 2 + 1 - core


def gather_send(buf, sems, tree, offset, k, unit, rows=slice(None), last=False):
    send, recv, late, hand = sems
    me, core, chip, partner = place()
    ref = buf.at[unit, rows]
    got = late.at[4] if last else late.at[offset] if k == 2 else recv.at[offset + 2 ** k - 1, tree]
    remote(ref, ref, send, got, neighbour(tree, k, core, chip)).start()


def gather_hand(buf, sems, slot, unit):
    send, recv, late, hand = sems
    me, core, chip, partner = place()
    remote(buf.at[unit], buf.at[unit], send, hand.at[slot], partner).start()


def gather_start(buf, sems, early):
    me = lax.axis_index(AXIS)
    for k in range(3):
        for t in range(TREES if k < 2 else early):
            gather_send(buf, sems, t, 0, k, me * TREES + t)
        if k == 0:
            for t in range(TREES):
                gather_hand(buf, sems, 0, me * TREES + t)


def gather_arrive(buf, sems, s, early, trees=range(TREES), slot=None, cut=None):
    send, recv, late, hand = sems
    me, core, chip, partner = place()
    units = {t: unit_at(t, s, core, chip) for t in trees}
    slot = s if slot is None else slot

    @pl.when(s < 4)
    def _():
        for t, u in units.items():
            remote(buf.at[u], buf.at[u], send, recv.at[s - 1, t], partner).wait_recv()
            split = cut is not None and t == TREES - 1

            @pl.when(s == 1)
            def _():
                gather_send(buf, sems, t, s, 1, u)

            @pl.when((s > 1) & (s < (3 if split else 4)))
            def _():
                gather_send(buf, sems, t, s, 2, u)
            if split:
                @pl.when(s == 3)
                def _():
                    gather_send(buf, sems, t, s, 2, u, slice(0, cut), True)
            gather_hand(buf, sems, slot, u)

    @pl.when(s >= 4)
    def _():
        some = buf.at[pl.ds(0, len(units))]
        which = late.at[s - 4] if len(units) > 1 else late.at[4]
        remote(some, some, send, which, partner).wait_recv()
        if cut is not None and TREES - 1 in units:
            @pl.when(s == 5)
            def _():
                gather_send(buf, sems, TREES - 1, s, 1, units[TREES - 1], slice(cut, None), True)
        for u in units.values():
            gather_hand(buf, sems, slot, u)

    @pl.when(s == 1)
    def _():
        for t in range(early, TREES):
            gather_send(buf, sems, t, 0, 2, me * TREES + t)
        for t, u in units.items():
            gather_send(buf, sems, t, s, 2, u)


def gather_take(buf, sems, slot, count=TREES):
    send, recv, late, hand = sems
    me, core, chip, partner = place()
    units = buf.at[pl.ds(0, count)]
    remote(units, units, send, hand.at[slot], partner).wait_recv()


def gather_drain(buf, sems):
    send, recv, late, hand = sems
    me, core, chip, partner = place()
    sent = buf.at[pl.ds(0, TREES * (STEPS - 1 + STEPS))]
    remote(sent, sent, send, hand.at[0], partner).wait_send()


def gather_sems():
    dma = pltpu.SemaphoreType.DMA
    return [dma, dma((3, TREES)), dma((5,)), dma((STEPS + 1,))]


def barrier_near():
    me, core, chip, partner = place()
    sem = pltpu.get_barrier_semaphore()
    pl.semaphore_signal(sem, inc=1, device_id=(partner,), device_id_type=MESH)
    for k in range(3):
        pl.semaphore_signal(sem, inc=1, device_id=(neighbour(0, k, core, chip),), device_id_type=MESH)
    pl.semaphore_wait(sem, 4)


def send_all(n, src, dst, send_sem, recv_sem):
    me = lax.axis_index(AXIS)
    for i in range(1, n):
        to = lax.rem(me + i, n)
        remote(src(to), dst, send_sem, recv_sem, to).start()


def wait_all(ref, send_sem, recv_sem):
    me, core, chip, partner = place()
    copy = remote(ref, ref, send_sem, recv_sem, partner)
    copy.wait_send()
    copy.wait_recv()


def step_kernel(n, x_ref, w_hbm, w2t_ref, y_ref, m_ref, adj, loss_ref, dw_ref, dw2_ref,
                ring, buf, acc, h_buf, s_one, z_one, u_two, w_v, small, count, stage, mine, total, child, part, parts, whole,
                small_parts, small_whole, pair, g_two, g_one, picked,
                ring_sem, x_sem, w_sem, count_send, count_recv, dsend, drecv, csend, crecv, fsend, frecv, gsend, grecv,
                ssend, srecv, bsend, brecv, psend, precv, qsend, qrecv, cut_sem, *sems):
    me, core, chip, partner = place()
    sems_x, sems_h = sems[:4], sems[4:]
    width = buf.shape[2]
    feats, rows = acc.shape
    hidden = h_buf.shape[1]
    chunks = [slice(t * width, (t + 1) * width) for t in range(TREES)]

    def slab(s, slot, j):
        u = unit_at(j % TREES, s, core if j < TREES else 1 - core, chip)
        return pltpu.make_async_copy(adj.at[:, pl.ds(pl.multiple_of(u * width, width), width)], ring.at[slot * 8 + j], ring_sem.at[slot, j // TREES])

    def load(s, slot, half):
        for t in range(TREES):
            slab(s, slot, half * TREES + t).start()

    def loaded(slot, half):
        four = ring.at[pl.ds(0, TREES)]
        pltpu.make_async_copy(four, four, ring_sem.at[slot, half]).wait()

    with jax.named_scope('start'):
        fetch = [pltpu.make_async_copy(x_ref.at[:, pl.ds(t * width, width)], buf.at[me * TREES + t], x_sem) for t in range(TREES)]
        for copy in fetch:
            copy.start()
        weight = m_ref[...].astype(jnp.float32)
        count[me] = jnp.broadcast_to(jnp.sum(weight, axis=1, keepdims=True), count.shape[1:])
        barrier_near()
        four = buf.at[pl.ds(0, TREES)]
        pltpu.make_async_copy(four, four, x_sem).wait()
    gather_start(buf, sems_x, 0)
    weights = pltpu.make_async_copy(w_hbm, w_v, w_sem)
    weights.start()
    for s in range(RING):
        for half in range(2):
            load(s, s, half)
    acc[...] = jnp.zeros_like(acc)

    def terms(units_ref, s, slot, half, trees=range(TREES)):
        which = core if half == 0 else 1 - core
        return [(units_ref, unit_at(t, s, which, chip), slot * 8 + half * TREES + t) for t in trees]

    def aggregate(out, pairs):
        for cols in chunks:
            out[:, cols] += sum(lax.dot_general(ref[u], ring[j, cols], COL_CONTRACT, preferred_element_type=jnp.float32) for ref, u, j in pairs)

    def step_one(s, carry):
        with jax.named_scope('arrive'):
            @pl.when(s > 0)
            def _():
                gather_arrive(buf, sems_x, s, 0, cut=cut)
        for half in range(2):
            with jax.named_scope('consume'):
                if half == 1:
                    gather_take(buf, sems_x, s)
                slot = lax.rem(s, RING)
                loaded(slot, half)
                aggregate(acc, terms(buf, s, slot, half))
                late = s // RING
                load((1 - late) * (s + RING) + late * early_order(s - late * RING), slot, half)
        return carry

    cut = feats * 2 // 3 // 16 * 16
    final, slot = STEPS - 1, (STEPS - 1) % RING
    lax.fori_loop(0, final, step_one, 0)
    early, late = (range(TREES - 1), final), (range(TREES - 1, TREES), STEPS)
    for half in range(2):
        for trees, hand in (early, late):
            with jax.named_scope('consume'):
                if half == 0:
                    gather_arrive(buf, sems_x, final, 0, trees, hand, cut)
                else:
                    gather_take(buf, sems_x, hand, len(trees))
                if hand == final:
                    loaded(slot, half)
                aggregate(acc, terms(buf, final, slot, half, trees))
    for half in range(2):
        load(early_order(final - RING), slot, half)
    with jax.named_scope('mid'):
        weights.wait()
        s_one[0:feats] = acc[...].astype(jnp.bfloat16)
        s_one[feats:] = jnp.zeros_like(s_one[feats:])
        w_rows = w_v[...].astype(jnp.bfloat16)
        for t, cols in enumerate(chunks):
            z = lax.dot_general(w_rows, s_one[0:feats, cols], ROW_CONTRACT, preferred_element_type=jnp.float32)
            z_one[:, cols] = z
            h_buf[me * TREES + t] = jnp.maximum(z, 0.0).astype(jnp.bfloat16)
    gather_start(h_buf, sems_h, TREES)
    send_all(n, lambda to: count.at[me], count.at[me], count_send, count_recv)
    two = acc.at[0:hidden]

    def take_two(p, half):
        loaded(lax.rem(p, RING), half)
        return terms(h_buf, early_order(p), lax.rem(p, RING), half)

    def back_order(i):
        return early_order(STEPS - 1 - i)

    def load_two(p, half):
        late = p // RING
        load((1 - late) * early_order(p + RING - late * RING) + late * back_order(p - late * RING), lax.rem(p, RING), half)

    two[...] = jnp.zeros_like(two)
    with jax.named_scope('consume'):
        aggregate(two, take_two(0, 0))
        load_two(0, 0)
        gather_take(h_buf, sems_h, 0)
        aggregate(two, take_two(0, 1))
        load_two(0, 1)
    with jax.named_scope('arrive'):
        gather_arrive(h_buf, sems_h, 1, TREES)
    with jax.named_scope('consume'):
        aggregate(two, take_two(1, 0))
        load_two(1, 0)

    for p in range(2, STEPS):
        with jax.named_scope('arrive'):
            gather_arrive(h_buf, sems_h, early_order(p), TREES)
            gather_take(h_buf, sems_h, early_order(p - 1))
        with jax.named_scope('consume'):
            aggregate(two, take_two(p - 1, 1) + take_two(p, 0))
            load_two(p - 1, 1)
            load_two(p, 0)
    with jax.named_scope('last'):
        gather_take(h_buf, sems_h, STEPS - 1)
        aggregate(two, take_two(STEPS - 1, 1))
        load_two(STEPS - 1, 1)
    with jax.named_scope('soft'):
        wait_all(count.at[pl.ds(0, n - 1)], count_send, count_recv)
        labelled = jnp.sum(count[...], axis=0)[0:1, 0:1]
        s_two = two[...].astype(jnp.bfloat16)
        w_two = w2t_ref[...].astype(jnp.bfloat16)
        logits = jnp.dot(w_two, s_two, preferred_element_type=jnp.float32)
        shifted = logits - jnp.max(logits, axis=0, keepdims=True)
        log_prob = shifted - jnp.log(jnp.sum(jnp.exp(shifted), axis=0, keepdims=True))
        hot = lax.broadcasted_iota(jnp.int32, logits.shape, 0) == y_ref[...]
        grad = (weight * (jnp.exp(log_prob) - hot.astype(jnp.float32)) / labelled).astype(jnp.bfloat16)
        u_two[...] = lax.dot_general(w_two, grad, ROW_CONTRACT, preferred_element_type=jnp.float32).astype(jnp.bfloat16)
        g_two[...] = grad
        picked[...] = -weight * jnp.sum(jnp.where(hot, log_prob, 0.0), axis=0, keepdims=True)
    classes = g_two.shape[0]
    edge = small.shape[0] - 8
    owners = small.shape[0] // 8
    tile = pl.ds(pl.multiple_of(me * 8, 8), 8)

    def send_small():
        loss = jnp.sum(picked[...], axis=1, keepdims=True)
        labelled = jnp.sum(count[...], axis=0)[0:1, 0:1]
        small[0:classes] = lax.dot_general(g_two[...], two[...].astype(jnp.bfloat16), COL_CONTRACT, preferred_element_type=jnp.float32)
        small[classes:edge] = jnp.zeros((edge - classes, hidden), jnp.float32)
        small[edge:] = jnp.broadcast_to(loss / labelled, (8, hidden))
        for o in range(owners):
            @pl.when(me != o)
            def _():
                remote(small.at[pl.ds(o * 8, 8)], small_parts.at[me], ssend, srecv, o).start()

    def to_partner(s, t):
        return remote(stage.at[s, t], total.at[s, t], dsend, drecv.at[s], partner)

    def to_parent(s, t, k):
        got = crecv.at[s + 8] if k == 2 else crecv.at[(s - 1) * TREES + t]
        return remote(total.at[s, t], child.at[s - 1, t], csend, got, neighbour(t, k, core, chip))

    def reduce_small():
        @pl.when(me < owners)
        def _():
            small_parts[me] = small[tile]
            got = small_parts.at[pl.ds(0, n - 1)]
            remote(got, got, ssend, srecv, partner).wait_recv()
            small_whole[tile] = jnp.sum(small_parts[...], axis=0)
            for i in range(1, n):
                remote(small_whole.at[tile], small_whole.at[tile], bsend, brecv, lax.rem(me + i, n)).start()

    def finish_small():
        sent = small_parts.at[pl.ds(0, n - 1)]
        fewer, every = small_whole.at[pl.ds(0, owners * 8 - 8)], small_whole.at[pl.ds(0, owners * 8)]

        @pl.when(me < owners)
        def _():
            remote(sent, sent, bsend, brecv, partner).wait_send()
            remote(fewer, fewer, ssend, brecv, partner).wait_send()
            remote(fewer, fewer, ssend, brecv, partner).wait_recv()

        @pl.when(me >= owners)
        def _():
            remote(every, every, ssend, brecv, partner).wait_send()
            remote(every, every, ssend, brecv, partner).wait_recv()

    far, edge_row = STEPS - 2, hidden * 2 // 3 // 8 * 8 + 8

    def from_far_to(which):
        rows, k = ((slice(0, edge_row), 2), (slice(edge_row, hidden), 1))[which]
        sem = cut_sem.at[which]
        return remote(total.at[far, TREES - 1, rows], child.at[far - 1, TREES - 1, rows], csend, sem, neighbour(TREES - 1, k, core, chip))

    def add_far(s, which):
        from_far_to(which).wait_recv()
        rows = (slice(0, edge_row), slice(edge_row, hidden))[which]
        total[s, TREES - 1, rows] = total[s, TREES - 1, rows] + child[far - 1, TREES - 1, rows]

    def give(s, slot):
        loaded(slot, 1)
        for t in range(TREES):
            stage[s, t] = jnp.dot(u_two[...], ring[slot * 8 + TREES + t], preferred_element_type=jnp.float32)
        for t in range(TREES):
            to_partner(s, t).start()
        loaded(slot, 0)
        for t in range(TREES):
            mine[t] = jnp.dot(u_two[...], ring[slot * 8 + t], preferred_element_type=jnp.float32)

    def join(s):
        remote(total.at[s], total.at[s], dsend, drecv.at[s], partner).wait_recv()

    def gather_children(s, t):
        total[s, t] = total[s, t] + mine[t]
        for k in range(3):
            skip = far - 4 if k == 2 and t == TREES - 1 else STEPS
            if k == 2 and t == 0:
                for few, here in ((TREES, (s < 4) & (s != far - 4)), (TREES - 1, s == far - 4)):
                    @pl.when(here)
                    def _():
                        some = child.at[0, pl.ds(0, few)]
                        remote(some, some, csend, crecv.at[s + 12], partner).wait_recv()

            @pl.when((s < 2 ** k) & (s != skip))
            def _():
                if k < 2:
                    to_parent(s + 2 ** k, t, k).wait_recv()
                total[s, t] = total[s, t] + child[s + 2 ** k - 1, t]
        if t == TREES - 1:
            for which, parent in ((0, far - 4), (1, far - 2)):
                @pl.when(s == parent)
                def _():
                    add_far(s, which)

    def step_back(i, carry):
        s = back_order(i)
        slot = lax.rem(i, RING)
        with jax.named_scope('give'):
            give(s, slot)

            @pl.when(i + RING < STEPS)
            def _():
                load(back_order(i + RING), slot, 1)
                load(back_order(i + RING), slot, 0)

            @pl.when(i == 0)
            def _():
                send_small()
        with jax.named_scope('take'):
            join(s)
            for t in range(TREES):
                gather_children(s, t)
                for k in range(3):
                    skip = far if k == 2 and t == TREES - 1 else STEPS

                    @pl.when((s >= 2 ** k) & (s < 2 ** (k + 1)) & (s != skip))
                    def _():
                        to_parent(s, t, k).start()
                if t == TREES - 1:
                    @pl.when(s == far)
                    def _():
                        from_far_to(0).start()
                        from_far_to(1).start()
        return carry

    lax.fori_loop(0, STEPS - 1, step_back, 0)
    chips = n // 2
    half, share = part.shape[0] // 2, part.shape[0] // n
    mine_rows = pl.ds(pl.multiple_of(core * half, 8), half)
    their_rows = pl.ds(pl.multiple_of((1 - core) * half, 8), half)
    most = slice(0, (TREES - 1) * width)
    with jax.named_scope('give'):
        give(0, (STEPS - 1) % RING)
        join(0)

    def hidden_grad(t):
        gather_children(0, t)
        g_one[:, chunks[t]] = jnp.where(z_one[:, chunks[t]] > 0.0, total[0, t], 0.0).astype(jnp.bfloat16)

    def weight_grad(out_rows, cols):
        return lax.dot_general(s_one[out_rows, cols], g_one[:, cols], COL_CONTRACT, preferred_element_type=jnp.float32)

    with jax.named_scope('take'):
        for t in range(TREES - 1):
            hidden_grad(t)
        part[...] = weight_grad(slice(None), most)
        hidden_grad(TREES - 1)
    with jax.named_scope('dw'):
        part[their_rows] = part[their_rows] + weight_grad(their_rows, chunks[-1])
        over = remote(part.at[their_rows], pair, psend, precv, partner)
        over.start()
        part[mine_rows] = part[mine_rows] + weight_grad(mine_rows, chunks[-1])
    reduce_small()
    with jax.named_scope('drain'):
        gather_drain(buf, sems_x)
        gather_drain(h_buf, sems_h)
        remote(stage, stage, dsend, drecv.at[0], partner).wait_send()
        remote(child, child, csend, crecv.at[0], partner).wait_send()
    with jax.named_scope('pair'):
        over.wait()
        pair[...] = pair[...] + part[mine_rows]

    def share_of(q):
        return pl.ds(pl.multiple_of(q * share, 8), share)

    for i in range(1, chips):
        to = lax.rem(chip + i, chips)
        remote(pair.at[share_of(to)], parts.at[chip], fsend, frecv, to * 2 + core).start()
    parts[chip] = pair[share_of(chip)]
    with jax.named_scope('red'):
        wait_all(parts.at[pl.ds(0, chips - 1)], fsend, frecv)
    own = whole.at[pl.ds(pl.multiple_of(core * half + chip * share, 8), share)]
    own[...] = jnp.sum(parts[...], axis=0)
    for i in range(1, chips):
        remote(own, own, gsend, grecv, lax.rem(chip + i, chips) * 2 + core).start()
    with jax.named_scope('spread'):
        wait_all(whole.at[pl.ds(0, (chips - 1) * share)], gsend, grecv)
    swap = remote(whole.at[mine_rows], whole.at[mine_rows], qsend, qrecv, partner)
    swap.start()
    finish_small()
    dw2_ref[...] = small_whole[0:dw2_ref.shape[0]]
    loss_ref[...] = small_whole[edge:edge + 8]
    with jax.named_scope('swap'):
        swap.wait()
    dw_ref[...] = whole[0:feats]


def finish_kernel(loss_in, dw_in, dw2_in, loss_ref, dw_ref, dw2_ref):
    loss_ref[...] = loss_in[0:1, 0:1]
    dw_ref[...] = dw_in[...]
    dw2_ref[...] = dw2_in[...]


def train_step(x_rows, w_one, w2t, labels, mask, adj):
    rows, nodes = adj.shape
    n = nodes // rows
    feats, width = x_rows.shape[0], rows // TREES
    classes, hidden = w2t.shape
    units = n * TREES
    small = -(-classes // 8) * 8 + 8
    share = -(-feats // (8 * n)) * 8
    vmem, hbm = pl.BlockSpec(memory_space=pltpu.VMEM), pl.BlockSpec(memory_space=pl.ANY)
    dma, f32, bf16 = pltpu.SemaphoreType.DMA, jnp.float32, jnp.bfloat16
    block = (TREES, hidden, width)
    loss, dw_one, dw_two = pl.pallas_call(
        functools.partial(step_kernel, n),
        name='step',
        out_shape=(pltpu.VMEM((8, hidden), f32), pltpu.VMEM((feats, hidden), f32), pltpu.VMEM((classes, hidden), f32)),
        in_specs=[hbm, hbm, vmem, vmem, vmem, hbm],
        out_specs=(vmem,) * 3,
        scratch_shapes=[
            pltpu.VMEM((RING * 8, rows, width), bf16), pltpu.VMEM((units, feats, width), bf16), pltpu.VMEM((feats, rows), f32),
            pltpu.VMEM((units, hidden, width), bf16), pltpu.VMEM((n * share, rows), bf16), pltpu.VMEM((hidden, rows), f32),
            pltpu.VMEM((hidden, rows), bf16), pltpu.VMEM((feats, hidden), f32), pltpu.VMEM((small, hidden), f32), pltpu.VMEM((n, 8, 128), f32),
            pltpu.VMEM((STEPS, *block), f32), pltpu.VMEM(block, f32), pltpu.VMEM((STEPS, *block), f32), pltpu.VMEM((STEPS - 1, *block), f32),
            pltpu.VMEM((n * share, hidden), f32), pltpu.VMEM((n // 2, share, hidden), f32), pltpu.VMEM((n * share, hidden), f32),
            pltpu.VMEM((n, 8, hidden), f32), pltpu.VMEM((small, hidden), f32), pltpu.VMEM((n // 2 * share, hidden), f32),
            pltpu.VMEM((classes, rows), bf16), pltpu.VMEM((hidden, rows), bf16), pltpu.VMEM((1, rows), f32),
            dma((RING, 2)), dma, dma, dma, dma, dma, dma((STEPS,)), dma, dma((16,)), *[dma] * 12, dma((2,)), *gather_sems(), *gather_sems()],
        compiler_params=pltpu.CompilerParams(collective_id=0, has_side_effects=True, vmem_limit_bytes=62000000),
        cost_estimate=pl.CostEstimate(flops=2 * rows * nodes * (feats + 2 * hidden), bytes_accessed=6 * rows * nodes, transcendentals=0),
    )(x_rows, w_one, w2t, labels, mask, adj)
    return pl.pallas_call(
        finish_kernel,
        name='finish',
        out_shape=(jax.ShapeDtypeStruct((1, 1), f32), jax.ShapeDtypeStruct((feats, hidden), f32), jax.ShapeDtypeStruct((classes, hidden), f32)),
        in_specs=[vmem] * 3,
        out_specs=(vmem,) * 3,
    )(*[pltpu.with_memory_space_constraint(x, pltpu.VMEM) for x in (loss, dw_one, dw_two)])


def solution(mesh):
    axis_name = AXIS

    def local_step(adj_rows, feat_rows, w_one, w_two, label_rows, mask_rows):
        rows = adj_rows.shape[0]
        loss, dw_one, dw_two = train_step(feat_rows.T, w_one, w_two.T, label_rows.reshape(1, rows), mask_rows.reshape(1, rows), adj_rows)
        return loss.reshape(1), dw_one, dw_two.T

    return jax.shard_map(local_step, mesh=mesh, in_specs=(P(axis_name, None), P(axis_name, None), P(None, None), P(None, None), P(axis_name), P(axis_name)), out_specs=(P(None), P(None, None), P(None, None)), check_vma=False)
```

```python
import functools

import jax
import jax.numpy as jnp
from jax import lax
from jax.experimental import pallas as pl
from jax.experimental.pallas import tpu as pltpu
from jax.sharding import PartitionSpec as P

MESH = pl.DeviceIdType.MESH
AXIS = 'nodes'
TREES = 4
RING = 4
STEPS = 8
COL_CONTRACT = (((1,), (1,)), ((), ()))
ROW_CONTRACT = (((0,), (0,)), ((), ()))


def tree_axis(tree, k, core, chip):
    if tree < 3:
        weight = 2 ** ((tree + k) % 3)
        return weight, lax.rem(chip // weight, 2)
    weight = (1 - core) * 2 ** k + core * 2 ** (2 - k)
    low, high = lax.rem(chip // 2 ** k, 2), lax.rem(chip // 2 ** (2 - k), 2)
    return weight, (1 - core) * low + core * high


def chip_at(tree, offset, core, chip):
    out = chip
    for k in range(3):
        weight, bit = tree_axis(tree, k, core, chip)
        out = out + lax.rem(offset // 2 ** k, 2) * weight * (1 - 2 * bit)
    return out


def early_order(place):
    pair = (place + 1) // 2
    return place + (pair * (4 - pair)) // 4 * (7 - 2 * place)


def unit_at(tree, offset, core, chip):
    return (chip_at(tree, offset, core, chip) * 2 + core) * TREES + tree


def neighbour(tree, k, core, chip):
    weight, bit = tree_axis(tree, k, core, chip)
    return (chip + weight * (1 - 2 * bit)) * 2 + core


def remote(src, dst, send_sem, recv_sem, device):
    return pltpu.make_async_remote_copy(src_ref=src, dst_ref=dst, send_sem=send_sem, recv_sem=recv_sem, device_id=(device,), device_id_type=MESH)


def place():
    me = lax.axis_index(AXIS)
    core, chip = lax.rem(me, 2), me // 2
    return me, core, chip, chip * 2 + 1 - core


def gather_send(buf, sems, tree, offset, k, unit, rows=slice(None)):
    send, recv, hand = sems
    me, core, chip, partner = place()
    ref = buf.at[unit, rows]
    remote(ref, ref, send, recv.at[offset + 2 ** k - 1, tree], neighbour(tree, k, core, chip)).start()


def gather_hand(buf, sems, slot, unit):
    send, recv, hand = sems
    me, core, chip, partner = place()
    remote(buf.at[unit], buf.at[unit], send, hand.at[slot], partner).start()


def gather_start(buf, sems, links):
    me = lax.axis_index(AXIS)
    for k in range(links):
        for t in range(TREES):
            gather_send(buf, sems, t, 0, k, me * TREES + t)
        if k == 0:
            for t in range(TREES):
                gather_hand(buf, sems, 0, me * TREES + t)


def gather_arrive(buf, sems, s, links, trees=range(TREES), slot=None, cut=None):
    send, recv, hand = sems
    me, core, chip, partner = place()
    units = {t: unit_at(t, s, core, chip) for t in trees}
    for t, u in units.items():
        remote(buf.at[u], buf.at[u], send, recv.at[s - 1, t], partner).wait_recv()
        split = cut is not None and t == TREES - 1

        @pl.when(s == 1)
        def _():
            gather_send(buf, sems, t, s, 1, u)

        @pl.when((s > 1) & (s < (3 if split else 4)))
        def _():
            gather_send(buf, sems, t, s, 2, u)
        if split:
            @pl.when(s == 3)
            def _():
                gather_send(buf, sems, t, s, 2, u, slice(0, cut))

            @pl.when(s == 5)
            def _():
                gather_send(buf, sems, t, s, 1, u, slice(cut, None))
        gather_hand(buf, sems, s if slot is None else slot, u)

    @pl.when(s == 1)
    def _():
        if links < 3:
            for t in range(TREES):
                gather_send(buf, sems, t, 0, 2, me * TREES + t)
        for t, u in units.items():
            gather_send(buf, sems, t, s, 2, u)


def gather_take(buf, sems, slot, count=TREES):
    send, recv, hand = sems
    me, core, chip, partner = place()
    units = buf.at[pl.ds(0, count)]
    remote(units, units, send, hand.at[slot], partner).wait_recv()


def gather_drain(buf, sems):
    send, recv, hand = sems
    me, core, chip, partner = place()
    sent = buf.at[pl.ds(0, TREES * (STEPS - 1 + STEPS))]
    remote(sent, sent, send, hand.at[0], partner).wait_send()


def gather_sems():
    dma = pltpu.SemaphoreType.DMA
    return [dma, dma((STEPS - 1, TREES)), dma((STEPS + 1,))]


def barrier_near():
    me, core, chip, partner = place()
    sem = pltpu.get_barrier_semaphore()
    pl.semaphore_signal(sem, inc=1, device_id=(partner,), device_id_type=MESH)
    for k in range(3):
        pl.semaphore_signal(sem, inc=1, device_id=(neighbour(0, k, core, chip),), device_id_type=MESH)
    pl.semaphore_wait(sem, 4)


def send_all(n, src, dst, send_sem, recv_sem):
    me = lax.axis_index(AXIS)
    for i in range(1, n):
        to = lax.rem(me + i, n)
        remote(src(to), dst, send_sem, recv_sem, to).start()


def wait_all(ref, send_sem, recv_sem):
    me, core, chip, partner = place()
    copy = remote(ref, ref, send_sem, recv_sem, partner)
    copy.wait_send()
    copy.wait_recv()


def step_kernel(n, x_ref, w_hbm, w2t_hbm, y_hbm, m_hbm, adj, loss_ref, dw_ref, dw2_ref,
                ring, buf, acc, h_buf, s_one, z_one, u_two, w_v, small, count, stage, mine, total, child, part, parts, whole,
                small_parts, small_whole, pair, g_two, g_one, picked, w2t_ref, y_ref, m_ref,
                ring_sem, x_sem, w_sem, count_send, count_recv, dsend, drecv, csend, crecv, fsend, frecv, gsend, grecv,
                ssend, srecv, bsend, brecv, psend, precv, qsend, qrecv, cut_sem, *sems):
    me, core, chip, partner = place()
    sems_x, sems_h = sems[:3], sems[3:]
    width = buf.shape[2]
    feats, rows = acc.shape
    hidden = h_buf.shape[1]
    chunks = [slice(t * width, (t + 1) * width) for t in range(TREES)]

    def slab(s, slot, j):
        u = unit_at(j % TREES, s, core if j < TREES else 1 - core, chip)
        return pltpu.make_async_copy(adj.at[:, pl.ds(pl.multiple_of(u * width, width), width)], ring.at[slot * 8 + j], ring_sem.at[slot, j // TREES])

    def load(s, slot, half):
        for t in range(TREES):
            slab(s, slot, half * TREES + t).start()

    def loaded(slot, half):
        four = ring.at[pl.ds(0, TREES)]
        pltpu.make_async_copy(four, four, ring_sem.at[slot, half]).wait()

    with jax.named_scope('start'):
        fetch = [pltpu.make_async_copy(x_ref.at[:, pl.ds(t * width, width)], buf.at[me * TREES + t], x_sem) for t in range(TREES)]
        for copy in fetch:
            copy.start()
        barrier_near()
        four = buf.at[pl.ds(0, TREES)]
        pltpu.make_async_copy(four, four, x_sem).wait()
    gather_start(buf, sems_x, 2)
    params = [pltpu.make_async_copy(src, dst, w_sem.at[i]) for i, (src, dst) in enumerate(((w_hbm, w_v), (w2t_hbm, w2t_ref), (y_hbm, y_ref), (m_hbm, m_ref)))]
    for copy in params:
        copy.start()
    for s in range(RING):
        for half in range(2):
            load(s, s, half)
    acc[...] = jnp.zeros_like(acc)

    def terms(units_ref, s, slot, half, trees=range(TREES)):
        which = core if half == 0 else 1 - core
        return [(units_ref, unit_at(t, s, which, chip), slot * 8 + half * TREES + t) for t in trees]

    def aggregate(out, pairs):
        for cols in chunks:
            out[:, cols] += sum(lax.dot_general(ref[u], ring[j, cols], COL_CONTRACT, preferred_element_type=jnp.float32) for ref, u, j in pairs)

    def step_one(s, carry):
        with jax.named_scope('arrive'):
            @pl.when(s > 0)
            def _():
                gather_arrive(buf, sems_x, s, 2, cut=cut)
        for half in range(2):
            with jax.named_scope('consume'):
                if half == 1:
                    gather_take(buf, sems_x, s)
                slot = lax.rem(s, RING)
                loaded(slot, half)
                aggregate(acc, terms(buf, s, slot, half))
                late = s // RING
                load((1 - late) * (s + RING) + late * early_order(s - late * RING), slot, half)
        return carry

    cut = feats * 2 // 3 // 16 * 16
    final, slot = STEPS - 1, (STEPS - 1) % RING
    lax.fori_loop(0, final, step_one, 0)
    early, late = (range(TREES - 1), final), (range(TREES - 1, TREES), STEPS)
    for half in range(2):
        for trees, hand in (early, late):
            with jax.named_scope('consume'):
                if half == 0:
                    gather_arrive(buf, sems_x, final, 2, trees, hand, cut)
                else:
                    gather_take(buf, sems_x, hand, len(trees))
                if hand == final:
                    loaded(slot, half)
                aggregate(acc, terms(buf, final, slot, half, trees))
    for half in range(2):
        load(early_order(final - RING), slot, half)
    with jax.named_scope('mid'):
        for copy in params:
            copy.wait()
        s_one[0:feats] = acc[...].astype(jnp.bfloat16)
        s_one[feats:] = jnp.zeros_like(s_one[feats:])
        w_rows = w_v[...].astype(jnp.bfloat16)
        for t, cols in enumerate(chunks):
            z = lax.dot_general(w_rows, s_one[0:feats, cols], ROW_CONTRACT, preferred_element_type=jnp.float32)
            z_one[:, cols] = z
            h_buf[me * TREES + t] = jnp.maximum(z, 0.0).astype(jnp.bfloat16)
    gather_start(h_buf, sems_h, 3)
    weight = m_ref[...].astype(jnp.float32)
    count[me] = jnp.broadcast_to(jnp.sum(weight, axis=1, keepdims=True), count.shape[1:])
    send_all(n, lambda to: count.at[me], count.at[me], count_send, count_recv)
    two = acc.at[0:hidden]

    def take_two(p, half):
        loaded(lax.rem(p, RING), half)
        return terms(h_buf, early_order(p), lax.rem(p, RING), half)

    def back_order(i):
        return early_order(STEPS - 1 - i)

    def load_two(p, half):
        late = p // RING
        load((1 - late) * early_order(p + RING - late * RING) + late * back_order(p - late * RING), lax.rem(p, RING), half)

    two[...] = jnp.zeros_like(two)
    with jax.named_scope('consume'):
        aggregate(two, take_two(0, 0))
        load_two(0, 0)
        gather_take(h_buf, sems_h, 0)
        aggregate(two, take_two(0, 1))
        load_two(0, 1)
    with jax.named_scope('arrive'):
        gather_arrive(h_buf, sems_h, 1, 3)
    with jax.named_scope('consume'):
        aggregate(two, take_two(1, 0))
        load_two(1, 0)

    for p in range(2, STEPS):
        with jax.named_scope('arrive'):
            gather_arrive(h_buf, sems_h, early_order(p), 3)
            gather_take(h_buf, sems_h, early_order(p - 1))
        with jax.named_scope('consume'):
            aggregate(two, take_two(p - 1, 1) + take_two(p, 0))
            load_two(p - 1, 1)
            load_two(p, 0)
    with jax.named_scope('last'):
        gather_take(h_buf, sems_h, STEPS - 1)
        aggregate(two, take_two(STEPS - 1, 1))
        load_two(STEPS - 1, 1)
    with jax.named_scope('soft'):
        wait_all(count.at[pl.ds(0, n - 1)], count_send, count_recv)
        labelled = jnp.sum(count[...], axis=0)[0:1, 0:1]
        s_two = two[...].astype(jnp.bfloat16)
        w_two = w2t_ref[...].astype(jnp.bfloat16)
        logits = jnp.dot(w_two, s_two, preferred_element_type=jnp.float32)
        shifted = logits - jnp.max(logits, axis=0, keepdims=True)
        log_prob = shifted - jnp.log(jnp.sum(jnp.exp(shifted), axis=0, keepdims=True))
        hot = lax.broadcasted_iota(jnp.int32, logits.shape, 0) == y_ref[...]
        grad = (weight * (jnp.exp(log_prob) - hot.astype(jnp.float32)) / labelled).astype(jnp.bfloat16)
        u_two[...] = lax.dot_general(w_two, grad, ROW_CONTRACT, preferred_element_type=jnp.float32).astype(jnp.bfloat16)
        g_two[...] = grad
        picked[...] = -weight * jnp.sum(jnp.where(hot, log_prob, 0.0), axis=0, keepdims=True)
    classes = g_two.shape[0]
    edge = small.shape[0] - 8
    owners = small.shape[0] // 8
    tile = pl.ds(pl.multiple_of(me * 8, 8), 8)

    def send_small():
        loss = jnp.sum(picked[...], axis=1, keepdims=True)
        labelled = jnp.sum(count[...], axis=0)[0:1, 0:1]
        small[0:classes] = lax.dot_general(g_two[...], two[...].astype(jnp.bfloat16), COL_CONTRACT, preferred_element_type=jnp.float32)
        small[classes:edge] = jnp.zeros((edge - classes, hidden), jnp.float32)
        small[edge:] = jnp.broadcast_to(loss / labelled, (8, hidden))
        for o in range(owners):
            @pl.when(me != o)
            def _():
                remote(small.at[pl.ds(o * 8, 8)], small_parts.at[me], ssend, srecv, o).start()

    def to_partner(s, t):
        return remote(stage.at[s, t], total.at[s, t], dsend, drecv.at[s], partner)

    def to_parent(s, t, k):
        return remote(total.at[s, t], child.at[s - 1, t], csend, crecv.at[s - 1, t], neighbour(t, k, core, chip))

    def reduce_small():
        @pl.when(me < owners)
        def _():
            small_parts[me] = small[tile]
            got = small_parts.at[pl.ds(0, n - 1)]
            remote(got, got, ssend, srecv, partner).wait_recv()
            small_whole[tile] = jnp.sum(small_parts[...], axis=0)
            for i in range(1, n):
                remote(small_whole.at[tile], small_whole.at[tile], bsend, brecv, lax.rem(me + i, n)).start()

    def finish_small():
        sent = small_parts.at[pl.ds(0, n - 1)]
        fewer, every = small_whole.at[pl.ds(0, owners * 8 - 8)], small_whole.at[pl.ds(0, owners * 8)]

        @pl.when(me < owners)
        def _():
            remote(sent, sent, bsend, brecv, partner).wait_send()
            remote(fewer, fewer, ssend, brecv, partner).wait_send()
            remote(fewer, fewer, ssend, brecv, partner).wait_recv()

        @pl.when(me >= owners)
        def _():
            remote(every, every, ssend, brecv, partner).wait_send()
            remote(every, every, ssend, brecv, partner).wait_recv()

    far, edge_row = STEPS - 2, hidden * 2 // 3 // 8 * 8 + 8

    def from_far_to(which):
        rows, k = ((slice(0, edge_row), 2), (slice(edge_row, hidden), 1))[which]
        sem = cut_sem if which else crecv.at[far - 1, TREES - 1]
        return remote(total.at[far, TREES - 1, rows], child.at[far - 1, TREES - 1, rows], csend, sem, neighbour(TREES - 1, k, core, chip))

    def add_far(s, which):
        from_far_to(which).wait_recv()
        rows = (slice(0, edge_row), slice(edge_row, hidden))[which]
        total[s, TREES - 1, rows] = total[s, TREES - 1, rows] + child[far - 1, TREES - 1, rows]

    def give(s, slot):
        loaded(slot, 1)
        for t in range(TREES):
            stage[s, t] = jnp.dot(u_two[...], ring[slot * 8 + TREES + t], preferred_element_type=jnp.float32)
        for t in range(TREES):
            to_partner(s, t).start()
        loaded(slot, 0)
        for t in range(TREES):
            mine[t] = jnp.dot(u_two[...], ring[slot * 8 + t], preferred_element_type=jnp.float32)

    def join(s):
        remote(total.at[s], total.at[s], dsend, drecv.at[s], partner).wait_recv()

    def gather_children(s, t):
        total[s, t] = total[s, t] + mine[t]
        for k in range(3):
            skip = far - 4 if k == 2 and t == TREES - 1 else STEPS

            @pl.when((s < 2 ** k) & (s != skip))
            def _():
                to_parent(s + 2 ** k, t, k).wait_recv()
                total[s, t] = total[s, t] + child[s + 2 ** k - 1, t]
        if t == TREES - 1:
            for which, parent in ((0, far - 4), (1, far - 2)):
                @pl.when(s == parent)
                def _():
                    add_far(s, which)

    def step_back(i, carry):
        s = back_order(i)
        slot = lax.rem(i, RING)
        with jax.named_scope('give'):
            give(s, slot)

            @pl.when(i + RING < STEPS)
            def _():
                load(back_order(i + RING), slot, 1)
                load(back_order(i + RING), slot, 0)

            @pl.when(i == 0)
            def _():
                send_small()
        with jax.named_scope('take'):
            join(s)
            for t in range(TREES):
                gather_children(s, t)
                for k in range(3):
                    skip = far if k == 2 and t == TREES - 1 else STEPS

                    @pl.when((s >= 2 ** k) & (s < 2 ** (k + 1)) & (s != skip))
                    def _():
                        to_parent(s, t, k).start()
                if t == TREES - 1:
                    @pl.when(s == far)
                    def _():
                        from_far_to(0).start()
                        from_far_to(1).start()
        return carry

    lax.fori_loop(0, STEPS - 1, step_back, 0)
    chips = n // 2
    half, share = part.shape[0] // 2, part.shape[0] // n
    mine_rows = pl.ds(pl.multiple_of(core * half, 8), half)
    their_rows = pl.ds(pl.multiple_of((1 - core) * half, 8), half)
    most = slice(0, (TREES - 1) * width)
    with jax.named_scope('give'):
        give(0, (STEPS - 1) % RING)
        join(0)

    def hidden_grad(t):
        gather_children(0, t)
        g_one[:, chunks[t]] = jnp.where(z_one[:, chunks[t]] > 0.0, total[0, t], 0.0).astype(jnp.bfloat16)

    def weight_grad(out_rows, cols):
        return lax.dot_general(s_one[out_rows, cols], g_one[:, cols], COL_CONTRACT, preferred_element_type=jnp.float32)

    with jax.named_scope('take'):
        for t in range(TREES - 1):
            hidden_grad(t)
        part[...] = weight_grad(slice(None), most)
        hidden_grad(TREES - 1)
    with jax.named_scope('dw'):
        part[their_rows] = part[their_rows] + weight_grad(their_rows, chunks[-1])
        over = remote(part.at[their_rows], pair, psend, precv, partner)
        over.start()
        part[mine_rows] = part[mine_rows] + weight_grad(mine_rows, chunks[-1])
    reduce_small()
    with jax.named_scope('drain'):
        gather_drain(buf, sems_x)
        gather_drain(h_buf, sems_h)
        remote(stage, stage, dsend, drecv.at[0], partner).wait_send()
        remote(child, child, csend, crecv.at[0, 0], partner).wait_send()
    with jax.named_scope('pair'):
        over.wait()
        pair[...] = pair[...] + part[mine_rows]

    def share_of(q):
        return pl.ds(pl.multiple_of(q * share, 8), share)

    for i in range(1, chips):
        to = lax.rem(chip + i, chips)
        remote(pair.at[share_of(to)], parts.at[chip], fsend, frecv, to * 2 + core).start()
    parts[chip] = pair[share_of(chip)]
    with jax.named_scope('red'):
        wait_all(parts.at[pl.ds(0, chips - 1)], fsend, frecv)
    own = whole.at[pl.ds(pl.multiple_of(core * half + chip * share, 8), share)]
    own[...] = jnp.sum(parts[...], axis=0)
    for i in range(1, chips):
        remote(own, own, gsend, grecv, lax.rem(chip + i, chips) * 2 + core).start()
    with jax.named_scope('spread'):
        wait_all(whole.at[pl.ds(0, (chips - 1) * share)], gsend, grecv)
    swap = remote(whole.at[mine_rows], whole.at[mine_rows], qsend, qrecv, partner)
    swap.start()
    finish_small()
    dw2_ref[...] = small_whole[0:dw2_ref.shape[0]]
    loss_ref[...] = small_whole[edge:edge + 8]
    with jax.named_scope('swap'):
        swap.wait()
    dw_ref[...] = whole[0:feats]


def finish_kernel(loss_in, dw_in, dw2_in, loss_ref, dw_ref, dw2_ref):
    loss_ref[...] = loss_in[0:1, 0:1]
    dw_ref[...] = dw_in[...]
    dw2_ref[...] = dw2_in[...]


def train_step(x_rows, w_one, w2t, labels, mask, adj):
    rows, nodes = adj.shape
    n = nodes // rows
    feats, width = x_rows.shape[0], rows // TREES
    classes, hidden = w2t.shape
    units = n * TREES
    small = -(-classes // 8) * 8 + 8
    share = -(-feats // (8 * n)) * 8
    vmem, hbm = pl.BlockSpec(memory_space=pltpu.VMEM), pl.BlockSpec(memory_space=pl.ANY)
    dma, f32, bf16 = pltpu.SemaphoreType.DMA, jnp.float32, jnp.bfloat16
    block = (TREES, hidden, width)
    loss, dw_one, dw_two = pl.pallas_call(
        functools.partial(step_kernel, n),
        name='step',
        out_shape=(pltpu.VMEM((8, hidden), f32), pltpu.VMEM((feats, hidden), f32), pltpu.VMEM((classes, hidden), f32)),
        in_specs=[hbm] * 6,
        out_specs=(vmem,) * 3,
        scratch_shapes=[
            pltpu.VMEM((RING * 8, rows, width), bf16), pltpu.VMEM((units, feats, width), bf16), pltpu.VMEM((feats, rows), f32),
            pltpu.VMEM((units, hidden, width), bf16), pltpu.VMEM((n * share, rows), bf16), pltpu.VMEM((hidden, rows), f32),
            pltpu.VMEM((hidden, rows), bf16), pltpu.VMEM((feats, hidden), f32), pltpu.VMEM((small, hidden), f32), pltpu.VMEM((n, 8, 128), f32),
            pltpu.VMEM((STEPS, *block), f32), pltpu.VMEM(block, f32), pltpu.VMEM((STEPS, *block), f32), pltpu.VMEM((STEPS - 1, *block), f32),
            pltpu.VMEM((n * share, hidden), f32), pltpu.VMEM((n // 2, share, hidden), f32), pltpu.VMEM((n * share, hidden), f32),
            pltpu.VMEM((n, 8, hidden), f32), pltpu.VMEM((small, hidden), f32), pltpu.VMEM((n // 2 * share, hidden), f32),
            pltpu.VMEM((classes, rows), bf16), pltpu.VMEM((hidden, rows), bf16), pltpu.VMEM((1, rows), f32),
            pltpu.VMEM((classes, hidden), f32), pltpu.VMEM((1, rows), jnp.int32), pltpu.VMEM((1, rows), jnp.int32),
            dma((RING, 2)), dma, dma((4,)), dma, dma, dma, dma((STEPS,)), dma, dma((STEPS - 1, TREES)), *[dma] * 13, *gather_sems(), *gather_sems()],
        compiler_params=pltpu.CompilerParams(collective_id=0, has_side_effects=True, vmem_limit_bytes=62000000),
        cost_estimate=pl.CostEstimate(flops=2 * rows * nodes * (feats + 2 * hidden), bytes_accessed=6 * rows * nodes, transcendentals=0),
    )(*[pltpu.with_memory_space_constraint(x, pltpu.HBM) for x in (x_rows, w_one, w2t, labels, mask, adj)])
    return pl.pallas_call(
        finish_kernel,
        name='finish',
        out_shape=(jax.ShapeDtypeStruct((1, 1), f32), jax.ShapeDtypeStruct((feats, hidden), f32), jax.ShapeDtypeStruct((classes, hidden), f32)),
        in_specs=[vmem] * 3,
        out_specs=(vmem,) * 3,
    )(*[pltpu.with_memory_space_constraint(x, pltpu.VMEM) for x in (loss, dw_one, dw_two)])


def solution(mesh):
    axis_name = AXIS

    def local_step(adj_rows, feat_rows, w_one, w_two, label_rows, mask_rows):
        rows = adj_rows.shape[0]
        loss, dw_one, dw_two = train_step(feat_rows.T, w_one, w_two.T, label_rows.reshape(1, rows), mask_rows.reshape(1, rows), adj_rows)
        return loss.reshape(1), dw_one, dw_two.T

    return jax.shard_map(local_step, mesh=mesh, in_specs=(P(axis_name, None), P(axis_name, None), P(None, None), P(None, None), P(axis_name), P(axis_name)), out_specs=(P(None), P(None, None), P(None, None)), check_vma=False)
```

```python
import functools

import jax
import jax.numpy as jnp
from jax import lax
from jax.experimental import pallas as pl
from jax.experimental.pallas import tpu as pltpu
from jax.sharding import PartitionSpec as P

MESH = pl.DeviceIdType.MESH
AXIS = 'nodes'
TREES = 4
RING = 4
STEPS = 8
COL_CONTRACT = (((1,), (1,)), ((), ()))
ROW_CONTRACT = (((0,), (0,)), ((), ()))


def tree_axis(tree, k, core, chip):
    if tree < 3:
        weight = 2 ** ((tree + k) % 3)
        return weight, lax.rem(chip // weight, 2)
    weight = (1 - core) * 2 ** k + core * 2 ** (2 - k)
    low, high = lax.rem(chip // 2 ** k, 2), lax.rem(chip // 2 ** (2 - k), 2)
    return weight, (1 - core) * low + core * high


def chip_at(tree, offset, core, chip):
    out = chip
    for k in range(3):
        weight, bit = tree_axis(tree, k, core, chip)
        out = out + lax.rem(offset // 2 ** k, 2) * weight * (1 - 2 * bit)
    return out


def early_order(place):
    pair = (place + 1) // 2
    return place + (pair * (4 - pair)) // 4 * (7 - 2 * place)


def other_chips(chip):
    for flips in ((1, 2, 4), (1, 4), (1, 2), (2, 4), (1,), (2,), (4,)):
        yield chip + sum(w * (1 - 2 * lax.rem(chip // w, 2)) for w in flips)


def unit_at(tree, offset, core, chip):
    return (chip_at(tree, offset, core, chip) * 2 + core) * TREES + tree


def neighbour(tree, k, core, chip):
    weight, bit = tree_axis(tree, k, core, chip)
    return (chip + weight * (1 - 2 * bit)) * 2 + core


def remote(src, dst, send_sem, recv_sem, device):
    return pltpu.make_async_remote_copy(src_ref=src, dst_ref=dst, send_sem=send_sem, recv_sem=recv_sem, device_id=(device,), device_id_type=MESH)


def place():
    me = lax.axis_index(AXIS)
    core, chip = lax.rem(me, 2), me // 2
    return me, core, chip, chip * 2 + 1 - core


def gather_send(buf, sems, tree, offset, k, unit, rows=slice(None)):
    send, recv, hand = sems
    me, core, chip, partner = place()
    ref = buf.at[unit, rows]
    remote(ref, ref, send, recv.at[offset + 2 ** k - 1, tree], neighbour(tree, k, core, chip)).start()


def gather_hand(buf, sems, slot, unit):
    send, recv, hand = sems
    me, core, chip, partner = place()
    remote(buf.at[unit], buf.at[unit], send, hand.at[slot], partner).start()


def gather_start(buf, sems, links):
    me = lax.axis_index(AXIS)
    for k in range(links):
        for t in range(TREES):
            gather_send(buf, sems, t, 0, k, me * TREES + t)
        if k == 0:
            for t in range(TREES):
                gather_hand(buf, sems, 0, me * TREES + t)


def gather_arrive(buf, sems, s, links, trees=range(TREES), slot=None, cut=None):
    send, recv, hand = sems
    me, core, chip, partner = place()
    units = {t: unit_at(t, s, core, chip) for t in trees}
    for t, u in units.items():
        remote(buf.at[u], buf.at[u], send, recv.at[s - 1, t], partner).wait_recv()
        split = cut is not None and t == TREES - 1

        @pl.when(s == 1)
        def _():
            gather_send(buf, sems, t, s, 1, u)

        @pl.when((s > 1) & (s < (3 if split else 4)))
        def _():
            gather_send(buf, sems, t, s, 2, u)
        if split:
            @pl.when(s == 3)
            def _():
                gather_send(buf, sems, t, s, 2, u, slice(0, cut))

            @pl.when(s == 5)
            def _():
                gather_send(buf, sems, t, s, 1, u, slice(cut, None))
        gather_hand(buf, sems, s if slot is None else slot, u)

    @pl.when(s == 1)
    def _():
        if links < 3:
            for t in range(TREES):
                gather_send(buf, sems, t, 0, 2, me * TREES + t)
        for t, u in units.items():
            gather_send(buf, sems, t, s, 2, u)


def gather_take(buf, sems, slot, count=TREES):
    send, recv, hand = sems
    me, core, chip, partner = place()
    units = buf.at[pl.ds(0, count)]
    remote(units, units, send, hand.at[slot], partner).wait_recv()


def gather_drain(buf, sems):
    send, recv, hand = sems
    me, core, chip, partner = place()
    sent = buf.at[pl.ds(0, TREES * (STEPS - 1 + STEPS))]
    remote(sent, sent, send, hand.at[0], partner).wait_send()


def gather_sems():
    dma = pltpu.SemaphoreType.DMA
    return [dma, dma((STEPS - 1, TREES)), dma((STEPS + 1,))]


def barrier_near():
    me, core, chip, partner = place()
    sem = pltpu.get_barrier_semaphore()
    pl.semaphore_signal(sem, inc=1, device_id=(partner,), device_id_type=MESH)
    for k in range(3):
        pl.semaphore_signal(sem, inc=1, device_id=(neighbour(0, k, core, chip),), device_id_type=MESH)
    pl.semaphore_wait(sem, 4)


def send_all(n, src, dst, send_sem, recv_sem):
    me = lax.axis_index(AXIS)
    for i in range(1, n):
        to = lax.rem(me + i, n)
        remote(src(to), dst, send_sem, recv_sem, to).start()


def wait_all(ref, send_sem, recv_sem):
    me, core, chip, partner = place()
    copy = remote(ref, ref, send_sem, recv_sem, partner)
    copy.wait_send()
    copy.wait_recv()


def step_kernel(n, x_ref, w_hbm, w2t_hbm, y_hbm, m_hbm, adj, loss_ref, dw_ref, dw2_ref,
                ring, buf, acc, h_buf, s_one, z_one, u_two, w_v, small, count, stage, mine, total, child, part, parts, whole,
                small_parts, small_whole, pair, g_two, g_one, picked, w2t_ref, y_ref, m_ref,
                ring_sem, x_sem, w_sem, count_send, count_recv, dsend, drecv, csend, crecv, fsend, frecv, gsend, grecv,
                ssend, srecv, bsend, brecv, psend, precv, qsend, qrecv, cut_sem, *sems):
    me, core, chip, partner = place()
    sems_x, sems_h = sems[:3], sems[3:]
    width = buf.shape[2]
    feats, rows = acc.shape
    hidden = h_buf.shape[1]
    chunks = [slice(t * width, (t + 1) * width) for t in range(TREES)]

    def slab(s, slot, j):
        u = unit_at(j % TREES, s, core if j < TREES else 1 - core, chip)
        return pltpu.make_async_copy(adj.at[:, pl.ds(pl.multiple_of(u * width, width), width)], ring.at[slot * 8 + j], ring_sem.at[slot, j // TREES])

    def load(s, slot, half):
        for t in range(TREES):
            slab(s, slot, half * TREES + t).start()

    def loaded(slot, half):
        four = ring.at[pl.ds(0, TREES)]
        pltpu.make_async_copy(four, four, ring_sem.at[slot, half]).wait()

    with jax.named_scope('start'):
        fetch = [pltpu.make_async_copy(x_ref.at[:, pl.ds(t * width, width)], buf.at[me * TREES + t], x_sem) for t in range(TREES)]
        for copy in fetch:
            copy.start()
        barrier_near()
        four = buf.at[pl.ds(0, TREES)]
        pltpu.make_async_copy(four, four, x_sem).wait()
    gather_start(buf, sems_x, 2)
    params = [pltpu.make_async_copy(src, dst, w_sem.at[i]) for i, (src, dst) in enumerate(((w_hbm, w_v), (w2t_hbm, w2t_ref), (y_hbm, y_ref), (m_hbm, m_ref)))]
    for copy in params:
        copy.start()
    for s in range(RING):
        for half in range(2):
            load(s, s, half)
    acc[...] = jnp.zeros_like(acc)

    def terms(units_ref, s, slot, half, trees=range(TREES)):
        which = core if half == 0 else 1 - core
        return [(units_ref, unit_at(t, s, which, chip), slot * 8 + half * TREES + t) for t in trees]

    def aggregate(out, pairs):
        for cols in chunks:
            out[:, cols] += sum(lax.dot_general(ref[u], ring[j, cols], COL_CONTRACT, preferred_element_type=jnp.float32) for ref, u, j in pairs)

    def step_one(s, carry):
        with jax.named_scope('arrive'):
            @pl.when(s > 0)
            def _():
                gather_arrive(buf, sems_x, s, 2, cut=cut)
        for half in range(2):
            with jax.named_scope('consume'):
                if half == 1:
                    gather_take(buf, sems_x, s)
                slot = lax.rem(s, RING)
                loaded(slot, half)
                aggregate(acc, terms(buf, s, slot, half))
                late = s // RING
                load((1 - late) * (s + RING) + late * early_order(s - late * RING), slot, half)
        return carry

    cut = feats * 2 // 3 // 16 * 16
    final, slot = STEPS - 1, (STEPS - 1) % RING
    lax.fori_loop(0, final, step_one, 0)
    early, late = (range(TREES - 1), final), (range(TREES - 1, TREES), STEPS)
    for half in range(2):
        for trees, hand in (early, late):
            with jax.named_scope('consume'):
                if half == 0:
                    gather_arrive(buf, sems_x, final, 2, trees, hand, cut)
                else:
                    gather_take(buf, sems_x, hand, len(trees))
                if hand == final:
                    loaded(slot, half)
                aggregate(acc, terms(buf, final, slot, half, trees))
    for half in range(2):
        load(early_order(final - RING), slot, half)
    with jax.named_scope('mid'):
        for copy in params:
            copy.wait()
        s_one[0:feats] = acc[...].astype(jnp.bfloat16)
        s_one[feats:] = jnp.zeros_like(s_one[feats:])
        w_rows = w_v[...].astype(jnp.bfloat16)
        for t, cols in enumerate(chunks):
            z = lax.dot_general(w_rows, s_one[0:feats, cols], ROW_CONTRACT, preferred_element_type=jnp.float32)
            z_one[:, cols] = z
            h_buf[me * TREES + t] = jnp.maximum(z, 0.0).astype(jnp.bfloat16)
    gather_start(h_buf, sems_h, 3)
    weight = m_ref[...].astype(jnp.float32)
    count[me] = jnp.broadcast_to(jnp.sum(weight, axis=1, keepdims=True), count.shape[1:])
    send_all(n, lambda to: count.at[me], count.at[me], count_send, count_recv)
    two = acc.at[0:hidden]

    def take_two(p, half):
        loaded(lax.rem(p, RING), half)
        return terms(h_buf, early_order(p), lax.rem(p, RING), half)

    def back_order(i):
        return early_order(STEPS - 1 - i)

    def load_two(p, half):
        late = p // RING
        load((1 - late) * early_order(p + RING - late * RING) + late * back_order(p - late * RING), lax.rem(p, RING), half)

    two[...] = jnp.zeros_like(two)
    with jax.named_scope('consume'):
        aggregate(two, take_two(0, 0))
        load_two(0, 0)
        gather_take(h_buf, sems_h, 0)
        aggregate(two, take_two(0, 1))
        load_two(0, 1)
    with jax.named_scope('arrive'):
        gather_arrive(h_buf, sems_h, 1, 3)
    with jax.named_scope('consume'):
        aggregate(two, take_two(1, 0))
        load_two(1, 0)

    for p in range(2, STEPS):
        with jax.named_scope('arrive'):
            gather_arrive(h_buf, sems_h, early_order(p), 3)
            gather_take(h_buf, sems_h, early_order(p - 1))
        with jax.named_scope('consume'):
            aggregate(two, take_two(p - 1, 1) + take_two(p, 0))
            load_two(p - 1, 1)
            load_two(p, 0)
    with jax.named_scope('last'):
        gather_take(h_buf, sems_h, STEPS - 1)
        aggregate(two, take_two(STEPS - 1, 1))
        load_two(STEPS - 1, 1)
    with jax.named_scope('soft'):
        wait_all(count.at[pl.ds(0, n - 1)], count_send, count_recv)
        labelled = jnp.sum(count[...], axis=0)[0:1, 0:1]
        s_two = two[...].astype(jnp.bfloat16)
        w_two = w2t_ref[...].astype(jnp.bfloat16)
        logits = jnp.dot(w_two, s_two, preferred_element_type=jnp.float32)
        shifted = logits - jnp.max(logits, axis=0, keepdims=True)
        log_prob = shifted - jnp.log(jnp.sum(jnp.exp(shifted), axis=0, keepdims=True))
        hot = lax.broadcasted_iota(jnp.int32, logits.shape, 0) == y_ref[...]
        grad = (weight * (jnp.exp(log_prob) - hot.astype(jnp.float32)) / labelled).astype(jnp.bfloat16)
        u_two[...] = lax.dot_general(w_two, grad, ROW_CONTRACT, preferred_element_type=jnp.float32).astype(jnp.bfloat16)
        g_two[...] = grad
        picked[...] = -weight * jnp.sum(jnp.where(hot, log_prob, 0.0), axis=0, keepdims=True)
    classes = g_two.shape[0]
    edge = small.shape[0] - 8
    owners = small.shape[0] // 8
    tile = pl.ds(pl.multiple_of(me * 8, 8), 8)

    def send_small():
        loss = jnp.sum(picked[...], axis=1, keepdims=True)
        labelled = jnp.sum(count[...], axis=0)[0:1, 0:1]
        small[0:classes] = lax.dot_general(g_two[...], two[...].astype(jnp.bfloat16), COL_CONTRACT, preferred_element_type=jnp.float32)
        small[classes:edge] = jnp.zeros((edge - classes, hidden), jnp.float32)
        small[edge:] = jnp.broadcast_to(loss / labelled, (8, hidden))
        for o in range(owners):
            @pl.when(me != o)
            def _():
                remote(small.at[pl.ds(o * 8, 8)], small_parts.at[me], ssend, srecv, o).start()

    def to_partner(s, t):
        return remote(stage.at[s, t], total.at[s, t], dsend, drecv.at[s], partner)

    def to_parent(s, t, k):
        return remote(total.at[s, t], child.at[s - 1, t], csend, crecv.at[s - 1, t], neighbour(t, k, core, chip))

    def reduce_small():
        @pl.when(me < owners)
        def _():
            small_parts[me] = small[tile]
            got = small_parts.at[pl.ds(0, n - 1)]
            remote(got, got, ssend, srecv, partner).wait_recv()
            small_whole[tile] = jnp.sum(small_parts[...], axis=0)
            for i in range(1, n):
                remote(small_whole.at[tile], small_whole.at[tile], bsend, brecv, lax.rem(me + i, n)).start()

    def finish_small():
        sent = small_parts.at[pl.ds(0, n - 1)]
        fewer, every = small_whole.at[pl.ds(0, owners * 8 - 8)], small_whole.at[pl.ds(0, owners * 8)]

        @pl.when(me < owners)
        def _():
            remote(sent, sent, bsend, brecv, partner).wait_send()
            remote(fewer, fewer, ssend, brecv, partner).wait_send()
            remote(fewer, fewer, ssend, brecv, partner).wait_recv()

        @pl.when(me >= owners)
        def _():
            remote(every, every, ssend, brecv, partner).wait_send()
            remote(every, every, ssend, brecv, partner).wait_recv()

    far, edge_row = STEPS - 2, hidden * 2 // 3 // 8 * 8 + 8

    def from_far_to(which):
        rows, k = ((slice(0, edge_row), 2), (slice(edge_row, hidden), 1))[which]
        sem = cut_sem if which else crecv.at[far - 1, TREES - 1]
        return remote(total.at[far, TREES - 1, rows], child.at[far - 1, TREES - 1, rows], csend, sem, neighbour(TREES - 1, k, core, chip))

    def add_far(s, which):
        from_far_to(which).wait_recv()
        rows = (slice(0, edge_row), slice(edge_row, hidden))[which]
        total[s, TREES - 1, rows] = total[s, TREES - 1, rows] + child[far - 1, TREES - 1, rows]

    def give(s, slot):
        loaded(slot, 1)
        for t in range(TREES):
            stage[s, t] = jnp.dot(u_two[...], ring[slot * 8 + TREES + t], preferred_element_type=jnp.float32)
        for t in range(TREES):
            to_partner(s, t).start()
        loaded(slot, 0)
        for t in range(TREES):
            mine[t] = jnp.dot(u_two[...], ring[slot * 8 + t], preferred_element_type=jnp.float32)

    def join(s):
        remote(total.at[s], total.at[s], dsend, drecv.at[s], partner).wait_recv()

    def gather_children(s, t):
        total[s, t] = total[s, t] + mine[t]
        for k in range(3):
            skip = far - 4 if k == 2 and t == TREES - 1 else STEPS

            @pl.when((s < 2 ** k) & (s != skip))
            def _():
                to_parent(s + 2 ** k, t, k).wait_recv()
                total[s, t] = total[s, t] + child[s + 2 ** k - 1, t]
        if t == TREES - 1:
            for which, parent in ((0, far - 4), (1, far - 2)):
                @pl.when(s == parent)
                def _():
                    add_far(s, which)

    def step_back(i, carry):
        s = back_order(i)
        slot = lax.rem(i, RING)
        with jax.named_scope('give'):
            give(s, slot)

            @pl.when(i + RING < STEPS)
            def _():
                load(back_order(i + RING), slot, 1)
                load(back_order(i + RING), slot, 0)

            @pl.when(i == 0)
            def _():
                send_small()
        with jax.named_scope('take'):
            join(s)
            for t in range(TREES):
                gather_children(s, t)
                for k in range(3):
                    skip = far if k == 2 and t == TREES - 1 else STEPS

                    @pl.when((s >= 2 ** k) & (s < 2 ** (k + 1)) & (s != skip))
                    def _():
                        to_parent(s, t, k).start()
                if t == TREES - 1:
                    @pl.when(s == far)
                    def _():
                        from_far_to(0).start()
                        from_far_to(1).start()
        return carry

    lax.fori_loop(0, STEPS - 1, step_back, 0)
    chips = n // 2
    half, share = part.shape[0] // 2, part.shape[0] // n
    mine_rows = pl.ds(pl.multiple_of(core * half, 8), half)
    their_rows = pl.ds(pl.multiple_of((1 - core) * half, 8), half)
    most = slice(0, (TREES - 1) * width)
    with jax.named_scope('give'):
        give(0, (STEPS - 1) % RING)
        join(0)

    def hidden_grad(t):
        gather_children(0, t)
        g_one[:, chunks[t]] = jnp.where(z_one[:, chunks[t]] > 0.0, total[0, t], 0.0).astype(jnp.bfloat16)

    def weight_grad(out_rows, cols):
        return lax.dot_general(s_one[out_rows, cols], g_one[:, cols], COL_CONTRACT, preferred_element_type=jnp.float32)

    with jax.named_scope('take'):
        for t in range(TREES - 1):
            hidden_grad(t)
        part[...] = weight_grad(slice(None), most)
        hidden_grad(TREES - 1)
    with jax.named_scope('dw'):
        part[their_rows] = part[their_rows] + weight_grad(their_rows, chunks[-1])
        over = remote(part.at[their_rows], pair, psend, precv, partner)
        over.start()
        part[mine_rows] = part[mine_rows] + weight_grad(mine_rows, chunks[-1])
    reduce_small()
    with jax.named_scope('drain'):
        gather_drain(buf, sems_x)
        gather_drain(h_buf, sems_h)
        remote(stage, stage, dsend, drecv.at[0], partner).wait_send()
        remote(child, child, csend, crecv.at[0, 0], partner).wait_send()
    with jax.named_scope('pair'):
        over.wait()
        pair[...] = pair[...] + part[mine_rows]

    def share_of(q):
        return pl.ds(pl.multiple_of(q * share, 8), share)

    for to in other_chips(chip):
        remote(pair.at[share_of(to)], parts.at[chip], fsend, frecv, to * 2 + core).start()
    parts[chip] = pair[share_of(chip)]
    with jax.named_scope('red'):
        wait_all(parts.at[pl.ds(0, chips - 1)], fsend, frecv)
    own = whole.at[pl.ds(pl.multiple_of(core * half + chip * share, 8), share)]
    own[...] = jnp.sum(parts[...], axis=0)
    for to in other_chips(chip):
        remote(own, own, gsend, grecv, to * 2 + core).start()
    with jax.named_scope('spread'):
        wait_all(whole.at[pl.ds(0, (chips - 1) * share)], gsend, grecv)
    swap = remote(whole.at[mine_rows], whole.at[mine_rows], qsend, qrecv, partner)
    swap.start()
    finish_small()
    dw2_ref[...] = small_whole[0:dw2_ref.shape[0]]
    loss_ref[...] = small_whole[edge:edge + 8]
    with jax.named_scope('swap'):
        swap.wait()
    dw_ref[...] = whole[0:feats]


def finish_kernel(loss_in, dw_in, dw2_in, loss_ref, dw_ref, dw2_ref):
    loss_ref[...] = loss_in[0:1, 0:1]
    dw_ref[...] = dw_in[...]
    dw2_ref[...] = dw2_in[...]


def train_step(x_rows, w_one, w2t, labels, mask, adj):
    rows, nodes = adj.shape
    n = nodes // rows
    feats, width = x_rows.shape[0], rows // TREES
    classes, hidden = w2t.shape
    units = n * TREES
    small = -(-classes // 8) * 8 + 8
    share = -(-feats // (8 * n)) * 8
    vmem, hbm = pl.BlockSpec(memory_space=pltpu.VMEM), pl.BlockSpec(memory_space=pl.ANY)
    dma, f32, bf16 = pltpu.SemaphoreType.DMA, jnp.float32, jnp.bfloat16
    block = (TREES, hidden, width)
    loss, dw_one, dw_two = pl.pallas_call(
        functools.partial(step_kernel, n),
        name='step',
        out_shape=(pltpu.VMEM((8, hidden), f32), pltpu.VMEM((feats, hidden), f32), pltpu.VMEM((classes, hidden), f32)),
        in_specs=[hbm] * 6,
        out_specs=(vmem,) * 3,
        scratch_shapes=[
            pltpu.VMEM((RING * 8, rows, width), bf16), pltpu.VMEM((units, feats, width), bf16), pltpu.VMEM((feats, rows), f32),
            pltpu.VMEM((units, hidden, width), bf16), pltpu.VMEM((n * share, rows), bf16), pltpu.VMEM((hidden, rows), f32),
            pltpu.VMEM((hidden, rows), bf16), pltpu.VMEM((feats, hidden), f32), pltpu.VMEM((small, hidden), f32), pltpu.VMEM((n, 8, 128), f32),
            pltpu.VMEM((STEPS, *block), f32), pltpu.VMEM(block, f32), pltpu.VMEM((STEPS, *block), f32), pltpu.VMEM((STEPS - 1, *block), f32),
            pltpu.VMEM((n * share, hidden), f32), pltpu.VMEM((n // 2, share, hidden), f32), pltpu.VMEM((n * share, hidden), f32),
            pltpu.VMEM((n, 8, hidden), f32), pltpu.VMEM((small, hidden), f32), pltpu.VMEM((n // 2 * share, hidden), f32),
            pltpu.VMEM((classes, rows), bf16), pltpu.VMEM((hidden, rows), bf16), pltpu.VMEM((1, rows), f32),
            pltpu.VMEM((classes, hidden), f32), pltpu.VMEM((1, rows), jnp.int32), pltpu.VMEM((1, rows), jnp.int32),
            dma((RING, 2)), dma, dma((4,)), dma, dma, dma, dma((STEPS,)), dma, dma((STEPS - 1, TREES)), *[dma] * 13, *gather_sems(), *gather_sems()],
        compiler_params=pltpu.CompilerParams(collective_id=0, has_side_effects=True, vmem_limit_bytes=62000000),
        cost_estimate=pl.CostEstimate(flops=2 * rows * nodes * (feats + 2 * hidden), bytes_accessed=6 * rows * nodes, transcendentals=0),
    )(*[pltpu.with_memory_space_constraint(x, pltpu.HBM) for x in (x_rows, w_one, w2t, labels, mask, adj)])
    return pl.pallas_call(
        finish_kernel,
        name='finish',
        out_shape=(jax.ShapeDtypeStruct((1, 1), f32), jax.ShapeDtypeStruct((feats, hidden), f32), jax.ShapeDtypeStruct((classes, hidden), f32)),
        in_specs=[vmem] * 3,
        out_specs=(vmem,) * 3,
    )(*[pltpu.with_memory_space_constraint(x, pltpu.VMEM) for x in (loss, dw_one, dw_two)])


def solution(mesh):
    axis_name = AXIS

    def local_step(adj_rows, feat_rows, w_one, w_two, label_rows, mask_rows):
        rows = adj_rows.shape[0]
        loss, dw_one, dw_two = train_step(feat_rows.T, w_one, w_two.T, label_rows.reshape(1, rows), mask_rows.reshape(1, rows), adj_rows)
        return loss.reshape(1), dw_one, dw_two.T

    return jax.shard_map(local_step, mesh=mesh, in_specs=(P(axis_name, None), P(axis_name, None), P(None, None), P(None, None), P(axis_name), P(axis_name)), out_specs=(P(None), P(None, None), P(None, None)), check_vma=False)
```

```python
import functools

import jax
import jax.numpy as jnp
from jax import lax
from jax.experimental import pallas as pl
from jax.experimental.pallas import tpu as pltpu
from jax.sharding import PartitionSpec as P

MESH = pl.DeviceIdType.MESH
AXIS = 'nodes'
TREES = 4
RING = 4
STEPS = 8
COL_CONTRACT = (((1,), (1,)), ((), ()))
ROW_CONTRACT = (((0,), (0,)), ((), ()))


def tree_axis(tree, k, core, chip):
    if tree < 3:
        weight = 2 ** ((tree + k) % 3)
        return weight, lax.rem(chip // weight, 2)
    weight = (1 - core) * 2 ** k + core * 2 ** (2 - k)
    low, high = lax.rem(chip // 2 ** k, 2), lax.rem(chip // 2 ** (2 - k), 2)
    return weight, (1 - core) * low + core * high


def chip_at(tree, offset, core, chip):
    out = chip
    for k in range(3):
        weight, bit = tree_axis(tree, k, core, chip)
        out = out + lax.rem(offset // 2 ** k, 2) * weight * (1 - 2 * bit)
    return out


def early_order(place):
    pair = (place + 1) // 2
    return place + (pair * (4 - pair)) // 4 * (7 - 2 * place)


def other_chips(chip):
    for flips in ((1, 2, 4), (1, 4), (1, 2), (2, 4), (1,), (2,), (4,)):
        yield chip + sum(w * (1 - 2 * lax.rem(chip // w, 2)) for w in flips)


def unit_at(tree, offset, core, chip):
    return (chip_at(tree, offset, core, chip) * 2 + core) * TREES + tree


def neighbour(tree, k, core, chip):
    weight, bit = tree_axis(tree, k, core, chip)
    return (chip + weight * (1 - 2 * bit)) * 2 + core


def remote(src, dst, send_sem, recv_sem, device):
    return pltpu.make_async_remote_copy(src_ref=src, dst_ref=dst, send_sem=send_sem, recv_sem=recv_sem, device_id=(device,), device_id_type=MESH)


def place():
    me = lax.axis_index(AXIS)
    core, chip = lax.rem(me, 2), me // 2
    return me, core, chip, chip * 2 + 1 - core


def gather_send(buf, sems, tree, offset, k, unit, rows=slice(None)):
    send, recv, hand = sems
    me, core, chip, partner = place()
    ref = buf.at[unit, rows]
    remote(ref, ref, send, recv.at[offset + 2 ** k - 1, tree], neighbour(tree, k, core, chip)).start()


def gather_hand(buf, sems, slot, unit):
    send, recv, hand = sems
    me, core, chip, partner = place()
    remote(buf.at[unit], buf.at[unit], send, hand.at[slot], partner).start()


def gather_start(buf, sems, links):
    me = lax.axis_index(AXIS)
    for k in range(links):
        for t in range(TREES):
            gather_send(buf, sems, t, 0, k, me * TREES + t)
        if k == 0:
            for t in range(TREES):
                gather_hand(buf, sems, 0, me * TREES + t)


def gather_arrive(buf, sems, s, links, trees=range(TREES), slot=None, cut=None):
    send, recv, hand = sems
    me, core, chip, partner = place()
    units = {t: unit_at(t, s, core, chip) for t in trees}
    for t, u in units.items():
        remote(buf.at[u], buf.at[u], send, recv.at[s - 1, t], partner).wait_recv()
        split = cut is not None and t == TREES - 1

        @pl.when(s == 1)
        def _():
            gather_send(buf, sems, t, s, 1, u)

        @pl.when((s > 1) & (s < (3 if split else 4)))
        def _():
            gather_send(buf, sems, t, s, 2, u)
        if split:
            @pl.when(s == 3)
            def _():
                gather_send(buf, sems, t, s, 2, u, slice(0, cut))

            @pl.when(s == 5)
            def _():
                gather_send(buf, sems, t, s, 1, u, slice(cut, None))
        gather_hand(buf, sems, s if slot is None else slot, u)

    @pl.when(s == 1)
    def _():
        if links < 3:
            for t in range(TREES):
                gather_send(buf, sems, t, 0, 2, me * TREES + t)
        for t, u in units.items():
            gather_send(buf, sems, t, s, 2, u)


def gather_take(buf, sems, slot, count=TREES):
    send, recv, hand = sems
    me, core, chip, partner = place()
    units = buf.at[pl.ds(0, count)]
    remote(units, units, send, hand.at[slot], partner).wait_recv()


def gather_drain(buf, sems):
    send, recv, hand = sems
    me, core, chip, partner = place()
    sent = buf.at[pl.ds(0, TREES * (STEPS - 1 + STEPS))]
    remote(sent, sent, send, hand.at[0], partner).wait_send()


def gather_sems():
    dma = pltpu.SemaphoreType.DMA
    return [dma, dma((STEPS - 1, TREES)), dma((STEPS + 1,))]


def barrier_near():
    me, core, chip, partner = place()
    sem = pltpu.get_barrier_semaphore()
    pl.semaphore_signal(sem, inc=1, device_id=(partner,), device_id_type=MESH)
    for k in range(3):
        pl.semaphore_signal(sem, inc=1, device_id=(neighbour(0, k, core, chip),), device_id_type=MESH)
    pl.semaphore_wait(sem, 4)


def send_all(n, src, dst, send_sem, recv_sem):
    me = lax.axis_index(AXIS)
    for i in range(1, n):
        to = lax.rem(me + i, n)
        remote(src(to), dst, send_sem, recv_sem, to).start()


def wait_all(ref, send_sem, recv_sem):
    me, core, chip, partner = place()
    copy = remote(ref, ref, send_sem, recv_sem, partner)
    copy.wait_send()
    copy.wait_recv()


def step_kernel(n, x_ref, w_hbm, w2t_hbm, y_hbm, m_hbm, adj, loss_ref, dw_ref, dw2_ref,
                ring, buf, acc, h_buf, s_one, z_one, u_two, w_v, small, count, stage, mine, total, child, part, parts, whole,
                small_parts, small_whole, pair, g_two, g_one, picked, w2t_ref, y_ref, m_ref,
                ring_sem, x_sem, w_sem, count_send, count_recv, dsend, drecv, csend, crecv, fsend, frecv, gsend, grecv,
                ssend, srecv, bsend, brecv, psend, precv, qsend, qrecv, cut_sem, *sems):
    me, core, chip, partner = place()
    sems_x, sems_h = sems[:3], sems[3:]
    width = buf.shape[2]
    feats, rows = acc.shape
    hidden = h_buf.shape[1]
    chunks = [slice(t * width, (t + 1) * width) for t in range(TREES)]

    def slab(s, slot, j):
        u = unit_at(j % TREES, s, core if j < TREES else 1 - core, chip)
        return pltpu.make_async_copy(adj.at[:, pl.ds(pl.multiple_of(u * width, width), width)], ring.at[slot * 8 + j], ring_sem.at[slot, j // TREES])

    def load(s, slot, half):
        for t in range(TREES):
            slab(s, slot, half * TREES + t).start()

    def loaded(slot, half):
        four = ring.at[pl.ds(0, TREES)]
        pltpu.make_async_copy(four, four, ring_sem.at[slot, half]).wait()

    with jax.named_scope('start'):
        fetch = [pltpu.make_async_copy(x_ref.at[:, pl.ds(t * width, width)], buf.at[me * TREES + t], x_sem) for t in range(TREES)]
        for copy in fetch:
            copy.start()
        barrier_near()
        four = buf.at[pl.ds(0, TREES)]
        pltpu.make_async_copy(four, four, x_sem).wait()
    gather_start(buf, sems_x, 2)
    params = [pltpu.make_async_copy(src, dst, w_sem.at[i]) for i, (src, dst) in enumerate(((w_hbm, w_v), (w2t_hbm, w2t_ref), (y_hbm, y_ref), (m_hbm, m_ref)))]
    for copy in params:
        copy.start()
    for s in range(RING):
        for half in range(2):
            load(s, s, half)
    acc[...] = jnp.zeros_like(acc)

    def terms(units_ref, s, slot, half, trees=range(TREES)):
        which = core if half == 0 else 1 - core
        return [(units_ref, unit_at(t, s, which, chip), slot * 8 + half * TREES + t) for t in trees]

    def aggregate(out, pairs):
        for cols in chunks:
            out[:, cols] += sum(lax.dot_general(ref[u], ring[j, cols], COL_CONTRACT, preferred_element_type=jnp.float32) for ref, u, j in pairs)

    def step_one(s, carry):
        with jax.named_scope('arrive'):
            @pl.when(s > 0)
            def _():
                gather_arrive(buf, sems_x, s, 2, cut=cut)
        for half in range(2):
            with jax.named_scope('consume'):
                if half == 1:
                    gather_take(buf, sems_x, s)
                slot = lax.rem(s, RING)
                loaded(slot, half)
                aggregate(acc, terms(buf, s, slot, half))
                late = s // RING
                load((1 - late) * (s + RING) + late * early_order(s - late * RING), slot, half)
        return carry

    cut = feats * 2 // 3 // 16 * 16
    final, slot = STEPS - 1, (STEPS - 1) % RING
    lax.fori_loop(0, final, step_one, 0)
    early, late = (range(TREES - 1), final), (range(TREES - 1, TREES), STEPS)
    for half in range(2):
        for trees, hand in (early, late):
            with jax.named_scope('consume'):
                if half == 0:
                    gather_arrive(buf, sems_x, final, 2, trees, hand, cut)
                else:
                    gather_take(buf, sems_x, hand, len(trees))
                if hand == final:
                    loaded(slot, half)
                aggregate(acc, terms(buf, final, slot, half, trees))
    for half in range(2):
        load(early_order(final - RING), slot, half)
    with jax.named_scope('mid'):
        for copy in params:
            copy.wait()
        s_one[0:feats] = acc[...].astype(jnp.bfloat16)
        s_one[feats:] = jnp.zeros_like(s_one[feats:])
        w_rows = w_v[...].astype(jnp.bfloat16)
        for t, cols in enumerate(chunks):
            z = lax.dot_general(w_rows, s_one[0:feats, cols], ROW_CONTRACT, preferred_element_type=jnp.float32)
            z_one[:, cols] = z
            h_buf[me * TREES + t] = jnp.maximum(z, 0.0).astype(jnp.bfloat16)
    gather_start(h_buf, sems_h, 3)
    weight = m_ref[...].astype(jnp.float32)
    count[me] = jnp.broadcast_to(jnp.sum(weight, axis=1, keepdims=True), count.shape[1:])
    send_all(n, lambda to: count.at[me], count.at[me], count_send, count_recv)
    two = acc.at[0:hidden]

    def take_two(p, half):
        loaded(lax.rem(p, RING), half)
        return terms(h_buf, early_order(p), lax.rem(p, RING), half)

    def back_order(i):
        return early_order(STEPS - 1 - i)

    def load_two(p, half):
        late = p // RING
        load((1 - late) * early_order(p + RING - late * RING) + late * back_order(p - late * RING), lax.rem(p, RING), half)

    two[...] = jnp.zeros_like(two)
    with jax.named_scope('consume'):
        aggregate(two, take_two(0, 0))
        load_two(0, 0)
        gather_take(h_buf, sems_h, 0)
        aggregate(two, take_two(0, 1))
        load_two(0, 1)
    with jax.named_scope('arrive'):
        gather_arrive(h_buf, sems_h, 1, 3)
    with jax.named_scope('consume'):
        aggregate(two, take_two(1, 0))
        load_two(1, 0)

    for p in range(2, STEPS):
        with jax.named_scope('arrive'):
            gather_arrive(h_buf, sems_h, early_order(p), 3)
            gather_take(h_buf, sems_h, early_order(p - 1))
        with jax.named_scope('consume'):
            aggregate(two, take_two(p - 1, 1) + take_two(p, 0))
            load_two(p - 1, 1)
            load_two(p, 0)
    with jax.named_scope('last'):
        gather_take(h_buf, sems_h, STEPS - 1)
        aggregate(two, take_two(STEPS - 1, 1))
        load_two(STEPS - 1, 1)
    with jax.named_scope('soft'):
        wait_all(count.at[pl.ds(0, n - 1)], count_send, count_recv)
        labelled = jnp.sum(count[...], axis=0)[0:1, 0:1]
        s_two = two[...].astype(jnp.bfloat16)
        w_two = w2t_ref[...].astype(jnp.bfloat16)
        logits = jnp.dot(w_two, s_two, preferred_element_type=jnp.float32)
        shifted = logits - jnp.max(logits, axis=0, keepdims=True)
        log_prob = shifted - jnp.log(jnp.sum(jnp.exp(shifted), axis=0, keepdims=True))
        hot = lax.broadcasted_iota(jnp.int32, logits.shape, 0) == y_ref[...]
        grad = (weight * (jnp.exp(log_prob) - hot.astype(jnp.float32)) / labelled).astype(jnp.bfloat16)
        u_two[...] = lax.dot_general(w_two, grad, ROW_CONTRACT, preferred_element_type=jnp.float32).astype(jnp.bfloat16)
        g_two[...] = grad
        picked[...] = -weight * jnp.sum(jnp.where(hot, log_prob, 0.0), axis=0, keepdims=True)
    classes = g_two.shape[0]
    edge = small.shape[0] - 8
    owners = small.shape[0] // 8
    tile = pl.ds(pl.multiple_of(me * 8, 8), 8)

    def send_small():
        loss = jnp.sum(picked[...], axis=1, keepdims=True)
        labelled = jnp.sum(count[...], axis=0)[0:1, 0:1]
        small[0:classes] = lax.dot_general(g_two[...], two[...].astype(jnp.bfloat16), COL_CONTRACT, preferred_element_type=jnp.float32)
        small[classes:edge] = jnp.zeros((edge - classes, hidden), jnp.float32)
        small[edge:] = jnp.broadcast_to(loss / labelled, (8, hidden))
        for o in range(owners):
            @pl.when(me != o)
            def _():
                remote(small.at[pl.ds(o * 8, 8)], small_parts.at[me], ssend, srecv, o).start()

    def to_partner(s, t):
        return remote(stage.at[s, t], total.at[s, t], dsend, drecv.at[s], partner)

    def to_parent(s, t, k):
        return remote(total.at[s, t], child.at[s - 1, t], csend, crecv.at[s - 1, t], neighbour(t, k, core, chip))

    def reduce_small():
        @pl.when(me < owners)
        def _():
            small_parts[me] = small[tile]
            got = small_parts.at[pl.ds(0, n - 1)]
            remote(got, got, ssend, srecv, partner).wait_recv()
            small_whole[tile] = jnp.sum(small_parts[...], axis=0)
            for i in range(1, n):
                remote(small_whole.at[tile], small_whole.at[tile], bsend, brecv, lax.rem(me + i, n)).start()

    def finish_small():
        sent = small_parts.at[pl.ds(0, n - 1)]
        fewer, every = small_whole.at[pl.ds(0, owners * 8 - 8)], small_whole.at[pl.ds(0, owners * 8)]

        @pl.when(me < owners)
        def _():
            remote(sent, sent, bsend, brecv, partner).wait_send()
            remote(fewer, fewer, ssend, brecv, partner).wait_send()
            remote(fewer, fewer, ssend, brecv, partner).wait_recv()

        @pl.when(me >= owners)
        def _():
            remote(every, every, ssend, brecv, partner).wait_send()
            remote(every, every, ssend, brecv, partner).wait_recv()

    far, edge_row = STEPS - 2, hidden * 2 // 3 // 8 * 8 + 8

    def from_far_to(which):
        rows, k = ((slice(0, edge_row), 2), (slice(edge_row, hidden), 1))[which]
        sem = cut_sem if which else crecv.at[far - 1, TREES - 1]
        return remote(total.at[far, TREES - 1, rows], child.at[far - 1, TREES - 1, rows], csend, sem, neighbour(TREES - 1, k, core, chip))

    def add_far(s, which):
        from_far_to(which).wait_recv()
        rows = (slice(0, edge_row), slice(edge_row, hidden))[which]
        total[s, TREES - 1, rows] = total[s, TREES - 1, rows] + child[far - 1, TREES - 1, rows]

    def give(s, slot):
        loaded(slot, 1)
        for t in range(TREES):
            stage[s, t] = jnp.dot(u_two[...], ring[slot * 8 + TREES + t], preferred_element_type=jnp.float32)
        for t in range(TREES):
            to_partner(s, t).start()
        loaded(slot, 0)
        for t in range(TREES):
            mine[t] = jnp.dot(u_two[...], ring[slot * 8 + t], preferred_element_type=jnp.float32)

    def join(s):
        remote(total.at[s], total.at[s], dsend, drecv.at[s], partner).wait_recv()

    def gather_children(s, t):
        total[s, t] = total[s, t] + mine[t]
        for k in range(3):
            skip = far - 4 if k == 2 and t == TREES - 1 else STEPS

            @pl.when((s < 2 ** k) & (s != skip))
            def _():
                to_parent(s + 2 ** k, t, k).wait_recv()
                total[s, t] = total[s, t] + child[s + 2 ** k - 1, t]
        if t == TREES - 1:
            for which, parent in ((0, far - 4), (1, far - 2)):
                @pl.when(s == parent)
                def _():
                    add_far(s, which)

    def step_back(i, carry):
        s = back_order(i)
        slot = lax.rem(i, RING)
        with jax.named_scope('give'):
            give(s, slot)

            @pl.when(i + RING < STEPS)
            def _():
                load(back_order(i + RING), slot, 1)
                load(back_order(i + RING), slot, 0)

            @pl.when(i == 0)
            def _():
                send_small()
        with jax.named_scope('take'):
            join(s)
            for t in range(TREES):
                gather_children(s, t)
                for k in range(3):
                    skip = far if k == 2 and t == TREES - 1 else STEPS

                    @pl.when((s >= 2 ** k) & (s < 2 ** (k + 1)) & (s != skip))
                    def _():
                        to_parent(s, t, k).start()
                if t == TREES - 1:
                    @pl.when(s == far)
                    def _():
                        from_far_to(0).start()
                        from_far_to(1).start()
        return carry

    lax.fori_loop(0, STEPS - 1, step_back, 0)
    chips = n // 2
    half, share = part.shape[0] // 2, part.shape[0] // n
    mine_rows = pl.ds(pl.multiple_of(core * half, 8), half)
    their_rows = pl.ds(pl.multiple_of((1 - core) * half, 8), half)
    most = slice(0, (TREES - 1) * width)
    with jax.named_scope('give'):
        give(0, (STEPS - 1) % RING)
        join(0)

    def hidden_grad(t):
        gather_children(0, t)
        g_one[:, chunks[t]] = jnp.where(z_one[:, chunks[t]] > 0.0, total[0, t], 0.0).astype(jnp.bfloat16)

    def weight_grad(out_rows, cols):
        return lax.dot_general(s_one[out_rows, cols], g_one[:, cols], COL_CONTRACT, preferred_element_type=jnp.float32)

    with jax.named_scope('take'):
        for t in range(TREES - 1):
            hidden_grad(t)
        part[...] = weight_grad(slice(None), most)
        hidden_grad(TREES - 1)
    with jax.named_scope('dw'):
        part[their_rows] = part[their_rows] + weight_grad(their_rows, chunks[-1])
        over = remote(part.at[their_rows], pair, psend, precv, partner)
        over.start()
        part[mine_rows] = part[mine_rows] + weight_grad(mine_rows, chunks[-1])
    reduce_small()
    with jax.named_scope('drain'):
        gather_drain(buf, sems_x)
        gather_drain(h_buf, sems_h)
        remote(stage, stage, dsend, drecv.at[0], partner).wait_send()
        remote(child, child, csend, crecv.at[0, 0], partner).wait_send()
    with jax.named_scope('pair'):
        over.wait()
        pair[...] = pair[...] + part[mine_rows]

    def share_of(q):
        return pl.ds(pl.multiple_of(q * share, 8), share)

    for to in other_chips(chip):
        remote(pair.at[share_of(to)], parts.at[chip], fsend, frecv, to * 2 + core).start()
    parts[chip] = pair[share_of(chip)]
    with jax.named_scope('red'):
        wait_all(parts.at[pl.ds(0, chips - 1)], fsend, frecv)
    own = whole.at[pl.ds(pl.multiple_of(core * half + chip * share, 8), share)]
    own[...] = jnp.sum(parts[...], axis=0)
    for to in other_chips(chip):
        remote(own, own, gsend, grecv, to * 2 + core).start()
    with jax.named_scope('spread'):
        wait_all(whole.at[pl.ds(0, (chips - 1) * share)], gsend, grecv)
    swap = remote(whole.at[mine_rows], whole.at[mine_rows], qsend, qrecv, partner)
    swap.start()
    finish_small()
    dw2_ref[...] = small_whole[0:dw2_ref.shape[0]]
    loss_ref[...] = small_whole[edge:edge + 8]
    with jax.named_scope('swap'):
        swap.wait()
    dw_ref[...] = whole[0:feats]


def finish_kernel(loss_in, dw_in, dw2_in, loss_ref, dw_ref, dw2_ref):
    loss_ref[...] = loss_in[0:1, 0:1]
    dw_ref[...] = dw_in[...]
    dw2_ref[...] = dw2_in[...]


def train_step(x_rows, w_one, w2t, labels, mask, adj):
    rows, nodes = adj.shape
    n = nodes // rows
    feats, width = x_rows.shape[0], rows // TREES
    classes, hidden = w2t.shape
    units = n * TREES
    small = -(-classes // 8) * 8 + 8
    share = -(-feats // (8 * n)) * 8
    vmem, hbm = pl.BlockSpec(memory_space=pltpu.VMEM), pl.BlockSpec(memory_space=pl.ANY)
    dma, f32, bf16 = pltpu.SemaphoreType.DMA, jnp.float32, jnp.bfloat16
    block = (TREES, hidden, width)
    loss, dw_one, dw_two = pl.pallas_call(
        functools.partial(step_kernel, n),
        name='step',
        out_shape=(pltpu.VMEM((8, hidden), f32), pltpu.VMEM((feats, hidden), f32), pltpu.VMEM((classes, hidden), f32)),
        in_specs=[hbm] * 6,
        out_specs=(vmem,) * 3,
        scratch_shapes=[
            pltpu.VMEM((RING * 8, rows, width), bf16), pltpu.VMEM((units, feats, width), bf16), pltpu.VMEM((feats, rows), f32),
            pltpu.VMEM((units, hidden, width), bf16), pltpu.VMEM((n * share, rows), bf16), pltpu.VMEM((hidden, rows), f32),
            pltpu.VMEM((hidden, rows), bf16), pltpu.VMEM((feats, hidden), f32), pltpu.VMEM((small, hidden), f32), pltpu.VMEM((n, 1, 128), f32),
            pltpu.VMEM((STEPS, *block), f32), pltpu.VMEM(block, f32), pltpu.VMEM((STEPS, *block), f32), pltpu.VMEM((STEPS - 1, *block), f32),
            pltpu.VMEM((n * share, hidden), f32), pltpu.VMEM((n // 2, share, hidden), f32), pltpu.VMEM((n * share, hidden), f32),
            pltpu.VMEM((n, 8, hidden), f32), pltpu.VMEM((small, hidden), f32), pltpu.VMEM((n // 2 * share, hidden), f32),
            pltpu.VMEM((classes, rows), bf16), pltpu.VMEM((hidden, rows), bf16), pltpu.VMEM((1, rows), f32),
            pltpu.VMEM((classes, hidden), f32), pltpu.VMEM((1, rows), jnp.int32), pltpu.VMEM((1, rows), jnp.int32),
            dma((RING, 2)), dma, dma((4,)), dma, dma, dma, dma((STEPS,)), dma, dma((STEPS - 1, TREES)), *[dma] * 13, *gather_sems(), *gather_sems()],
        compiler_params=pltpu.CompilerParams(collective_id=0, has_side_effects=True, vmem_limit_bytes=62000000),
        cost_estimate=pl.CostEstimate(flops=2 * rows * nodes * (feats + 2 * hidden), bytes_accessed=6 * rows * nodes, transcendentals=0),
    )(*[pltpu.with_memory_space_constraint(x, pltpu.HBM) for x in (x_rows, w_one, w2t, labels, mask, adj)])
    return pl.pallas_call(
        finish_kernel,
        name='finish',
        out_shape=(jax.ShapeDtypeStruct((1, 1), f32), jax.ShapeDtypeStruct((feats, hidden), f32), jax.ShapeDtypeStruct((classes, hidden), f32)),
        in_specs=[vmem] * 3,
        out_specs=(vmem,) * 3,
    )(*[pltpu.with_memory_space_constraint(x, pltpu.VMEM) for x in (loss, dw_one, dw_two)])


def solution(mesh):
    axis_name = AXIS

    def local_step(adj_rows, feat_rows, w_one, w_two, label_rows, mask_rows):
        rows = adj_rows.shape[0]
        loss, dw_one, dw_two = train_step(feat_rows.T, w_one, w_two.T, label_rows.reshape(1, rows), mask_rows.reshape(1, rows), adj_rows)
        return loss.reshape(1), dw_one, dw_two.T

    return jax.shard_map(local_step, mesh=mesh, in_specs=(P(axis_name, None), P(axis_name, None), P(None, None), P(None, None), P(axis_name), P(axis_name)), out_specs=(P(None), P(None, None), P(None, None)), check_vma=False)
```

```python
import functools

import jax
import jax.numpy as jnp
from jax import lax
from jax.experimental import pallas as pl
from jax.experimental.pallas import tpu as pltpu
from jax.sharding import PartitionSpec as P

MESH = pl.DeviceIdType.MESH
AXIS = 'nodes'
TREES = 4
RING = 4
STEPS = 8
COL_CONTRACT = (((1,), (1,)), ((), ()))
ROW_CONTRACT = (((0,), (0,)), ((), ()))


def tree_axis(tree, k, core, chip):
    if tree < 3:
        weight = 2 ** ((tree + k) % 3)
        return weight, lax.rem(chip // weight, 2)
    weight = (1 - core) * 2 ** k + core * 2 ** (2 - k)
    low, high = lax.rem(chip // 2 ** k, 2), lax.rem(chip // 2 ** (2 - k), 2)
    return weight, (1 - core) * low + core * high


def chip_at(tree, offset, core, chip):
    out = chip
    for k in range(3):
        weight, bit = tree_axis(tree, k, core, chip)
        out = out + lax.rem(offset // 2 ** k, 2) * weight * (1 - 2 * bit)
    return out


def early_order(place):
    pair = (place + 1) // 2
    return place + (pair * (4 - pair)) // 4 * (7 - 2 * place)


def other_chips(chip):
    for flips in ((1, 2, 4), (1, 4), (1, 2), (2, 4), (1,), (2,), (4,)):
        yield chip + sum(w * (1 - 2 * lax.rem(chip // w, 2)) for w in flips)


def unit_at(tree, offset, core, chip):
    return (chip_at(tree, offset, core, chip) * 2 + core) * TREES + tree


def neighbour(tree, k, core, chip):
    weight, bit = tree_axis(tree, k, core, chip)
    return (chip + weight * (1 - 2 * bit)) * 2 + core


def remote(src, dst, send_sem, recv_sem, device):
    return pltpu.make_async_remote_copy(src_ref=src, dst_ref=dst, send_sem=send_sem, recv_sem=recv_sem, device_id=(device,), device_id_type=MESH)


def place():
    me = lax.axis_index(AXIS)
    core, chip = lax.rem(me, 2), me // 2
    return me, core, chip, chip * 2 + 1 - core


def gather_send(buf, sems, tree, offset, k, unit, rows=slice(None)):
    send, recv, hand = sems
    me, core, chip, partner = place()
    ref = buf.at[unit, rows]
    remote(ref, ref, send, recv.at[offset + 2 ** k - 1, tree], neighbour(tree, k, core, chip)).start()


def gather_hand(buf, sems, slot, unit):
    send, recv, hand = sems
    me, core, chip, partner = place()
    remote(buf.at[unit], buf.at[unit], send, hand.at[slot], partner).start()


def gather_start(buf, sems, links):
    me = lax.axis_index(AXIS)
    for k in range(links):
        for t in range(TREES):
            gather_send(buf, sems, t, 0, k, me * TREES + t)
        if k == 0:
            for t in range(TREES):
                gather_hand(buf, sems, 0, me * TREES + t)


def gather_arrive(buf, sems, s, links, trees=range(TREES), slot=None, cut=None):
    send, recv, hand = sems
    me, core, chip, partner = place()
    units = {t: unit_at(t, s, core, chip) for t in trees}
    for t, u in units.items():
        remote(buf.at[u], buf.at[u], send, recv.at[s - 1, t], partner).wait_recv()
        split = cut is not None and t == TREES - 1

        @pl.when(s == 1)
        def _():
            gather_send(buf, sems, t, s, 1, u)

        @pl.when((s > 1) & (s < (3 if split else 4)))
        def _():
            gather_send(buf, sems, t, s, 2, u)
        if split:
            @pl.when(s == 3)
            def _():
                gather_send(buf, sems, t, s, 2, u, slice(0, cut))

            @pl.when(s == 5)
            def _():
                gather_send(buf, sems, t, s, 1, u, slice(cut, None))
        gather_hand(buf, sems, s if slot is None else slot, u)

    @pl.when(s == 1)
    def _():
        if links < 3:
            for t in range(TREES):
                gather_send(buf, sems, t, 0, 2, me * TREES + t)
        for t, u in units.items():
            gather_send(buf, sems, t, s, 2, u)


def gather_take(buf, sems, slot, count=TREES):
    send, recv, hand = sems
    me, core, chip, partner = place()
    units = buf.at[pl.ds(0, count)]
    remote(units, units, send, hand.at[slot], partner).wait_recv()


def gather_drain(buf, sems):
    send, recv, hand = sems
    me, core, chip, partner = place()
    sent = buf.at[pl.ds(0, TREES * (STEPS - 1 + STEPS))]
    remote(sent, sent, send, hand.at[0], partner).wait_send()


def gather_sems():
    dma = pltpu.SemaphoreType.DMA
    return [dma, dma((STEPS - 1, TREES)), dma((STEPS + 1,))]


def barrier_near():
    me, core, chip, partner = place()
    sem = pltpu.get_barrier_semaphore()
    pl.semaphore_signal(sem, inc=1, device_id=(partner,), device_id_type=MESH)
    for k in range(3):
        pl.semaphore_signal(sem, inc=1, device_id=(neighbour(0, k, core, chip),), device_id_type=MESH)
    pl.semaphore_wait(sem, 4)


def send_all(n, src, dst, send_sem, recv_sem):
    me = lax.axis_index(AXIS)
    for i in range(1, n):
        to = lax.rem(me + i, n)
        remote(src(to), dst, send_sem, recv_sem, to).start()


def wait_all(ref, send_sem, recv_sem):
    me, core, chip, partner = place()
    copy = remote(ref, ref, send_sem, recv_sem, partner)
    copy.wait_send()
    copy.wait_recv()


def step_kernel(n, x_ref, w_hbm, w2t_hbm, y_hbm, m_hbm, adj, loss_ref, dw_ref, dw2_ref,
                ring, buf, acc, h_buf, s_one, z_one, u_two, w_v, small, count, stage, mine, total, child, part, parts, whole,
                small_parts, small_whole, pair, g_two, g_one, picked, w2t_ref, y_ref, m_ref,
                ring_sem, x_sem, w_sem, count_send, count_recv, dsend, drecv, csend, crecv, fsend, frecv, gsend, grecv,
                ssend, srecv, bsend, brecv, psend, precv, qsend, qrecv, cut_sem, *sems):
    me, core, chip, partner = place()
    sems_x, sems_h = sems[:3], sems[3:]
    width = buf.shape[2]
    feats, rows = acc.shape
    hidden = h_buf.shape[1]
    chunks = [slice(t * width, (t + 1) * width) for t in range(TREES)]

    def slab(s, slot, j):
        u = unit_at(j % TREES, s, core if j < TREES else 1 - core, chip)
        return pltpu.make_async_copy(adj.at[:, pl.ds(pl.multiple_of(u * width, width), width)], ring.at[slot * 8 + j], ring_sem.at[slot, j // TREES])

    def load(s, slot, half):
        for t in range(TREES):
            slab(s, slot, half * TREES + t).start()

    def loaded(slot, half):
        four = ring.at[pl.ds(0, TREES)]
        pltpu.make_async_copy(four, four, ring_sem.at[slot, half]).wait()

    with jax.named_scope('start'):
        fetch = [pltpu.make_async_copy(x_ref.at[:, pl.ds(t * width, width)], buf.at[me * TREES + t], x_sem) for t in range(TREES)]
        for copy in fetch:
            copy.start()
        barrier_near()
        four = buf.at[pl.ds(0, TREES)]
        pltpu.make_async_copy(four, four, x_sem).wait()
    gather_start(buf, sems_x, 2)
    params = [pltpu.make_async_copy(src, dst, w_sem.at[i]) for i, (src, dst) in enumerate(((w_hbm, w_v), (w2t_hbm, w2t_ref), (y_hbm, y_ref), (m_hbm, m_ref)))]
    for copy in params:
        copy.start()
    for s in range(RING):
        for half in range(2):
            load(s, s, half)
    acc[...] = jnp.zeros_like(acc)

    def terms(units_ref, s, slot, half, trees=range(TREES)):
        which = core if half == 0 else 1 - core
        return [(units_ref, unit_at(t, s, which, chip), slot * 8 + half * TREES + t) for t in trees]

    def aggregate(out, pairs):
        for cols in chunks:
            out[:, cols] += sum(lax.dot_general(ref[u], ring[j, cols], COL_CONTRACT, preferred_element_type=jnp.float32) for ref, u, j in pairs)

    def step_one(s, carry):
        with jax.named_scope('arrive'):
            @pl.when(s > 0)
            def _():
                gather_arrive(buf, sems_x, s, 2, cut=cut)
        for half in range(2):
            with jax.named_scope('consume'):
                if half == 1:
                    gather_take(buf, sems_x, s)
                slot = lax.rem(s, RING)
                loaded(slot, half)
                aggregate(acc, terms(buf, s, slot, half))
                late = s // RING
                load((1 - late) * (s + RING) + late * early_order(s - late * RING), slot, half)
        return carry

    cut = feats * 2 // 3 // 16 * 16
    final, slot = STEPS - 1, (STEPS - 1) % RING
    lax.fori_loop(0, final, step_one, 0)
    early, late = (range(TREES - 1), final), (range(TREES - 1, TREES), STEPS)
    for half in range(2):
        for trees, hand in (early, late):
            with jax.named_scope('consume'):
                if half == 0:
                    gather_arrive(buf, sems_x, final, 2, trees, hand, cut)
                else:
                    gather_take(buf, sems_x, hand, len(trees))
                if hand == final:
                    loaded(slot, half)
                aggregate(acc, terms(buf, final, slot, half, trees))
    for half in range(2):
        load(early_order(final - RING), slot, half)
    with jax.named_scope('mid'):
        for copy in params:
            copy.wait()
        s_one[0:feats] = acc[...].astype(jnp.bfloat16)
        s_one[feats:] = jnp.zeros_like(s_one[feats:])
        w_rows = w_v[...].astype(jnp.bfloat16)
        for t, cols in enumerate(chunks):
            z = lax.dot_general(w_rows, s_one[0:feats, cols], ROW_CONTRACT, preferred_element_type=jnp.float32)
            z_one[:, cols] = z
            h_buf[me * TREES + t] = jnp.maximum(z, 0.0).astype(jnp.bfloat16)
    gather_start(h_buf, sems_h, 3)
    weight = m_ref[...].astype(jnp.float32)
    count[me] = jnp.broadcast_to(jnp.sum(weight, axis=1, keepdims=True), count.shape[1:])
    send_all(n, lambda to: count.at[me], count.at[me], count_send, count_recv)
    two = acc.at[0:hidden]

    def take_two(p, half):
        loaded(lax.rem(p, RING), half)
        return terms(h_buf, early_order(p), lax.rem(p, RING), half)

    def back_order(i):
        return early_order(STEPS - 1 - i)

    def load_two(p, half):
        late = p // RING
        load((1 - late) * early_order(p + RING - late * RING) + late * back_order(p - late * RING), lax.rem(p, RING), half)

    two[...] = jnp.zeros_like(two)
    with jax.named_scope('consume'):
        aggregate(two, take_two(0, 0))
        load_two(0, 0)
        gather_take(h_buf, sems_h, 0)
        aggregate(two, take_two(0, 1))
        load_two(0, 1)
    with jax.named_scope('arrive'):
        gather_arrive(h_buf, sems_h, 1, 3)
    with jax.named_scope('consume'):
        aggregate(two, take_two(1, 0))
        load_two(1, 0)

    for p in range(2, STEPS):
        with jax.named_scope('arrive'):
            gather_arrive(h_buf, sems_h, early_order(p), 3)
            gather_take(h_buf, sems_h, early_order(p - 1))
        with jax.named_scope('consume'):
            aggregate(two, take_two(p - 1, 1) + take_two(p, 0))
            load_two(p - 1, 1)
            load_two(p, 0)
    with jax.named_scope('last'):
        gather_take(h_buf, sems_h, STEPS - 1)
        aggregate(two, take_two(STEPS - 1, 1))
        load_two(STEPS - 1, 1)
    with jax.named_scope('soft'):
        wait_all(count.at[pl.ds(0, n - 1)], count_send, count_recv)
        labelled = jnp.sum(count[...], axis=0)[0:1, 0:1]
        s_two = two[...].astype(jnp.bfloat16)
        w_two = w2t_ref[...].astype(jnp.bfloat16)
        logits = jnp.dot(w_two, s_two, preferred_element_type=jnp.float32)
        shifted = logits - jnp.max(logits, axis=0, keepdims=True)
        log_prob = shifted - jnp.log(jnp.sum(jnp.exp(shifted), axis=0, keepdims=True))
        hot = lax.broadcasted_iota(jnp.int32, logits.shape, 0) == y_ref[...]
        grad = (weight * (jnp.exp(log_prob) - hot.astype(jnp.float32)) / labelled).astype(jnp.bfloat16)
        u_two[...] = lax.dot_general(w_two, grad, ROW_CONTRACT, preferred_element_type=jnp.float32).astype(jnp.bfloat16)
        g_two[...] = grad
        picked[...] = -weight * jnp.sum(jnp.where(hot, log_prob, 0.0), axis=0, keepdims=True)
    classes = g_two.shape[0]
    edge = small.shape[0] - 8
    owners = small.shape[0] // 8
    tile = pl.ds(pl.multiple_of(me * 8, 8), 8)

    def send_small():
        loss = jnp.sum(picked[...], axis=1, keepdims=True)
        labelled = jnp.sum(count[...], axis=0)[0:1, 0:1]
        small[0:classes] = lax.dot_general(g_two[...], two[...].astype(jnp.bfloat16), COL_CONTRACT, preferred_element_type=jnp.float32)
        small[classes:edge] = jnp.zeros((edge - classes, hidden), jnp.float32)
        small[edge:] = jnp.broadcast_to(loss / labelled, (8, hidden))
        for o in range(owners):
            @pl.when(me != o)
            def _():
                remote(small.at[pl.ds(o * 8, 8)], small_parts.at[me], ssend, srecv, o).start()

    def to_partner(s, t):
        return remote(stage.at[s, t], total.at[s, t], dsend, drecv.at[s], partner)

    def to_parent(s, t, k):
        return remote(total.at[s, t], child.at[s - 1, t], csend, crecv.at[s - 1, t], neighbour(t, k, core, chip))

    def reduce_small():
        @pl.when(me < owners)
        def _():
            small_parts[me] = small[tile]
            got = small_parts.at[pl.ds(0, n - 1)]
            remote(got, got, ssend, srecv, partner).wait_recv()
            small_whole[tile] = jnp.sum(small_parts[...], axis=0)
            for i in range(1, n):
                remote(small_whole.at[tile], small_whole.at[tile], bsend, brecv, lax.rem(me + i, n)).start()

    def finish_small():
        sent = small_parts.at[pl.ds(0, n - 1)]
        fewer, every = small_whole.at[pl.ds(0, owners * 8 - 8)], small_whole.at[pl.ds(0, owners * 8)]

        @pl.when(me < owners)
        def _():
            remote(sent, sent, bsend, brecv, partner).wait_send()
            remote(fewer, fewer, ssend, brecv, partner).wait_send()
            remote(fewer, fewer, ssend, brecv, partner).wait_recv()

        @pl.when(me >= owners)
        def _():
            remote(every, every, ssend, brecv, partner).wait_send()
            remote(every, every, ssend, brecv, partner).wait_recv()

    far, edge_row = STEPS - 2, hidden * 2 // 3 // 8 * 8 + 8

    def from_far_to(which):
        rows, k = ((slice(0, edge_row), 2), (slice(edge_row, hidden), 1))[which]
        sem = cut_sem if which else crecv.at[far - 1, TREES - 1]
        return remote(total.at[far, TREES - 1, rows], child.at[far - 1, TREES - 1, rows], csend, sem, neighbour(TREES - 1, k, core, chip))

    def add_far(s, which):
        from_far_to(which).wait_recv()
        rows = (slice(0, edge_row), slice(edge_row, hidden))[which]
        total[s, TREES - 1, rows] = total[s, TREES - 1, rows] + child[far - 1, TREES - 1, rows]

    def give(s, slot):
        loaded(slot, 1)
        for two_trees in (range(TREES // 2), range(TREES // 2, TREES)):
            for t in two_trees:
                stage[s, t] = jnp.dot(u_two[...], ring[slot * 8 + TREES + t], preferred_element_type=jnp.float32)
            for t in two_trees:
                to_partner(s, t).start()
        loaded(slot, 0)
        for t in range(TREES):
            mine[t] = jnp.dot(u_two[...], ring[slot * 8 + t], preferred_element_type=jnp.float32)

    def join(s):
        remote(total.at[s], total.at[s], dsend, drecv.at[s], partner).wait_recv()

    def gather_children(s, t):
        total[s, t] = total[s, t] + mine[t]
        for k in range(3):
            skip = far - 4 if k == 2 and t == TREES - 1 else STEPS

            @pl.when((s < 2 ** k) & (s != skip))
            def _():
                to_parent(s + 2 ** k, t, k).wait_recv()
                total[s, t] = total[s, t] + child[s + 2 ** k - 1, t]
        if t == TREES - 1:
            for which, parent in ((0, far - 4), (1, far - 2)):
                @pl.when(s == parent)
                def _():
                    add_far(s, which)

    def step_back(i, carry):
        s = back_order(i)
        slot = lax.rem(i, RING)
        with jax.named_scope('give'):
            give(s, slot)

            @pl.when(i + RING < STEPS)
            def _():
                load(back_order(i + RING), slot, 1)
                load(back_order(i + RING), slot, 0)

            @pl.when(i == 0)
            def _():
                send_small()
        with jax.named_scope('take'):
            join(s)
            for t in range(TREES):
                gather_children(s, t)
                for k in range(3):
                    skip = far if k == 2 and t == TREES - 1 else STEPS

                    @pl.when((s >= 2 ** k) & (s < 2 ** (k + 1)) & (s != skip))
                    def _():
                        to_parent(s, t, k).start()
                if t == TREES - 1:
                    @pl.when(s == far)
                    def _():
                        from_far_to(0).start()
                        from_far_to(1).start()
        return carry

    lax.fori_loop(0, STEPS - 1, step_back, 0)
    chips = n // 2
    half, share = part.shape[0] // 2, part.shape[0] // n
    mine_rows = pl.ds(pl.multiple_of(core * half, 8), half)
    their_rows = pl.ds(pl.multiple_of((1 - core) * half, 8), half)
    most = slice(0, (TREES - 1) * width)
    with jax.named_scope('give'):
        give(0, (STEPS - 1) % RING)
        join(0)

    def hidden_grad(t):
        gather_children(0, t)
        g_one[:, chunks[t]] = jnp.where(z_one[:, chunks[t]] > 0.0, total[0, t], 0.0).astype(jnp.bfloat16)

    def weight_grad(out_rows, cols):
        return lax.dot_general(s_one[out_rows, cols], g_one[:, cols], COL_CONTRACT, preferred_element_type=jnp.float32)

    with jax.named_scope('take'):
        for t in range(TREES - 1):
            hidden_grad(t)
        part[...] = weight_grad(slice(None), most)
        hidden_grad(TREES - 1)
    with jax.named_scope('dw'):
        part[their_rows] = part[their_rows] + weight_grad(their_rows, chunks[-1])
        over = remote(part.at[their_rows], pair, psend, precv, partner)
        over.start()
        part[mine_rows] = part[mine_rows] + weight_grad(mine_rows, chunks[-1])
    reduce_small()
    with jax.named_scope('drain'):
        gather_drain(buf, sems_x)
        gather_drain(h_buf, sems_h)
        remote(stage, stage, dsend, drecv.at[0], partner).wait_send()
        remote(child, child, csend, crecv.at[0, 0], partner).wait_send()
    with jax.named_scope('pair'):
        over.wait()
        pair[...] = pair[...] + part[mine_rows]

    def share_of(q):
        return pl.ds(pl.multiple_of(q * share, 8), share)

    for to in other_chips(chip):
        remote(pair.at[share_of(to)], parts.at[chip], fsend, frecv, to * 2 + core).start()
    parts[chip] = pair[share_of(chip)]
    with jax.named_scope('red'):
        wait_all(parts.at[pl.ds(0, chips - 1)], fsend, frecv)
    own = whole.at[pl.ds(pl.multiple_of(core * half + chip * share, 8), share)]
    own[...] = jnp.sum(parts[...], axis=0)
    for to in other_chips(chip):
        remote(own, own, gsend, grecv, to * 2 + core).start()
    with jax.named_scope('spread'):
        wait_all(whole.at[pl.ds(0, (chips - 1) * share)], gsend, grecv)
    swap = remote(whole.at[mine_rows], whole.at[mine_rows], qsend, qrecv, partner)
    swap.start()
    finish_small()
    dw2_ref[...] = small_whole[0:dw2_ref.shape[0]]
    loss_ref[...] = small_whole[edge:edge + 8]
    with jax.named_scope('swap'):
        swap.wait()
    dw_ref[...] = whole[0:feats]


def finish_kernel(loss_in, dw_in, dw2_in, loss_ref, dw_ref, dw2_ref):
    loss_ref[...] = loss_in[0:1, 0:1]
    dw_ref[...] = dw_in[...]
    dw2_ref[...] = dw2_in[...]


def train_step(x_rows, w_one, w2t, labels, mask, adj):
    rows, nodes = adj.shape
    n = nodes // rows
    feats, width = x_rows.shape[0], rows // TREES
    classes, hidden = w2t.shape
    units = n * TREES
    small = -(-classes // 8) * 8 + 8
    share = -(-feats // (8 * n)) * 8
    vmem, hbm = pl.BlockSpec(memory_space=pltpu.VMEM), pl.BlockSpec(memory_space=pl.ANY)
    dma, f32, bf16 = pltpu.SemaphoreType.DMA, jnp.float32, jnp.bfloat16
    block = (TREES, hidden, width)
    loss, dw_one, dw_two = pl.pallas_call(
        functools.partial(step_kernel, n),
        name='step',
        out_shape=(pltpu.VMEM((8, hidden), f32), pltpu.VMEM((feats, hidden), f32), pltpu.VMEM((classes, hidden), f32)),
        in_specs=[hbm] * 6,
        out_specs=(vmem,) * 3,
        scratch_shapes=[
            pltpu.VMEM((RING * 8, rows, width), bf16), pltpu.VMEM((units, feats, width), bf16), pltpu.VMEM((feats, rows), f32),
            pltpu.VMEM((units, hidden, width), bf16), pltpu.VMEM((n * share, rows), bf16), pltpu.VMEM((hidden, rows), f32),
            pltpu.VMEM((hidden, rows), bf16), pltpu.VMEM((feats, hidden), f32), pltpu.VMEM((small, hidden), f32), pltpu.VMEM((n, 1, 128), f32),
            pltpu.VMEM((STEPS, *block), f32), pltpu.VMEM(block, f32), pltpu.VMEM((STEPS, *block), f32), pltpu.VMEM((STEPS - 1, *block), f32),
            pltpu.VMEM((n * share, hidden), f32), pltpu.VMEM((n // 2, share, hidden), f32), pltpu.VMEM((n * share, hidden), f32),
            pltpu.VMEM((n, 8, hidden), f32), pltpu.VMEM((small, hidden), f32), pltpu.VMEM((n // 2 * share, hidden), f32),
            pltpu.VMEM((classes, rows), bf16), pltpu.VMEM((hidden, rows), bf16), pltpu.VMEM((1, rows), f32),
            pltpu.VMEM((classes, hidden), f32), pltpu.VMEM((1, rows), jnp.int32), pltpu.VMEM((1, rows), jnp.int32),
            dma((RING, 2)), dma, dma((4,)), dma, dma, dma, dma((STEPS,)), dma, dma((STEPS - 1, TREES)), *[dma] * 13, *gather_sems(), *gather_sems()],
        compiler_params=pltpu.CompilerParams(collective_id=0, has_side_effects=True, vmem_limit_bytes=62000000),
        cost_estimate=pl.CostEstimate(flops=2 * rows * nodes * (feats + 2 * hidden), bytes_accessed=6 * rows * nodes, transcendentals=0),
    )(*[pltpu.with_memory_space_constraint(x, pltpu.HBM) for x in (x_rows, w_one, w2t, labels, mask, adj)])
    return pl.pallas_call(
        finish_kernel,
        name='finish',
        out_shape=(jax.ShapeDtypeStruct((1, 1), f32), jax.ShapeDtypeStruct((feats, hidden), f32), jax.ShapeDtypeStruct((classes, hidden), f32)),
        in_specs=[vmem] * 3,
        out_specs=(vmem,) * 3,
    )(*[pltpu.with_memory_space_constraint(x, pltpu.VMEM) for x in (loss, dw_one, dw_two)])


def solution(mesh):
    axis_name = AXIS

    def local_step(adj_rows, feat_rows, w_one, w_two, label_rows, mask_rows):
        rows = adj_rows.shape[0]
        loss, dw_one, dw_two = train_step(feat_rows.T, w_one, w_two.T, label_rows.reshape(1, rows), mask_rows.reshape(1, rows), adj_rows)
        return loss.reshape(1), dw_one, dw_two.T

    return jax.shard_map(local_step, mesh=mesh, in_specs=(P(axis_name, None), P(axis_name, None), P(None, None), P(None, None), P(axis_name), P(axis_name)), out_specs=(P(None), P(None, None), P(None, None)), check_vma=False)
```

```python
import functools

import jax
import jax.numpy as jnp
from jax import lax
from jax.experimental import pallas as pl
from jax.experimental.pallas import tpu as pltpu
from jax.sharding import PartitionSpec as P

MESH = pl.DeviceIdType.MESH
AXIS = 'nodes'
TREES = 4
RING = 4
STEPS = 8
COL_CONTRACT = (((1,), (1,)), ((), ()))
ROW_CONTRACT = (((0,), (0,)), ((), ()))


def tree_axis(tree, k, core, chip):
    if tree < 3:
        weight = 2 ** ((tree + k) % 3)
        return weight, lax.rem(chip // weight, 2)
    weight = (1 - core) * 2 ** k + core * 2 ** (2 - k)
    low, high = lax.rem(chip // 2 ** k, 2), lax.rem(chip // 2 ** (2 - k), 2)
    return weight, (1 - core) * low + core * high


def chip_at(tree, offset, core, chip):
    out = chip
    for k in range(3):
        weight, bit = tree_axis(tree, k, core, chip)
        out = out + lax.rem(offset // 2 ** k, 2) * weight * (1 - 2 * bit)
    return out


def early_order(place):
    pair = (place + 1) // 2
    return place + (pair * (4 - pair)) // 4 * (7 - 2 * place)


def other_chips(chip):
    for flips in ((1, 2, 4), (1, 4), (1, 2), (2, 4), (1,), (2,), (4,)):
        yield chip + sum(w * (1 - 2 * lax.rem(chip // w, 2)) for w in flips)


def unit_at(tree, offset, core, chip):
    return (chip_at(tree, offset, core, chip) * 2 + core) * TREES + tree


def neighbour(tree, k, core, chip):
    weight, bit = tree_axis(tree, k, core, chip)
    return (chip + weight * (1 - 2 * bit)) * 2 + core


def remote(src, dst, send_sem, recv_sem, device):
    return pltpu.make_async_remote_copy(src_ref=src, dst_ref=dst, send_sem=send_sem, recv_sem=recv_sem, device_id=(device,), device_id_type=MESH)


def place():
    me = lax.axis_index(AXIS)
    core, chip = lax.rem(me, 2), me // 2
    return me, core, chip, chip * 2 + 1 - core


def gather_send(buf, sems, tree, offset, k, unit, rows=slice(None)):
    send, recv, hand = sems
    me, core, chip, partner = place()
    ref = buf.at[unit, rows]
    remote(ref, ref, send, recv.at[offset + 2 ** k - 1, tree], neighbour(tree, k, core, chip)).start()


def gather_hand(buf, sems, slot, unit):
    send, recv, hand = sems
    me, core, chip, partner = place()
    remote(buf.at[unit], buf.at[unit], send, hand.at[slot], partner).start()


def gather_start(buf, sems, links):
    me = lax.axis_index(AXIS)
    for k in range(links):
        for t in range(TREES):
            gather_send(buf, sems, t, 0, k, me * TREES + t)
        if k == 0:
            for t in range(TREES):
                gather_hand(buf, sems, 0, me * TREES + t)


def gather_arrive(buf, sems, s, links, trees=range(TREES), slot=None, cut=None):
    send, recv, hand = sems
    me, core, chip, partner = place()
    units = {t: unit_at(t, s, core, chip) for t in trees}
    for t, u in units.items():
        remote(buf.at[u], buf.at[u], send, recv.at[s - 1, t], partner).wait_recv()
        split = cut is not None and t == TREES - 1

        @pl.when(s == 1)
        def _():
            gather_send(buf, sems, t, s, 1, u)

        @pl.when((s > 1) & (s < (3 if split else 4)))
        def _():
            gather_send(buf, sems, t, s, 2, u)
        if split:
            @pl.when(s == 3)
            def _():
                gather_send(buf, sems, t, s, 2, u, slice(0, cut))

            @pl.when(s == 5)
            def _():
                gather_send(buf, sems, t, s, 1, u, slice(cut, None))
        gather_hand(buf, sems, s if slot is None else slot, u)

    @pl.when(s == 1)
    def _():
        if links < 3:
            for t in range(TREES):
                gather_send(buf, sems, t, 0, 2, me * TREES + t)
        for t, u in units.items():
            gather_send(buf, sems, t, s, 2, u)


def gather_take(buf, sems, slot, count=TREES):
    send, recv, hand = sems
    me, core, chip, partner = place()
    units = buf.at[pl.ds(0, count)]
    remote(units, units, send, hand.at[slot], partner).wait_recv()


def gather_drain(buf, sems):
    send, recv, hand = sems
    me, core, chip, partner = place()
    sent = buf.at[pl.ds(0, TREES * (STEPS - 1 + STEPS))]
    remote(sent, sent, send, hand.at[0], partner).wait_send()


def gather_sems():
    dma = pltpu.SemaphoreType.DMA
    return [dma, dma((STEPS - 1, TREES)), dma((STEPS + 1,))]


def barrier_near():
    me, core, chip, partner = place()
    sem = pltpu.get_barrier_semaphore()
    pl.semaphore_signal(sem, inc=1, device_id=(partner,), device_id_type=MESH)
    for k in range(3):
        pl.semaphore_signal(sem, inc=1, device_id=(neighbour(0, k, core, chip),), device_id_type=MESH)
    pl.semaphore_wait(sem, 4)


def send_all(n, src, dst, send_sem, recv_sem):
    me = lax.axis_index(AXIS)
    for i in range(1, n):
        to = lax.rem(me + i, n)
        remote(src(to), dst, send_sem, recv_sem, to).start()


def wait_all(ref, send_sem, recv_sem):
    me, core, chip, partner = place()
    copy = remote(ref, ref, send_sem, recv_sem, partner)
    copy.wait_send()
    copy.wait_recv()


def step_kernel(n, x_ref, w_hbm, w2t_hbm, y_hbm, m_hbm, adj, loss_ref, dw_ref, dw2_ref,
                ring, buf, acc, h_buf, s_one, z_one, u_two, w_v, small, count, stage, mine, total, child, part, parts, whole,
                small_parts, small_whole, pair, g_two, g_one, picked, w2t_ref, y_ref, m_ref,
                ring_sem, x_sem, w_sem, count_send, count_recv, dsend, drecv, csend, crecv, fsend, frecv, gsend, grecv,
                ssend, srecv, bsend, brecv, psend, precv, qsend, qrecv, cut_sem, *sems):
    me, core, chip, partner = place()
    sems_x, sems_h = sems[:3], sems[3:]
    width = buf.shape[2]
    feats, rows = acc.shape
    hidden = h_buf.shape[1]
    chunks = [slice(t * width, (t + 1) * width) for t in range(TREES)]

    def slab(s, slot, j):
        u = unit_at(j % TREES, s, core if j < TREES else 1 - core, chip)
        return pltpu.make_async_copy(adj.at[:, pl.ds(pl.multiple_of(u * width, width), width)], ring.at[slot * 8 + j], ring_sem.at[slot, j // TREES])

    def load(s, slot, half):
        for t in range(TREES):
            slab(s, slot, half * TREES + t).start()

    def loaded(slot, half):
        four = ring.at[pl.ds(0, TREES)]
        pltpu.make_async_copy(four, four, ring_sem.at[slot, half]).wait()

    with jax.named_scope('start'):
        fetch = [pltpu.make_async_copy(x_ref.at[:, pl.ds(t * width, width)], buf.at[me * TREES + t], x_sem) for t in range(TREES)]
        for copy in fetch:
            copy.start()
        barrier_near()
        four = buf.at[pl.ds(0, TREES)]
        pltpu.make_async_copy(four, four, x_sem).wait()
    gather_start(buf, sems_x, 2)
    params = [pltpu.make_async_copy(src, dst, w_sem.at[i]) for i, (src, dst) in enumerate(((w_hbm, w_v), (w2t_hbm, w2t_ref), (y_hbm, y_ref), (m_hbm, m_ref)))]
    for copy in params:
        copy.start()
    for s in range(RING):
        for half in range(2):
            load(s, s, half)
    acc[...] = jnp.zeros_like(acc)

    def terms(units_ref, s, slot, half, trees=range(TREES)):
        which = core if half == 0 else 1 - core
        return [(units_ref, unit_at(t, s, which, chip), slot * 8 + half * TREES + t) for t in trees]

    def aggregate(out, pairs):
        for cols in chunks:
            out[:, cols] += sum(lax.dot_general(ref[u], ring[j, cols], COL_CONTRACT, preferred_element_type=jnp.float32) for ref, u, j in pairs)

    def step_one(s, carry):
        with jax.named_scope('arrive'):
            @pl.when(s > 0)
            def _():
                gather_arrive(buf, sems_x, s, 2, cut=cut)
        for half in range(2):
            with jax.named_scope('consume'):
                if half == 1:
                    gather_take(buf, sems_x, s)
                slot = lax.rem(s, RING)
                loaded(slot, half)
                aggregate(acc, terms(buf, s, slot, half))
                late = s // RING
                load((1 - late) * (s + RING) + late * early_order(s - late * RING), slot, half)
        return carry

    cut = feats * 2 // 3 // 16 * 16
    final, slot = STEPS - 1, (STEPS - 1) % RING
    lax.fori_loop(0, final, step_one, 0)
    early, late = (range(TREES - 1), final), (range(TREES - 1, TREES), STEPS)
    for half in range(2):
        for trees, hand in (early, late):
            with jax.named_scope('consume'):
                if half == 0:
                    gather_arrive(buf, sems_x, final, 2, trees, hand, cut)
                else:
                    gather_take(buf, sems_x, hand, len(trees))
                if hand == final:
                    loaded(slot, half)
                aggregate(acc, terms(buf, final, slot, half, trees))
    for half in range(2):
        load(early_order(final - RING), slot, half)
    with jax.named_scope('mid'):
        for copy in params:
            copy.wait()
        s_one[0:feats] = acc[...].astype(jnp.bfloat16)
        s_one[feats:] = jnp.zeros_like(s_one[feats:])
        w_rows = w_v[...].astype(jnp.bfloat16)
        for t, cols in enumerate(chunks):
            z = lax.dot_general(w_rows, s_one[0:feats, cols], ROW_CONTRACT, preferred_element_type=jnp.float32)
            z_one[:, cols] = z
            h_buf[me * TREES + t] = jnp.maximum(z, 0.0).astype(jnp.bfloat16)
    gather_start(h_buf, sems_h, 3)
    weight = m_ref[...].astype(jnp.float32)
    count[me] = jnp.broadcast_to(jnp.sum(weight, axis=1, keepdims=True), count.shape[1:])
    send_all(n, lambda to: count.at[me], count.at[me], count_send, count_recv)
    two = acc.at[0:hidden]

    def take_two(p, half):
        loaded(lax.rem(p, RING), half)
        return terms(h_buf, early_order(p), lax.rem(p, RING), half)

    def back_order(i):
        return early_order(STEPS - 1 - i)

    def load_two(p, half):
        late = p // RING
        load((1 - late) * early_order(p + RING - late * RING) + late * back_order(p - late * RING), lax.rem(p, RING), half)

    two[...] = jnp.zeros_like(two)
    with jax.named_scope('consume'):
        aggregate(two, take_two(0, 0))
        load_two(0, 0)
        gather_take(h_buf, sems_h, 0)
        aggregate(two, take_two(0, 1))
        load_two(0, 1)
    with jax.named_scope('arrive'):
        gather_arrive(h_buf, sems_h, 1, 3)
    with jax.named_scope('consume'):
        aggregate(two, take_two(1, 0))
        load_two(1, 0)

    for p in range(2, STEPS):
        with jax.named_scope('arrive'):
            gather_arrive(h_buf, sems_h, early_order(p), 3, cut=hidden * 2 // 3 // 16 * 16)
            gather_take(h_buf, sems_h, early_order(p - 1))
        with jax.named_scope('consume'):
            aggregate(two, take_two(p - 1, 1) + take_two(p, 0))
            load_two(p - 1, 1)
            load_two(p, 0)
    with jax.named_scope('last'):
        gather_take(h_buf, sems_h, STEPS - 1)
        aggregate(two, take_two(STEPS - 1, 1))
        load_two(STEPS - 1, 1)
    with jax.named_scope('soft'):
        wait_all(count.at[pl.ds(0, n - 1)], count_send, count_recv)
        labelled = jnp.sum(count[...], axis=0)[0:1, 0:1]
        s_two = two[...].astype(jnp.bfloat16)
        w_two = w2t_ref[...].astype(jnp.bfloat16)
        logits = jnp.dot(w_two, s_two, preferred_element_type=jnp.float32)
        shifted = logits - jnp.max(logits, axis=0, keepdims=True)
        log_prob = shifted - jnp.log(jnp.sum(jnp.exp(shifted), axis=0, keepdims=True))
        hot = lax.broadcasted_iota(jnp.int32, logits.shape, 0) == y_ref[...]
        grad = (weight * (jnp.exp(log_prob) - hot.astype(jnp.float32)) / labelled).astype(jnp.bfloat16)
        u_two[...] = lax.dot_general(w_two, grad, ROW_CONTRACT, preferred_element_type=jnp.float32).astype(jnp.bfloat16)
        g_two[...] = grad
        picked[...] = -weight * jnp.sum(jnp.where(hot, log_prob, 0.0), axis=0, keepdims=True)
    classes = g_two.shape[0]
    edge = small.shape[0] - 8
    owners = small.shape[0] // 8
    tile = pl.ds(pl.multiple_of(me * 8, 8), 8)

    def send_small():
        loss = jnp.sum(picked[...], axis=1, keepdims=True)
        labelled = jnp.sum(count[...], axis=0)[0:1, 0:1]
        small[0:classes] = lax.dot_general(g_two[...], two[...].astype(jnp.bfloat16), COL_CONTRACT, preferred_element_type=jnp.float32)
        small[classes:edge] = jnp.zeros((edge - classes, hidden), jnp.float32)
        small[edge:] = jnp.broadcast_to(loss / labelled, (8, hidden))
        for o in range(owners):
            @pl.when(me != o)
            def _():
                remote(small.at[pl.ds(o * 8, 8)], small_parts.at[me], ssend, srecv, o).start()

    def to_partner(s, t):
        return remote(stage.at[s, t], total.at[s, t], dsend, drecv.at[s], partner)

    def to_parent(s, t, k):
        return remote(total.at[s, t], child.at[s - 1, t], csend, crecv.at[s - 1, t], neighbour(t, k, core, chip))

    def reduce_small():
        @pl.when(me < owners)
        def _():
            small_parts[me] = small[tile]
            got = small_parts.at[pl.ds(0, n - 1)]
            remote(got, got, ssend, srecv, partner).wait_recv()
            small_whole[tile] = jnp.sum(small_parts[...], axis=0)
            for i in range(1, n):
                remote(small_whole.at[tile], small_whole.at[tile], bsend, brecv, lax.rem(me + i, n)).start()

    def finish_small():
        sent = small_parts.at[pl.ds(0, n - 1)]
        fewer, every = small_whole.at[pl.ds(0, owners * 8 - 8)], small_whole.at[pl.ds(0, owners * 8)]

        @pl.when(me < owners)
        def _():
            remote(sent, sent, bsend, brecv, partner).wait_send()
            remote(fewer, fewer, ssend, brecv, partner).wait_send()
            remote(fewer, fewer, ssend, brecv, partner).wait_recv()

        @pl.when(me >= owners)
        def _():
            remote(every, every, ssend, brecv, partner).wait_send()
            remote(every, every, ssend, brecv, partner).wait_recv()

    far, edge_row = STEPS - 2, hidden * 2 // 3 // 8 * 8 + 8

    def from_far_to(which):
        rows, k = ((slice(0, edge_row), 2), (slice(edge_row, hidden), 1))[which]
        sem = cut_sem if which else crecv.at[far - 1, TREES - 1]
        return remote(total.at[far, TREES - 1, rows], child.at[far - 1, TREES - 1, rows], csend, sem, neighbour(TREES - 1, k, core, chip))

    def add_far(s, which):
        from_far_to(which).wait_recv()
        rows = (slice(0, edge_row), slice(edge_row, hidden))[which]
        total[s, TREES - 1, rows] = total[s, TREES - 1, rows] + child[far - 1, TREES - 1, rows]

    def give(s, slot):
        loaded(slot, 1)
        for t in range(TREES):
            stage[s, t] = jnp.dot(u_two[...], ring[slot * 8 + TREES + t], preferred_element_type=jnp.float32)
        for t in range(TREES):
            to_partner(s, t).start()
        loaded(slot, 0)
        for t in range(TREES):
            mine[t] = jnp.dot(u_two[...], ring[slot * 8 + t], preferred_element_type=jnp.float32)

    def join(s):
        remote(total.at[s], total.at[s], dsend, drecv.at[s], partner).wait_recv()

    def gather_children(s, t):
        total[s, t] = total[s, t] + mine[t]
        for k in range(3):
            skip = far - 4 if k == 2 and t == TREES - 1 else STEPS

            @pl.when((s < 2 ** k) & (s != skip))
            def _():
                to_parent(s + 2 ** k, t, k).wait_recv()
                total[s, t] = total[s, t] + child[s + 2 ** k - 1, t]
        if t == TREES - 1:
            for which, parent in ((0, far - 4), (1, far - 2)):
                @pl.when(s == parent)
                def _():
                    add_far(s, which)

    def step_back(i, carry):
        s = back_order(i)
        slot = lax.rem(i, RING)
        with jax.named_scope('give'):
            give(s, slot)

            @pl.when(i + RING < STEPS)
            def _():
                load(back_order(i + RING), slot, 1)
                load(back_order(i + RING), slot, 0)

            @pl.when(i == 0)
            def _():
                send_small()
        with jax.named_scope('take'):
            join(s)
            for t in range(TREES):
                gather_children(s, t)
                for k in range(3):
                    skip = far if k == 2 and t == TREES - 1 else STEPS

                    @pl.when((s >= 2 ** k) & (s < 2 ** (k + 1)) & (s != skip))
                    def _():
                        to_parent(s, t, k).start()
                if t == TREES - 1:
                    @pl.when(s == far)
                    def _():
                        from_far_to(0).start()
                        from_far_to(1).start()
        return carry

    lax.fori_loop(0, STEPS - 1, step_back, 0)
    chips = n // 2
    half, share = part.shape[0] // 2, part.shape[0] // n
    mine_rows = pl.ds(pl.multiple_of(core * half, 8), half)
    their_rows = pl.ds(pl.multiple_of((1 - core) * half, 8), half)
    most = slice(0, (TREES - 1) * width)
    with jax.named_scope('give'):
        give(0, (STEPS - 1) % RING)
        join(0)

    def hidden_grad(t):
        gather_children(0, t)
        g_one[:, chunks[t]] = jnp.where(z_one[:, chunks[t]] > 0.0, total[0, t], 0.0).astype(jnp.bfloat16)

    def weight_grad(out_rows, cols):
        return lax.dot_general(s_one[out_rows, cols], g_one[:, cols], COL_CONTRACT, preferred_element_type=jnp.float32)

    with jax.named_scope('take'):
        for t in range(TREES - 1):
            hidden_grad(t)
        part[...] = weight_grad(slice(None), most)
        hidden_grad(TREES - 1)
    with jax.named_scope('dw'):
        part[their_rows] = part[their_rows] + weight_grad(their_rows, chunks[-1])
        over = remote(part.at[their_rows], pair, psend, precv, partner)
        over.start()
        part[mine_rows] = part[mine_rows] + weight_grad(mine_rows, chunks[-1])
    reduce_small()
    with jax.named_scope('drain'):
        gather_drain(buf, sems_x)
        gather_drain(h_buf, sems_h)
        remote(stage, stage, dsend, drecv.at[0], partner).wait_send()
        remote(child, child, csend, crecv.at[0, 0], partner).wait_send()
    with jax.named_scope('pair'):
        over.wait()
        pair[...] = pair[...] + part[mine_rows]

    def share_of(q):
        return pl.ds(pl.multiple_of(q * share, 8), share)

    for to in other_chips(chip):
        remote(pair.at[share_of(to)], parts.at[chip], fsend, frecv, to * 2 + core).start()
    parts[chip] = pair[share_of(chip)]
    with jax.named_scope('red'):
        wait_all(parts.at[pl.ds(0, chips - 1)], fsend, frecv)
    own = whole.at[pl.ds(pl.multiple_of(core * half + chip * share, 8), share)]
    own[...] = jnp.sum(parts[...], axis=0)
    for to in other_chips(chip):
        remote(own, own, gsend, grecv, to * 2 + core).start()
    with jax.named_scope('spread'):
        wait_all(whole.at[pl.ds(0, (chips - 1) * share)], gsend, grecv)
    swap = remote(whole.at[mine_rows], whole.at[mine_rows], qsend, qrecv, partner)
    swap.start()
    finish_small()
    dw2_ref[...] = small_whole[0:dw2_ref.shape[0]]
    loss_ref[...] = small_whole[edge:edge + 8]
    with jax.named_scope('swap'):
        swap.wait()
    dw_ref[...] = whole[0:feats]


def finish_kernel(loss_in, dw_in, dw2_in, loss_ref, dw_ref, dw2_ref):
    loss_ref[...] = loss_in[0:1, 0:1]
    dw_ref[...] = dw_in[...]
    dw2_ref[...] = dw2_in[...]


def train_step(x_rows, w_one, w2t, labels, mask, adj):
    rows, nodes = adj.shape
    n = nodes // rows
    feats, width = x_rows.shape[0], rows // TREES
    classes, hidden = w2t.shape
    units = n * TREES
    small = -(-classes // 8) * 8 + 8
    share = -(-feats // (8 * n)) * 8
    vmem, hbm = pl.BlockSpec(memory_space=pltpu.VMEM), pl.BlockSpec(memory_space=pl.ANY)
    dma, f32, bf16 = pltpu.SemaphoreType.DMA, jnp.float32, jnp.bfloat16
    block = (TREES, hidden, width)
    loss, dw_one, dw_two = pl.pallas_call(
        functools.partial(step_kernel, n),
        name='step',
        out_shape=(pltpu.VMEM((8, hidden), f32), pltpu.VMEM((feats, hidden), f32), pltpu.VMEM((classes, hidden), f32)),
        in_specs=[hbm] * 6,
        out_specs=(vmem,) * 3,
        scratch_shapes=[
            pltpu.VMEM((RING * 8, rows, width), bf16), pltpu.VMEM((units, feats, width), bf16), pltpu.VMEM((feats, rows), f32),
            pltpu.VMEM((units, hidden, width), bf16), pltpu.VMEM((n * share, rows), bf16), pltpu.VMEM((hidden, rows), f32),
            pltpu.VMEM((hidden, rows), bf16), pltpu.VMEM((feats, hidden), f32), pltpu.VMEM((small, hidden), f32), pltpu.VMEM((n, 1, 128), f32),
            pltpu.VMEM((STEPS, *block), f32), pltpu.VMEM(block, f32), pltpu.VMEM((STEPS, *block), f32), pltpu.VMEM((STEPS - 1, *block), f32),
            pltpu.VMEM((n * share, hidden), f32), pltpu.VMEM((n // 2, share, hidden), f32), pltpu.VMEM((n * share, hidden), f32),
            pltpu.VMEM((n, 8, hidden), f32), pltpu.VMEM((small, hidden), f32), pltpu.VMEM((n // 2 * share, hidden), f32),
            pltpu.VMEM((classes, rows), bf16), pltpu.VMEM((hidden, rows), bf16), pltpu.VMEM((1, rows), f32),
            pltpu.VMEM((classes, hidden), f32), pltpu.VMEM((1, rows), jnp.int32), pltpu.VMEM((1, rows), jnp.int32),
            dma((RING, 2)), dma, dma((4,)), dma, dma, dma, dma((STEPS,)), dma, dma((STEPS - 1, TREES)), *[dma] * 13, *gather_sems(), *gather_sems()],
        compiler_params=pltpu.CompilerParams(collective_id=0, has_side_effects=True, vmem_limit_bytes=62000000),
        cost_estimate=pl.CostEstimate(flops=2 * rows * nodes * (feats + 2 * hidden), bytes_accessed=6 * rows * nodes, transcendentals=0),
    )(*[pltpu.with_memory_space_constraint(x, pltpu.HBM) for x in (x_rows, w_one, w2t, labels, mask, adj)])
    return pl.pallas_call(
        finish_kernel,
        name='finish',
        out_shape=(jax.ShapeDtypeStruct((1, 1), f32), jax.ShapeDtypeStruct((feats, hidden), f32), jax.ShapeDtypeStruct((classes, hidden), f32)),
        in_specs=[vmem] * 3,
        out_specs=(vmem,) * 3,
    )(*[pltpu.with_memory_space_constraint(x, pltpu.VMEM) for x in (loss, dw_one, dw_two)])


def solution(mesh):
    axis_name = AXIS

    def local_step(adj_rows, feat_rows, w_one, w_two, label_rows, mask_rows):
        rows = adj_rows.shape[0]
        loss, dw_one, dw_two = train_step(feat_rows.T, w_one, w_two.T, label_rows.reshape(1, rows), mask_rows.reshape(1, rows), adj_rows)
        return loss.reshape(1), dw_one, dw_two.T

    return jax.shard_map(local_step, mesh=mesh, in_specs=(P(axis_name, None), P(axis_name, None), P(None, None), P(None, None), P(axis_name), P(axis_name)), out_specs=(P(None), P(None, None), P(None, None)), check_vma=False)
```
